32 devices in a mesh: section: 2 (over core), tensor: 4 (over y, x), dp: 4 (over z).
Axes of the slice: x: 2, y: 2, z: 4, core: 2. Of those that a mesh axis runs over, the one named last changes fastest.
Arguments:
- block_input: bfloat16 [8, 144, 2048], P('dp'), may hold values from -6 to 6
- grad_output: bfloat16 [8, 144, 2048], P('dp'), may hold values from -6 to 6
- segment_ids: int32 [8, 144], P('dp'), may hold values from 0 to 2, never falling along the last dimension, each value on 1 to 72 neighbouring positions
- w_qkv: bfloat16 [2, 2048, 3, 2048], P('section', None, None, 'tensor'), may hold values from -0.35355339 to 0.35355339
- w_out: bfloat16 [2, 2048, 2048], P('section', 'tensor'), may hold values from -0.375 to 0.375
- w_fc1: bfloat16 [2, 2048, 8192], P('section', None, 'tensor'), may hold values from -0.125 to 0.125
- w_fc2: bfloat16 [2, 8192, 2048], P('section', 'tensor'), may hold values from -0.0625 to 0.0625
- norm_gains: float32 [2, 2, 2048], P('section'), may hold values from 0.5 to 1.5
- norm_biases: float32 [2, 2, 2048], P('section'), may hold values from -3 to 3
Outputs:
- layer_outputs: bfloat16 [2, 8, 144, 2048], P('section', 'dp')
- input_grads: float32 [2, 8, 144, 2048], P('section', 'dp')
- grad_qkv: float32 [2, 2048, 3, 2048], P('section', 'dp', None, 'tensor')
- grad_out_proj: float32 [2, 2048, 2048], P('section', 'tensor', 'dp')
- grad_fc1: float32 [2, 2048, 8192], P('section', 'dp', 'tensor')
- grad_fc2: float32 [2, 8192, 2048], P('section', 'tensor', 'dp')
- grad_gains: float32 [2, 2, 2048], P('section', None, 'dp')
- grad_biases: float32 [2, 2, 2048], P('section', None, 'dp')
The draws below stay inside these ranges and needn't reach their ends.
All inputs are finite; a program needn't handle non-finite values.
Results may differ from the reference program's by a relative error of at most 0.012.
Values may be sent and summed in bfloat16 or wider, within the bound.
A program may use at most 256 MiB of HBM per device.

```python
import math
import jax
import jax.numpy as jnp
import numpy as np
from jax import lax

D = 2048
HEAD = 256
ROT = 64
FF = 8192
LEN = 144
MICRO = 2
LAYERS = 2
ROWS = 8


def draw_w_qkv(key, part):
    normal_draw = jnp.clip(jax.random.normal(key, (LAYERS, D, 3, D), jnp.float32), -4.0, 4.0) * D ** (-0.5)
    return normal_draw.astype(jnp.bfloat16)


def shard_levels(rng, shape, cuts, smallest, top_value):
    gain, own = 1.0, jax.random.fold_in(rng, 6)
    for dim, blocks in cuts:
        heights = jnp.exp(jax.random.uniform(jax.random.fold_in(own, dim), (blocks,), jnp.float32, smallest / len(cuts), top_value / len(cuts)))
        gain = gain * jnp.repeat(heights, shape[dim] // blocks).reshape([-1 if axis == dim else 1 for axis in range(len(shape))])
    return gain


def profile(count, total, most, lean):
    portions = [(1 << 20) // math.isqrt(grade ** lean) + 1 for grade in range(2, count + 1)]
    rest, counts = total - most - (count - 1), [1] * (count - 1)
    while rest > 0:
        candidates = [i for i in range(count - 1) if counts[i] < most]
        pool, left = sum([portions[i] for i in candidates]), rest
        for i in candidates:
            addition = min(most - counts[i], max(1, left * portions[i] // pool), rest)
            counts[i] = counts[i] + addition
            rest = rest - addition
    return np.array([most] + counts)


def uneven(key, number_of, total, reach, lean):
    if number_of == 2:
        one = jax.random.randint(key, (), max(1, total - reach), min(reach, total - 1) + 1)
        return jnp.stack([one, total - one])
    lengths = jnp.asarray(profile(number_of, total, reach, lean), jnp.int32)
    couples = (number_of - 1) // 2
    giver, sink = lengths[1:1 + 2 * couples:2], lengths[2:2 + 2 * couples:2]
    margin = jnp.minimum(giver - 1, reach - sink)
    moved = jax.random.randint(jax.random.fold_in(key, 1), (couples,), 0, 1 << 20) % (margin + 1)
    lengths = lengths.at[1:1 + 2 * couples:2].set(giver - moved).at[2:2 + 2 * couples:2].set(sink + moved)
    return lengths[jax.random.permutation(jax.random.fold_in(key, 2), number_of)]


def noise(own_key, extent, deviation, reach, cuts=(), held_as=jnp.bfloat16):
    level = shard_levels(own_key, extent, cuts, -0.22, 0.18) if cuts else 1.0
    values = jax.random.normal(own_key, extent, jnp.float32) * deviation * level
    return jnp.minimum(jnp.maximum(values, -reach), reach).astype(held_as)


def setup_inputs(seed: int = 0) -> dict:
    key_list = jax.random.split(jax.random.key(seed), 10)
    return {
        "block_input": noise(key_list[0], (ROWS, LEN, D), 1.0, 6.0, ((0, 4),)),
        "grad_output": noise(key_list[1], (ROWS, LEN, D), 1.0, 6.0, ((0, 4),)),
        "segment_ids": jax.vmap(lambda own: jnp.searchsorted(jnp.cumsum(uneven(own, 3, LEN, LEN // 2, 0)), jnp.arange(LEN), side="right"))(jax.random.split(key_list[2], ROWS)).reshape((ROWS, LEN)).astype(jnp.int32),
        "w_qkv": draw_w_qkv(jax.random.fold_in(key_list[9], 71), 0),
        "w_out": noise(key_list[4], (LAYERS, D, D), (D // 8) ** -0.5, 0.375, ((0, 2), (1, 4))),
        "w_fc1": noise(key_list[5], (LAYERS, D, FF), D ** -0.5, 0.125, ((0, 2), (2, 4))),
        "w_fc2": noise(key_list[6], (LAYERS, FF, D), FF ** -0.5, 0.0625, ((0, 2), (1, 4))),
        "norm_gains": jnp.clip(1.0 + 0.1 * jax.random.normal(key_list[7], (LAYERS, 2, D), jnp.float32), 0.5, 1.5),
        "norm_biases": noise(key_list[8], (LAYERS, 2, D), 0.5, 3.0, ((0, 2),), jnp.float32),
    }


NORM_EPSILON = 1e-05

def as_float(array):
    return lax.optimization_barrier(array).astype(jnp.float32)

def positions_of(segment):
    earlier = (segment[:, None, :] < segment[:, :, None]).astype(jnp.int32)
    return jnp.arange(segment.shape[1], dtype=jnp.int32)[None, :] - lax.optimization_barrier(jnp.sum(earlier, axis=2))

def rotary_tables(positions):
    frequency = jnp.exp(jnp.arange(ROT // 2, dtype=jnp.float32) * (-2.0 * math.log(10000.0) / ROT))
    angles = positions.astype(jnp.float32)[..., None] * frequency
    cosine = jnp.concatenate([jnp.cos(angles), jnp.cos(angles)], axis=-1)[:, :, None, :]
    sine_table = jnp.concatenate([jnp.sin(angles), jnp.sin(angles)], axis=-1)[:, :, None, :]
    return (cosine, sine_table)

def rotate(inputs, cosine, sine_table):
    rotated_part = inputs[..., :ROT]
    turned = jnp.concatenate([-rotated_part[..., ROT // 2:], rotated_part[..., :ROT // 2]], axis=-1)
    return jnp.concatenate([rotated_part * cosine + turned * sine_table, inputs[..., ROT:]], axis=-1)

def unrotate(gradient, cosine, sine_table):
    rotated_part = gradient[..., :ROT]
    scaled = rotated_part * sine_table
    turned = jnp.concatenate([scaled[..., ROT // 2:], -scaled[..., :ROT // 2]], axis=-1)
    return jnp.concatenate([rotated_part * cosine + turned, gradient[..., ROT:]], axis=-1)

def norm_forward(inputs, gain_vec, bias_vec):
    row_mean = lax.optimization_barrier(jnp.mean(inputs, axis=-1, keepdims=True))
    centred = inputs - row_mean
    inv_std = lax.rsqrt(lax.optimization_barrier(jnp.mean(centred * centred, axis=-1, keepdims=True)) + NORM_EPSILON)
    normed = centred * inv_std
    return ((normed * gain_vec + bias_vec).astype(jnp.bfloat16), normed, inv_std)

def norm_backward(gradient, normed, inv_std, gain_vec):
    scaled = gradient * gain_vec
    d_inputs = inv_std * (scaled - lax.optimization_barrier(jnp.mean(scaled, axis=-1, keepdims=True)) - normed * lax.optimization_barrier(jnp.mean(scaled * normed, axis=-1, keepdims=True)))
    return (d_inputs, lax.optimization_barrier(jnp.sum(gradient * normed, axis=(0, 1))), lax.optimization_barrier(jnp.sum(gradient, axis=(0, 1))))

def gelu_parts(hidden):
    normal_cdf = 0.5 * (1.0 + lax.erf(hidden * (1.0 / math.sqrt(2.0))))
    density = jnp.exp(-0.5 * hidden * hidden) * (1.0 / math.sqrt(2.0 * math.pi))
    return (hidden * normal_cdf, normal_cdf + hidden * density)

def attention_scores(queries, key_rows, allowed):
    scores = jnp.einsum('bqhd,bkhd->bhqk', as_float(queries), as_float(key_rows)) * (1.0 / math.sqrt(HEAD))
    return jnp.where(allowed[:, None], scores, -jnp.inf)

def layer_forward(inputs, segment, weights):
    w_qkv, w_out, w_fc1, w_fc2, gains, biases = weights
    batch_size, length, model_width = inputs.shape
    head_count = w_qkv.shape[2] // HEAD
    widened = inputs.astype(jnp.float32)
    attn_in, normed_a, inv_std_a = norm_forward(widened, gains[0], biases[0])
    mlp_in, normed_m, inv_std_m = norm_forward(widened, gains[1], biases[1])
    projected = jnp.dot(attn_in.reshape(-1, model_width), w_qkv.reshape(model_width, -1), preferred_element_type=jnp.float32)
    projected = projected.reshape(batch_size, length, 3, head_count, HEAD)
    cosine, sine_table = rotary_tables(positions_of(segment))
    queries = rotate(projected[:, :, 0], cosine, sine_table).astype(jnp.bfloat16)
    key_rows = rotate(projected[:, :, 1], cosine, sine_table).astype(jnp.bfloat16)
    values = projected[:, :, 2].astype(jnp.bfloat16)
    positions = jnp.arange(length, dtype=jnp.int32)
    allowed = (segment[:, :, None] == segment[:, None, :]) & (positions[None, :, None] >= positions[None, None, :])
    scores = attention_scores(queries, key_rows, allowed)
    row_max = lax.optimization_barrier(jnp.max(scores, axis=-1, keepdims=True))
    log_total = row_max + jnp.log(lax.optimization_barrier(jnp.sum(jnp.exp(scores - row_max), axis=-1, keepdims=True)))
    attn_probs = jnp.exp(scores - log_total).astype(jnp.bfloat16)
    context = jnp.einsum('bhqk,bkhd->bqhd', as_float(attn_probs), as_float(values))
    context = context.astype(jnp.bfloat16).reshape(batch_size * length, head_count * HEAD)
    hidden = jnp.dot(mlp_in.reshape(-1, model_width), w_fc1, preferred_element_type=jnp.float32)
    activated, gelu_slope = gelu_parts(hidden)
    activated = activated.astype(jnp.bfloat16)
    partial_value = jnp.dot(context, w_out, preferred_element_type=jnp.float32) + jnp.dot(activated, w_fc2, preferred_element_type=jnp.float32)
    stored = (attn_in, mlp_in, normed_a, inv_std_a, normed_m, inv_std_m, queries, key_rows, values, log_total, context, gelu_slope, activated, allowed, cosine, sine_table)
    return (partial_value.reshape(batch_size, length, model_width), stored)

def layer_backward(cotangent, stored, weights):
    w_qkv, w_out, w_fc1, w_fc2, gains, biases = weights
    attn_in, mlp_in, normed_a, inv_std_a, normed_m, inv_std_m, queries, key_rows, values, log_total, context, gelu_slope, activated, allowed, cosine, sine_table = stored
    batch_size, length, model_width = cotangent.shape
    head_count = queries.shape[2]
    grad_b = cotangent.astype(jnp.bfloat16).reshape(-1, model_width)
    g_fc2 = jnp.dot(activated.T, grad_b, preferred_element_type=jnp.float32)
    d_act = jnp.dot(grad_b, w_fc2.T, preferred_element_type=jnp.float32)
    d_hidden = (d_act * gelu_slope).astype(jnp.bfloat16)
    g_fc1 = jnp.dot(mlp_in.reshape(-1, model_width).T, d_hidden, preferred_element_type=jnp.float32)
    d_mlp = jnp.dot(d_hidden, w_fc1.T, preferred_element_type=jnp.float32).reshape(batch_size, length, model_width)
    g_out = jnp.dot(context.T, grad_b, preferred_element_type=jnp.float32)
    d_context = jnp.dot(grad_b, w_out.T, preferred_element_type=jnp.float32).astype(jnp.bfloat16)
    d_context = d_context.reshape(batch_size, length, head_count, HEAD)
    attn_probs = jnp.exp(attention_scores(queries, key_rows, allowed) - log_total)
    rounded_probs = attn_probs.astype(jnp.bfloat16)
    d_values = jnp.einsum('bhqk,bqhd->bkhd', as_float(rounded_probs), as_float(d_context))
    d_probs = jnp.einsum('bqhd,bkhd->bhqk', as_float(d_context), as_float(values))
    delta = lax.optimization_barrier(jnp.sum(attn_probs * d_probs, axis=-1, keepdims=True))
    d_scores = (attn_probs * (d_probs - delta) * (1.0 / math.sqrt(HEAD))).astype(jnp.bfloat16)
    d_queries = jnp.einsum('bhqk,bkhd->bqhd', as_float(d_scores), as_float(key_rows))
    d_keys = jnp.einsum('bhqk,bqhd->bkhd', as_float(d_scores), as_float(queries))
    d_proj = jnp.stack([unrotate(d_queries, cosine, sine_table), unrotate(d_keys, cosine, sine_table), d_values], axis=2).astype(jnp.bfloat16).reshape(batch_size * length, 3 * head_count * HEAD)
    g_qkv = jnp.dot(attn_in.reshape(-1, model_width).T, d_proj, preferred_element_type=jnp.float32)
    g_qkv = g_qkv.reshape(model_width, 3, head_count * HEAD)
    d_attn = jnp.dot(d_proj, w_qkv.reshape(model_width, -1).T, preferred_element_type=jnp.float32)
    d_attn = d_attn.reshape(batch_size, length, model_width)
    return ((d_attn, d_mlp), (g_qkv, g_out, g_fc1, g_fc2))

def layer_finish(cotangent, summed, stored, gains):
    dx_attn, gain_a, bias_a = norm_backward(summed[0], stored[2], stored[3], gains[0])
    dx_mlp, gain_m, bias_m = norm_backward(summed[1], stored[4], stored[5], gains[1])
    return (cotangent + dx_attn + dx_mlp, jnp.stack([gain_a, gain_m]), jnp.stack([bias_a, bias_m]))

def reference(block_input, grad_output, segment_ids, w_qkv, w_out, w_fc1, w_fc2, norm_gains, norm_biases):
    layers = [(w_qkv[layer], w_out[layer], w_fc1[layer], w_fc2[layer], norm_gains[layer], norm_biases[layer]) for layer in range(LAYERS)]
    groups = block_input.shape[0] // MICRO

    def run(totals, group_items):
        inputs, upstream, segment = group_items
        layer_outs = []
        saved_list = []
        for weights in layers:
            partial_value, stored = layer_forward(inputs, segment, weights)
            inputs = (inputs.astype(jnp.float32) + partial_value).astype(jnp.bfloat16)
            layer_outs.append(inputs)
            saved_list.append(stored)
        cotangent = upstream.astype(jnp.float32)
        d_inputs = [None] * LAYERS
        updated = list(totals)
        for layer in range(LAYERS - 1, -1, -1):
            summed, grad_terms = layer_backward(cotangent, saved_list[layer], layers[layer])
            cotangent, d_gain, d_bias = layer_finish(cotangent, summed, saved_list[layer], layers[layer][4])
            d_inputs[layer] = cotangent
            updated[layer] = tuple((left_term + right_term for left_term, right_term in zip(totals[layer], grad_terms + (d_gain, d_bias))))
        return (tuple(updated), (jnp.stack(layer_outs), jnp.stack(d_inputs)))
    zero_terms = tuple(((jnp.zeros(w_qkv.shape[1:], jnp.float32), jnp.zeros(w_out.shape[1:], jnp.float32), jnp.zeros(w_fc1.shape[1:], jnp.float32), jnp.zeros(w_fc2.shape[1:], jnp.float32), jnp.zeros(norm_gains.shape[1:], jnp.float32), jnp.zeros(norm_biases.shape[1:], jnp.float32)) for layer in range(LAYERS)))
    group_items = (block_input.reshape(groups, MICRO, LEN, -1), grad_output.reshape(groups, MICRO, LEN, -1), segment_ids.reshape(groups, MICRO, LEN))
    totals, stacked = lax.scan(run, zero_terms, group_items)
    model_width = block_input.shape[2]
    layer_outputs = jnp.moveaxis(stacked[0], 1, 0).reshape(LAYERS, -1, LEN, model_width)
    input_grads = jnp.moveaxis(stacked[1], 1, 0).reshape(LAYERS, -1, LEN, model_width)
    gathered = [jnp.stack([totals[layer][member] for layer in range(LAYERS)]) for member in range(6)]
    return (layer_outputs, input_grads, gathered[0], gathered[1], gathered[2], gathered[3], gathered[4], gathered[5])
```

```python
import math

import jax
import jax.numpy as jnp
from jax import lax
from jax.sharding import PartitionSpec as P

HEAD = 256
ROT = 64
NORM_EPSILON = 1e-05


def passed_along(value, axis, steps):
    count = lax.axis_size(axis)
    leading, last = (max(0, -steps), min(count, count - steps))
    return lax.ppermute(value, axis, [(source, source + steps) for source in range(leading, last)])


def positions_of(segment):
    earlier = (segment[:, None, :] < segment[:, :, None]).astype(jnp.int32)
    return jnp.arange(segment.shape[1], dtype=jnp.int32)[None, :] - jnp.sum(earlier, axis=2)


def rotary_tables(positions):
    frequency = jnp.exp(jnp.arange(ROT // 2, dtype=jnp.float32) * (-2.0 * math.log(10000.0) / ROT))
    angles = positions.astype(jnp.float32)[..., None] * frequency
    cosine = jnp.concatenate([jnp.cos(angles), jnp.cos(angles)], axis=-1)[:, :, None, :]
    sine_table = jnp.concatenate([jnp.sin(angles), jnp.sin(angles)], axis=-1)[:, :, None, :]
    return (cosine, sine_table)


def rotate(inputs, cosine, sine_table):
    rotated_part = inputs[..., :ROT]
    turned = jnp.concatenate(
        [-rotated_part[..., ROT // 2 :], rotated_part[..., : ROT // 2]], axis=-1
    )
    return jnp.concatenate(
        [rotated_part * cosine + turned * sine_table, inputs[..., ROT:]], axis=-1
    )


def unrotate(gradient, cosine, sine_table):
    rotated_part = gradient[..., :ROT]
    scaled = rotated_part * sine_table
    turned = jnp.concatenate([scaled[..., ROT // 2 :], -scaled[..., : ROT // 2]], axis=-1)
    return jnp.concatenate([rotated_part * cosine + turned, gradient[..., ROT:]], axis=-1)


def norm_parts(inputs):
    row_mean = jnp.mean(inputs, axis=-1, keepdims=True)
    centred = inputs - row_mean
    inv_std = lax.rsqrt(jnp.mean(centred * centred, axis=-1, keepdims=True) + NORM_EPSILON)
    return row_mean, inv_std


def gelu_parts(hidden):
    normal_cdf = 0.5 * (1.0 + lax.erf(hidden * (1.0 / math.sqrt(2.0))))
    density = jnp.exp(-0.5 * hidden * hidden) * (1.0 / math.sqrt(2.0 * math.pi))
    return (hidden * normal_cdf, normal_cdf + hidden * density)


def attention_scores(queries, key_rows, allowed):
    scores = jnp.einsum("bqhd,bkhd->bhqk", queries, key_rows, preferred_element_type=jnp.float32)
    return jnp.where(allowed[:, None], scores * (1.0 / math.sqrt(HEAD)), -jnp.inf)


def dot(left, right):
    return jnp.dot(left, right, preferred_element_type=jnp.float32)


def layer_forward(inputs, tables, weights, batch):
    w_qkv, w_out, w_fc1, w_fc2, gains, biases = weights
    cosine, sine_table, allowed = tables
    tokens, model_width = inputs.shape
    length = tokens // batch
    head_count = w_qkv.shape[2] // HEAD
    widened = inputs.astype(jnp.float32)
    row_mean, inv_std = norm_parts(widened)
    normed = (widened - row_mean) * inv_std
    attn_in = (normed * gains[0] + biases[0]).astype(jnp.bfloat16)
    mlp_in = (normed * gains[1] + biases[1]).astype(jnp.bfloat16)
    projected = dot(attn_in, w_qkv.reshape(model_width, -1))
    projected = projected.reshape(batch, length, 3, head_count, HEAD)
    queries = rotate(projected[:, :, 0], cosine, sine_table).astype(jnp.bfloat16)
    key_rows = rotate(projected[:, :, 1], cosine, sine_table).astype(jnp.bfloat16)
    values = projected[:, :, 2].astype(jnp.bfloat16)
    scores = attention_scores(queries, key_rows, allowed)
    row_max = jnp.max(scores, axis=-1, keepdims=True)
    log_total = row_max + jnp.log(jnp.sum(jnp.exp(scores - row_max), axis=-1, keepdims=True))
    attn_probs = jnp.exp(scores - log_total).astype(jnp.bfloat16)
    context = jnp.einsum("bhqk,bkhd->bqhd", attn_probs, values, preferred_element_type=jnp.float32)
    context = context.astype(jnp.bfloat16).reshape(tokens, head_count * HEAD)
    hidden = dot(mlp_in, w_fc1)
    activated, gelu_slope = gelu_parts(hidden)
    activated = activated.astype(jnp.bfloat16)
    partial_value = dot(context, w_out) + dot(activated, w_fc2)
    stored = (row_mean, inv_std, queries, key_rows, values, log_total, context, gelu_slope, activated)
    return partial_value, stored


def layer_backward(grad_b, inputs, stored, tables, weights, batch):
    w_qkv, w_out, w_fc1, w_fc2, gains, biases = weights
    cosine, sine_table, allowed = tables
    row_mean, inv_std, queries, key_rows, values, log_total, context, gelu_slope, activated = stored
    tokens, model_width = grad_b.shape
    length = tokens // batch
    head_count = queries.shape[2]
    d_act = dot(grad_b, w_fc2.T)
    d_hidden = (d_act * gelu_slope).astype(jnp.bfloat16)
    d_mlp = dot(d_hidden, w_fc1.T)
    d_context = dot(grad_b, w_out.T).astype(jnp.bfloat16)
    d_context = d_context.reshape(batch, length, head_count, HEAD)
    attn_probs = jnp.exp(attention_scores(queries, key_rows, allowed) - log_total)
    rounded_probs = attn_probs.astype(jnp.bfloat16)
    d_values = jnp.einsum(
        "bhqk,bqhd->bkhd", rounded_probs, d_context, preferred_element_type=jnp.float32
    )
    d_probs = jnp.einsum("bqhd,bkhd->bhqk", d_context, values, preferred_element_type=jnp.float32)
    delta = jnp.sum(attn_probs * d_probs, axis=-1, keepdims=True)
    d_scores = (attn_probs * (d_probs - delta) * (1.0 / math.sqrt(HEAD))).astype(jnp.bfloat16)
    d_queries = jnp.einsum(
        "bhqk,bkhd->bqhd", d_scores, key_rows, preferred_element_type=jnp.float32
    )
    d_keys = jnp.einsum("bhqk,bqhd->bkhd", d_scores, queries, preferred_element_type=jnp.float32)
    d_proj = (
        jnp.stack(
            [
                unrotate(d_queries, cosine, sine_table),
                unrotate(d_keys, cosine, sine_table),
                d_values,
            ],
            axis=2,
        )
        .astype(jnp.bfloat16)
        .reshape(tokens, 3 * head_count * HEAD)
    )
    d_attn = dot(d_proj, w_qkv.reshape(model_width, -1).T)
    normed = (inputs.astype(jnp.float32) - row_mean) * inv_std
    e_terms = d_attn * gains[0] + d_mlp * gains[1]
    vectors = jnp.stack(
        [
            jnp.sum(d_attn * normed, axis=0),
            jnp.sum(d_mlp * normed, axis=0),
            jnp.sum(d_attn, axis=0),
            jnp.sum(d_mlp, axis=0),
        ]
    )
    return e_terms, vectors, d_hidden, d_proj


def norm_backward(e_sum, inputs, row_mean, inv_std):
    normed = (inputs.astype(jnp.float32) - row_mean) * inv_std
    return inv_std * (
        e_sum
        - jnp.mean(e_sum, axis=-1, keepdims=True)
        - normed * jnp.mean(e_sum * normed, axis=-1, keepdims=True)
    )


def shards(
    block_input, grad_output, segment_ids, w_qkv, w_out, w_fc1, w_fc2, norm_gains, norm_biases
):
    first_section = lax.axis_index("section") == 0
    batch, length, width = block_input.shape
    tokens = batch * length
    dp_count = lax.axis_size("dp")
    weights = (w_qkv[0], w_out[0], w_fc1[0], w_fc2[0], norm_gains[0], norm_biases[0])
    cosine, sine_table = rotary_tables(positions_of(segment_ids))
    order = jnp.arange(length, dtype=jnp.int32)
    allowed = (segment_ids[:, :, None] == segment_ids[:, None, :]) & (
        order[None, :, None] >= order[None, None, :]
    )
    tables = (cosine, sine_table, allowed)
    own_input = block_input.reshape(tokens, width)
    own_grad = grad_output.reshape(tokens, width)

    def forward(inputs):
        partial_value, stored = layer_forward(inputs, tables, weights, batch)
        branch_sum = lax.psum(partial_value.astype(jnp.bfloat16), "tensor").astype(jnp.float32)
        return (inputs.astype(jnp.float32) + branch_sum).astype(jnp.bfloat16), stored

    first_out, _ = forward(own_input)
    received = passed_along(first_out, "section", 1)
    inputs = jnp.where(first_section, own_input, received)
    layer_out, stored = forward(inputs)
    row_mean, inv_std = stored[:2]
    context, activated = stored[6], stored[8]

    def backward(cotangent):
        grad_b = cotangent.astype(jnp.bfloat16)
        e_terms, vectors, d_hidden, d_proj = layer_backward(
            grad_b, inputs, stored, tables, weights, batch
        )
        e_sum = lax.psum(e_terms.astype(jnp.bfloat16), "tensor").astype(jnp.float32)
        d_inputs = cotangent.astype(jnp.float32) + norm_backward(e_sum, inputs, row_mean, inv_std)
        return d_inputs, vectors, d_hidden, d_proj

    last_grad = backward(own_grad)[0]
    from_next = passed_along(last_grad.astype(jnp.bfloat16), "section", -1)
    grad_b = jnp.where(first_section, from_next, own_grad)
    input_grads, vectors, d_hidden, d_proj = backward(grad_b)

    def gathered(value):
        return lax.all_gather(value, "dp", axis=0, tiled=True)

    def sliced(value):
        return lax.all_to_all(value, "dp", split_axis=1, concat_axis=0, tiled=True)

    mine = width // dp_count
    start = lax.axis_index("dp") * mine
    gains = lax.dynamic_slice_in_dim(norm_gains[0], start, mine, 1)
    biases = lax.dynamic_slice_in_dim(norm_biases[0], start, mine, 1)
    rows = gathered(jnp.concatenate([row_mean, inv_std], axis=1))
    normed = (sliced(inputs).astype(jnp.float32) - rows[:, :1]) * rows[:, 1:]
    attn_in = (normed * gains[0] + biases[0]).astype(jnp.bfloat16)
    mlp_in = (normed * gains[1] + biases[1]).astype(jnp.bfloat16)
    grads_mine = sliced(grad_b)
    g_fc2 = dot(gathered(activated).T, grads_mine)
    g_out = dot(gathered(context).T, grads_mine)
    g_fc1 = dot(mlp_in.T, gathered(d_hidden))
    g_qkv = dot(attn_in.T, gathered(d_proj)).reshape(mine, 3, -1)
    summed = lax.psum(lax.psum_scatter(vectors, "dp", scatter_dimension=1, tiled=True), "tensor")
    shape = (1, batch, length, width)
    return (
        layer_out.reshape(shape),
        input_grads.reshape(shape),
        g_qkv[None],
        g_out[None],
        g_fc1[None],
        g_fc2[None],
        summed[None, :2],
        summed[None, 2:],
    )


def solution(mesh):
    return jax.shard_map(
        shards,
        mesh=mesh,
        in_specs=(
            P("dp", None, None),
            P("dp", None, None),
            P("dp", None),
            P("section", None, None, "tensor"),
            P("section", "tensor", None),
            P("section", None, "tensor"),
            P("section", "tensor", None),
            P("section", None, None),
            P("section", None, None),
        ),
        out_specs=(
            P("section", "dp", None, None),
            P("section", "dp", None, None),
            P("section", "dp", None, "tensor"),
            P("section", "tensor", "dp"),
            P("section", "dp", "tensor"),
            P("section", "tensor", "dp"),
            P("section", None, "dp"),
            P("section", None, "dp"),
        ),
        check_vma=False,
    )
```

```python
import functools
import math

import jax
import jax.numpy as jnp
from jax import lax
from jax.experimental import pallas as pl
from jax.experimental.pallas import tpu as pltpu
from jax.sharding import PartitionSpec as P

MESH = pl.DeviceIdType.MESH

HEAD = 256
ROT = 64
NORM_EPSILON = 1e-05


def passed_along(value, axis, steps):
    count = lax.axis_size(axis)
    leading, last = (max(0, -steps), min(count, count - steps))
    return lax.ppermute(value, axis, [(source, source + steps) for source in range(leading, last)])


def positions_of(segment):
    earlier = (segment[:, None, :] < segment[:, :, None]).astype(jnp.int32)
    return jnp.arange(segment.shape[1], dtype=jnp.int32)[None, :] - jnp.sum(earlier, axis=2)


def rotary_tables(positions):
    frequency = jnp.exp(jnp.arange(ROT // 2, dtype=jnp.float32) * (-2.0 * math.log(10000.0) / ROT))
    angles = positions.astype(jnp.float32)[..., None] * frequency
    cosine = jnp.concatenate([jnp.cos(angles), jnp.cos(angles)], axis=-1)[:, :, None, :]
    sine_table = jnp.concatenate([jnp.sin(angles), jnp.sin(angles)], axis=-1)[:, :, None, :]
    return (cosine, sine_table)


def rotate(inputs, cosine, sine_table):
    rotated_part = inputs[..., :ROT]
    turned = jnp.concatenate(
        [-rotated_part[..., ROT // 2 :], rotated_part[..., : ROT // 2]], axis=-1
    )
    return jnp.concatenate(
        [rotated_part * cosine + turned * sine_table, inputs[..., ROT:]], axis=-1
    )


def unrotate(gradient, cosine, sine_table):
    rotated_part = gradient[..., :ROT]
    scaled = rotated_part * sine_table
    turned = jnp.concatenate([scaled[..., ROT // 2 :], -scaled[..., : ROT // 2]], axis=-1)
    return jnp.concatenate([rotated_part * cosine + turned, gradient[..., ROT:]], axis=-1)


def partner(index, step, count):
    if count & (count - 1):
        return lax.rem(index + step, count), lax.rem(index + count - step, count)
    bit = 1
    while bit < count:
        if step & bit:
            index = index + bit - 2 * bit * ((index // bit) % 2)
        bit *= 2
    return index, index


def reduce_kernel(source, count, has_extra, *refs):
    if has_extra:
        term, extra, out, arrived, parts, send, recv, send_part, recv_part, send_back, recv_back = refs
    else:
        term, out, arrived, parts, send, recv, send_part, recv_part, send_back, recv_back = refs
    section, me = lax.axis_index("section"), lax.axis_index("tensor")
    width = term.shape[2]

    def at(section, index):
        return {"section": section, "tensor": index}

    barrier = pltpu.get_barrier_semaphore()
    for step in range(count):
        peer = partner(me, step, count)[0]
        pl.semaphore_signal(barrier, inc=1, device_id=at(1 - section, peer), device_id_type=MESH)
        if step:
            pl.semaphore_signal(barrier, inc=1, device_id=at(section, peer), device_id_type=MESH)
    pl.semaphore_wait(barrier, 2 * count - 1)

    def scatter(step):
        peer = partner(me, step, count)[0]
        return pltpu.make_async_remote_copy(
            src_ref=term.at[peer],
            dst_ref=arrived.at[step],
            send_sem=send.at[step],
            recv_sem=recv.at[step],
            device_id=at(section, peer),
            device_id_type=MESH,
        )

    def gather(step):
        peer = partner(me, step, count)[0]
        return pltpu.make_async_remote_copy(
            src_ref=parts.at[0],
            dst_ref=parts.at[step],
            send_sem=send_part.at[step],
            recv_sem=recv_part.at[step],
            device_id=at(1 - section, peer),
            device_id_type=MESH,
        )

    def back(step):
        return pltpu.make_async_remote_copy(
            src_ref=parts.at[step],
            dst_ref=parts.at[step],
            send_sem=send_back.at[step],
            recv_sem=recv_back.at[step],
            device_id=at(1 - section, me),
            device_id_type=MESH,
        )

    def place(step):
        owner = partner(me, step, count)[1]
        columns = pl.ds(pl.multiple_of(owner * width, width), width)
        out[:, columns] = parts[step]

    order = list(range(count - 1, 0, -1))

    @pl.when(section == source)
    def _():
        for step in order:
            scatter(step).start()
        total = term[me].astype(jnp.float32)
        if has_extra:
            total = total + extra[...].astype(jnp.float32)
        for step in order[::-1]:
            scatter(step).wait_recv()
            total = total + arrived[step].astype(jnp.float32)
        parts[0] = total.astype(parts.dtype)
        for step in order + [0]:
            gather(step).start()
        place(0)
        for step in order[::-1]:
            back(step).wait_recv()
            place(step)
        for step in order:
            scatter(step).wait_send()
            gather(step).wait_send()
        gather(0).wait_send()

    @pl.when(section != source)
    def _():
        gather(0).wait_recv()
        place(0)
        for step in order[::-1]:
            gather(step).wait_recv()
            back(step).start()
            place(step)
        for step in order:
            back(step).wait_send()


def reduced(term, extra, source, collective_id):
    count = lax.axis_size("tensor")
    tokens, width = term.shape
    part = width // count
    chunks = jnp.transpose(term.reshape(tokens, count, part), (1, 0, 2))
    operands = [chunks]
    if extra is not None:
        start = lax.axis_index("tensor") * part
        operands.append(lax.dynamic_slice_in_dim(extra, start, part, 1))
    return pl.pallas_call(
        functools.partial(reduce_kernel, source, count, extra is not None),
        out_shape=jax.ShapeDtypeStruct((tokens, width), jnp.bfloat16),
        in_specs=[pl.BlockSpec(memory_space=pltpu.VMEM)] * len(operands),
        out_specs=pl.BlockSpec(memory_space=pltpu.VMEM),
        scratch_shapes=[
            pltpu.VMEM((count, tokens, part), jnp.bfloat16),
            pltpu.VMEM((count, tokens, part), jnp.bfloat16),
        ]
        + [pltpu.SemaphoreType.DMA((count,))] * 6,
        compiler_params=pltpu.CompilerParams(collective_id=collective_id, has_side_effects=True),
        name=f"reduce{collective_id}",
    )(*operands)


def norm_parts(inputs):
    row_mean = jnp.mean(inputs, axis=-1, keepdims=True)
    centred = inputs - row_mean
    inv_std = lax.rsqrt(jnp.mean(centred * centred, axis=-1, keepdims=True) + NORM_EPSILON)
    return row_mean, inv_std


def gelu_parts(hidden):
    normal_cdf = 0.5 * (1.0 + lax.erf(hidden * (1.0 / math.sqrt(2.0))))
    density = jnp.exp(-0.5 * hidden * hidden) * (1.0 / math.sqrt(2.0 * math.pi))
    return (hidden * normal_cdf, normal_cdf + hidden * density)


def attention_scores(queries, key_rows, allowed):
    scores = jnp.einsum("bqhd,bkhd->bhqk", queries, key_rows, preferred_element_type=jnp.float32)
    return jnp.where(allowed[:, None], scores * (1.0 / math.sqrt(HEAD)), -jnp.inf)


def dot(left, right):
    return jnp.dot(left, right, preferred_element_type=jnp.float32)


def layer_forward(inputs, tables, weights, batch):
    w_qkv, w_out, w_fc1, w_fc2, gains, biases = weights
    cosine, sine_table, allowed = tables
    tokens, model_width = inputs.shape
    length = tokens // batch
    head_count = w_qkv.shape[2] // HEAD
    widened = inputs.astype(jnp.float32)
    row_mean, inv_std = norm_parts(widened)
    normed = (widened - row_mean) * inv_std
    attn_in = (normed * gains[0] + biases[0]).astype(jnp.bfloat16)
    mlp_in = (normed * gains[1] + biases[1]).astype(jnp.bfloat16)
    projected = dot(attn_in, w_qkv.reshape(model_width, -1))
    projected = projected.reshape(batch, length, 3, head_count, HEAD)
    queries = rotate(projected[:, :, 0], cosine, sine_table).astype(jnp.bfloat16)
    key_rows = rotate(projected[:, :, 1], cosine, sine_table).astype(jnp.bfloat16)
    values = projected[:, :, 2].astype(jnp.bfloat16)
    scores = attention_scores(queries, key_rows, allowed)
    row_max = jnp.max(scores, axis=-1, keepdims=True)
    log_total = row_max + jnp.log(jnp.sum(jnp.exp(scores - row_max), axis=-1, keepdims=True))
    attn_probs = jnp.exp(scores - log_total).astype(jnp.bfloat16)
    context = jnp.einsum("bhqk,bkhd->bqhd", attn_probs, values, preferred_element_type=jnp.float32)
    context = context.astype(jnp.bfloat16).reshape(tokens, head_count * HEAD)
    hidden = dot(mlp_in, w_fc1)
    activated, gelu_slope = gelu_parts(hidden)
    activated = activated.astype(jnp.bfloat16)
    partial_value = dot(context, w_out) + dot(activated, w_fc2)
    stored = (row_mean, inv_std, queries, key_rows, values, log_total, context, gelu_slope, activated)
    return partial_value, stored


def layer_backward(grad_b, inputs, stored, tables, weights, batch):
    w_qkv, w_out, w_fc1, w_fc2, gains, biases = weights
    cosine, sine_table, allowed = tables
    row_mean, inv_std, queries, key_rows, values, log_total, context, gelu_slope, activated = stored
    tokens, model_width = grad_b.shape
    length = tokens // batch
    head_count = queries.shape[2]
    d_act = dot(grad_b, w_fc2.T)
    d_hidden = (d_act * gelu_slope).astype(jnp.bfloat16)
    d_mlp = dot(d_hidden, w_fc1.T)
    d_context = dot(grad_b, w_out.T).astype(jnp.bfloat16)
    d_context = d_context.reshape(batch, length, head_count, HEAD)
    attn_probs = jnp.exp(attention_scores(queries, key_rows, allowed) - log_total)
    rounded_probs = attn_probs.astype(jnp.bfloat16)
    d_values = jnp.einsum(
        "bhqk,bqhd->bkhd", rounded_probs, d_context, preferred_element_type=jnp.float32
    )
    d_probs = jnp.einsum("bqhd,bkhd->bhqk", d_context, values, preferred_element_type=jnp.float32)
    delta = jnp.sum(attn_probs * d_probs, axis=-1, keepdims=True)
    d_scores = (attn_probs * (d_probs - delta) * (1.0 / math.sqrt(HEAD))).astype(jnp.bfloat16)
    d_queries = jnp.einsum(
        "bhqk,bkhd->bqhd", d_scores, key_rows, preferred_element_type=jnp.float32
    )
    d_keys = jnp.einsum("bhqk,bqhd->bkhd", d_scores, queries, preferred_element_type=jnp.float32)
    d_proj = (
        jnp.stack(
            [
                unrotate(d_queries, cosine, sine_table),
                unrotate(d_keys, cosine, sine_table),
                d_values,
            ],
            axis=2,
        )
        .astype(jnp.bfloat16)
        .reshape(tokens, 3 * head_count * HEAD)
    )
    d_attn = dot(d_proj, w_qkv.reshape(model_width, -1).T)
    normed = (inputs.astype(jnp.float32) - row_mean) * inv_std
    e_terms = d_attn * gains[0] + d_mlp * gains[1]
    vectors = jnp.stack(
        [
            jnp.sum(d_attn * normed, axis=0),
            jnp.sum(d_mlp * normed, axis=0),
            jnp.sum(d_attn, axis=0),
            jnp.sum(d_mlp, axis=0),
        ]
    )
    return e_terms, vectors, d_hidden, d_proj


def norm_backward(e_sum, inputs, row_mean, inv_std):
    normed = (inputs.astype(jnp.float32) - row_mean) * inv_std
    return inv_std * (
        e_sum
        - jnp.mean(e_sum, axis=-1, keepdims=True)
        - normed * jnp.mean(e_sum * normed, axis=-1, keepdims=True)
    )


def shards(
    block_input, grad_output, segment_ids, w_qkv, w_out, w_fc1, w_fc2, norm_gains, norm_biases
):
    first_section = lax.axis_index("section") == 0
    batch, length, width = block_input.shape
    tokens = batch * length
    dp_count = lax.axis_size("dp")
    weights = (w_qkv[0], w_out[0], w_fc1[0], w_fc2[0], norm_gains[0], norm_biases[0])
    cosine, sine_table = rotary_tables(positions_of(segment_ids))
    order = jnp.arange(length, dtype=jnp.int32)
    allowed = (segment_ids[:, :, None] == segment_ids[:, None, :]) & (
        order[None, :, None] >= order[None, None, :]
    )
    tables = (cosine, sine_table, allowed)
    own_input = block_input.reshape(tokens, width)
    own_grad = grad_output.reshape(tokens, width)

    partial_value, _ = layer_forward(own_input, tables, weights, batch)
    first_out = reduced(partial_value.astype(jnp.bfloat16), own_input, 0, 0)
    inputs = jnp.where(first_section, own_input, first_out)
    partial_value, stored = layer_forward(inputs, tables, weights, batch)
    second_out = reduced(partial_value.astype(jnp.bfloat16), inputs, 1, 1)
    layer_out = jnp.where(first_section, first_out, second_out)
    row_mean, inv_std = stored[:2]
    context, activated = stored[6], stored[8]

    def backward(cotangent, source):
        grad_b = cotangent.astype(jnp.bfloat16)
        e_terms, vectors, d_hidden, d_proj = layer_backward(
            grad_b, inputs, stored, tables, weights, batch
        )
        e_sum = reduced(e_terms.astype(jnp.bfloat16), None, source, 3 - source).astype(jnp.float32)
        d_inputs = cotangent.astype(jnp.float32) + norm_backward(e_sum, inputs, row_mean, inv_std)
        return d_inputs, vectors, d_hidden, d_proj

    last_grad = backward(own_grad, 1)[0]
    from_next = passed_along(last_grad.astype(jnp.bfloat16), "section", -1)
    grad_b = jnp.where(first_section, from_next, own_grad)
    first_grad, vectors, d_hidden, d_proj = backward(grad_b, 0)
    input_grads = jnp.where(first_section, first_grad, last_grad)

    def gathered(value):
        return lax.all_gather(value, "dp", axis=0, tiled=True)

    def sliced(value):
        return lax.all_to_all(value, "dp", split_axis=1, concat_axis=0, tiled=True)

    mine = width // dp_count
    start = lax.axis_index("dp") * mine
    gains = lax.dynamic_slice_in_dim(norm_gains[0], start, mine, 1)
    biases = lax.dynamic_slice_in_dim(norm_biases[0], start, mine, 1)
    rows = gathered(jnp.concatenate([row_mean, inv_std], axis=1))
    normed = (sliced(inputs).astype(jnp.float32) - rows[:, :1]) * rows[:, 1:]
    attn_in = (normed * gains[0] + biases[0]).astype(jnp.bfloat16)
    mlp_in = (normed * gains[1] + biases[1]).astype(jnp.bfloat16)
    grads_mine = sliced(grad_b)
    g_fc2 = dot(gathered(activated).T, grads_mine)
    g_out = dot(gathered(context).T, grads_mine)
    g_fc1 = dot(mlp_in.T, gathered(d_hidden))
    g_qkv = dot(attn_in.T, gathered(d_proj)).reshape(mine, 3, -1)
    summed = lax.psum(lax.psum_scatter(vectors, "dp", scatter_dimension=1, tiled=True), "tensor")
    shape = (1, batch, length, width)
    return (
        layer_out.reshape(shape),
        input_grads.reshape(shape),
        g_qkv[None],
        g_out[None],
        g_fc1[None],
        g_fc2[None],
        summed[None, :2],
        summed[None, 2:],
    )


def solution(mesh):
    return jax.shard_map(
        shards,
        mesh=mesh,
        in_specs=(
            P("dp", None, None),
            P("dp", None, None),
            P("dp", None),
            P("section", None, None, "tensor"),
            P("section", "tensor", None),
            P("section", None, "tensor"),
            P("section", "tensor", None),
            P("section", None, None),
            P("section", None, None),
        ),
        out_specs=(
            P("section", "dp", None, None),
            P("section", "dp", None, None),
            P("section", "dp", None, "tensor"),
            P("section", "tensor", "dp"),
            P("section", "dp", "tensor"),
            P("section", "tensor", "dp"),
            P("section", None, "dp"),
            P("section", None, "dp"),
        ),
        check_vma=False,
    )
```

```python
import functools
import math

import jax
import jax.numpy as jnp
from jax import lax
from jax.experimental import pallas as pl
from jax.experimental.pallas import tpu as pltpu
from jax.sharding import PartitionSpec as P

HEAD = 256
ROT = 64
LANES = 128
TILE = 256
NORM_EPSILON = 1e-05
MESH = pl.DeviceIdType.MESH
BF16 = jnp.bfloat16
F32 = jnp.float32


def partner(index, step, count):
    if count & (count - 1):
        return lax.rem(index + step, count), lax.rem(index + count - step, count)
    bit = 1
    while bit < count:
        index = index + ((step // bit) % 2) * (bit - 2 * bit * ((index // bit) % 2))
        bit *= 2
    return index, index


def loop(count, body, unroll=1):
    lax.fori_loop(0, count, lambda i, carry: (body(i), carry)[1], 0, unroll=unroll)


def tile_of(i, size):
    return pl.ds(pl.multiple_of(i * size, size), size)


def dot(left, right):
    return jnp.dot(left, right, preferred_element_type=jnp.float32)


def dot_nt(left, right):
    return lax.dot_general(left, right, (((1,), (1,)), ((), ())), preferred_element_type=jnp.float32)


def dot_tn(left, right):
    return lax.dot_general(left, right, (((0,), (0,)), ((), ())), preferred_element_type=jnp.float32)


def gelu_parts(hidden):
    normal_cdf = 0.5 * (1.0 + lax.erf(hidden * (1.0 / math.sqrt(2.0))))
    density = jnp.exp(-0.5 * hidden * hidden) * (1.0 / math.sqrt(2.0 * math.pi))
    return (hidden * normal_cdf, normal_cdf + hidden * density)


def lanes_of(shape):
    return lax.broadcasted_iota(jnp.int32, shape, len(shape) - 1)


def rotated(tile, cosine, sine):
    half = ROT // 2
    left, right = pltpu.roll(tile, LANES - half, 1), pltpu.roll(tile, half, 1)
    lane = lanes_of(tile.shape)
    turned = jnp.where(lane < half, -left, right)
    return tile * cosine + turned * sine


def unrotated(tile, cosine, sine):
    half = ROT // 2
    scaled = tile * sine
    left, right = pltpu.roll(scaled, LANES - half, 1), pltpu.roll(scaled, half, 1)
    lane = lanes_of(tile.shape)
    turned = jnp.where(lane < half, left, jnp.where(lane < ROT, -right, 0.0))
    return tile * cosine + turned


def row_norm(values):
    mean = jnp.mean(values, axis=-1, keepdims=True)
    centred = values - mean
    inv_std = lax.rsqrt(jnp.mean(centred * centred, axis=-1, keepdims=True) + NORM_EPSILON)
    return centred * inv_std, mean, inv_std


def row_norm_backward(summed, normed, inv_std):
    return inv_std * (
        summed
        - jnp.mean(summed, axis=-1, keepdims=True)
        - normed * jnp.mean(summed * normed, axis=-1, keepdims=True)
    )


def chain_kernel(count, batch, *refs):
    (
        x_hbm, go_hbm, seg_col, seg_row, w3_hbm, wo_hbm, w1_hbm, w2_hbm, gains, biases,
        layer_out, input_grad, vectors, x_out, act_out, context_out, dh_out, dproj_out, gb_out,
        w3, wo, w1, w2, xv, other, gbv, attn_in, mlp_in, qkv, context, probs, act, slope, dh, dctx,
        dproj, means, inv_stds, tables, term, arrived, parts, full,
        load, store, send, recv, part_send, part_recv, back_send, back_recv,
    ) = refs
    section, me = lax.axis_index("section"), lax.axis_index("tensor")
    tokens, width = xv.shape
    length = tokens // batch
    heads = qkv.shape[2] // HEAD
    hidden_width = act.shape[1]
    part = width // count
    row_tile = 32 if tokens % 32 == 0 else 16
    row_tiles = tokens // row_tile
    scale = 1.0 / math.sqrt(HEAD)

    qkv_loads = [pltpu.make_async_copy(w3_hbm.at[k], w3.at[k], load.at[k]) for k in range(3)]
    blocks = 4
    block = hidden_width // blocks

    def fc1_load(i):
        columns = tile_of(i, block)
        return pltpu.make_async_copy(w1_hbm.at[:, columns], w1.at[:, columns], load.at[3 + i])

    out_load = pltpu.make_async_copy(wo_hbm, wo, load.at[7])
    fc2_load = pltpu.make_async_copy(w2_hbm, w2, load.at[8])
    x_load = pltpu.make_async_copy(x_hbm, xv, load.at[9])
    go_load = pltpu.make_async_copy(go_hbm, gbv, load.at[10])

    @pl.when(section == 0)
    def _():
        x_load.start()

    for copy in qkv_loads:
        copy.start()
    for i in range(blocks):
        fc1_load(i).start()
    out_load.start()
    fc2_load.start()
    go_load.start()

    def at(section, index):
        return {"section": section, "tensor": index}

    barrier = pltpu.get_barrier_semaphore()
    for step in range(count):
        peer = partner(me, step, count)[0]
        pl.semaphore_signal(barrier, inc=1, device_id=at(1 - section, peer), device_id_type=MESH)
        if step:
            pl.semaphore_signal(barrier, inc=1, device_id=at(section, peer), device_id_type=MESH)

    def scatter(kind, step):
        peer = partner(me, step, count)[0]
        return pltpu.make_async_remote_copy(
            src_ref=term.at[peer],
            dst_ref=arrived.at[kind, step],
            send_sem=send.at[kind, step],
            recv_sem=recv.at[kind, step],
            device_id=at(section, peer),
            device_id_type=MESH,
        )

    def gather(number, step, target):
        peer = partner(me, step, count)[0]
        return pltpu.make_async_remote_copy(
            src_ref=parts.at[number, 0],
            dst_ref=parts.at[number, step],
            send_sem=part_send.at[number, step],
            recv_sem=part_recv.at[number, step],
            device_id=at(target, peer),
            device_id_type=MESH,
        )

    def back(number, step):
        return pltpu.make_async_remote_copy(
            src_ref=parts.at[number, step],
            dst_ref=parts.at[number, step],
            send_sem=back_send.at[number, step],
            recv_sem=back_recv.at[number, step],
            device_id=at(1 - section, me),
            device_id_type=MESH,
        )

    steps = list(range(1, count))

    def place(number, step, target):
        owner = partner(me, step, count)[1]
        target[:, tile_of(owner, part)] = parts[number, step]

    def reduce(kind, number, with_input):
        for step in steps:
            scatter(kind, step).wait_recv()

        def rows_of(i):
            rows = tile_of(i, row_tile)
            total = term[me, rows, :].astype(F32)
            if with_input:
                total = total + xv[rows, tile_of(me, part)].astype(F32)
            for step in steps:
                total = total + arrived[kind, step, rows, :].astype(F32)
            parts[number, 0, rows, :] = total.astype(BF16)

        loop(row_tiles, rows_of)

    def finish_sends(kind):
        for step in steps:
            scatter(kind, step).wait_send()

    def to_other_section(number):
        for step in steps[::-1] + [0]:
            gather(number, step, 1 - section).start()

    def from_own_section(number, target):
        place(number, 0, target)
        for step in steps:
            back(number, step).wait_recv()
            place(number, step, target)
        for step in [0] + steps:
            gather(number, step, 1 - section).wait_send()

    def from_other_section(number, target):
        gather(number, 0, 1 - section).wait_recv()
        place(number, 0, target)
        for step in steps:
            gather(number, step, 1 - section).wait_recv()
            back(number, step).start()
            place(number, step, target)

    def finish_back(number):
        for step in steps:
            back(number, step).wait_send()

    def within_section(number, target):
        for step in steps[::-1]:
            gather(number, step, section).start()
        place(number, 0, target)
        for step in steps:
            gather(number, step, section).wait_recv()
            place(number, step, target)
        for step in steps:
            gather(number, step, section).wait_send()

    def each_chunk(kind, compute):
        def chunk(i):
            step = count - 1 - i
            owner = partner(me, step, count)[0]
            loop(part // TILE, lambda j: compute(owner, j))

            @pl.when(step > 0)
            def _():
                scatter(kind, step).start()

        loop(count, chunk)

    lane = lanes_of((1, LANES)).astype(F32)
    exponent = jnp.where(lane < ROT // 2, lane, lane - ROT // 2)
    frequency = jnp.exp(exponent * (-2.0 * math.log(10000.0) / ROT))
    for b in range(batch):
        rows = pl.ds(b * length, length)
        earlier = (seg_row[b : b + 1, :] < seg_col[rows, :]).astype(F32)
        number_of = jnp.sum(earlier, axis=1, keepdims=True)
        index = lax.broadcasted_iota(jnp.int32, (length, 1), 0).astype(F32)
        angles = (index - number_of) * frequency
        inside = lanes_of((length, LANES)) < ROT
        tables[rows, :LANES] = jnp.where(inside, jnp.cos(angles), 1.0)
        tables[rows, LANES:] = jnp.where(inside, jnp.sin(angles), 0.0)

    def allowed_of(b):
        row = lax.broadcasted_iota(jnp.int32, (length, length), 0)
        column = lax.broadcasted_iota(jnp.int32, (length, length), 1)
        same = seg_row[b : b + 1, :] == seg_col[pl.ds(b * length, length), :]
        return same & (column <= row)

    pl.semaphore_wait(barrier, 2 * count - 1)

    @pl.when(section == 0)
    def _():
        x_load.wait()

    @pl.when(section == 1)
    def _():
        from_other_section(0, xv)

    def norm_rows(i):
        rows = tile_of(i, row_tile)
        normed, mean, inv_std = row_norm(xv[rows, :].astype(F32))
        means[rows, :] = mean
        inv_stds[rows, :] = inv_std
        attn_in[rows, :] = (normed * gains[0:1, :] + biases[0:1, :]).astype(BF16)
        mlp_in[rows, :] = (normed * gains[1:2, :] + biases[1:2, :]).astype(BF16)

    loop(row_tiles, norm_rows)

    def rotary_head(i):
        which, h = i // heads, lax.rem(i, heads)
        tile = dot(attn_in[...], w3[which, :, tile_of(h, HEAD)])
        first = rotated(tile[:, :LANES], tables[:, :LANES], tables[:, LANES:])
        qkv[which, :, pl.ds(pl.multiple_of(h * HEAD, HEAD), LANES)] = first.astype(BF16)
        qkv[which, :, pl.ds(pl.multiple_of(h * HEAD + LANES, LANES), HEAD - LANES)] = tile[
            :, LANES:
        ].astype(BF16)

    def value_head(h):
        qkv[2, :, tile_of(h, HEAD)] = dot(attn_in[...], w3[2, :, tile_of(h, HEAD)]).astype(BF16)

    qkv_loads[0].wait()
    qkv_loads[1].wait()
    loop(2 * heads, rotary_head)
    qkv_loads[2].wait()
    loop(heads, value_head)

    for b in range(batch):
        rows = pl.ds(b * length, length)
        allowed = allowed_of(b)
        for h in range(heads):
            columns = pl.ds(h * HEAD, HEAD)
            scores = dot_nt(qkv[0, rows, columns], qkv[1, rows, columns]) * scale
            scores = jnp.where(allowed, scores, -jnp.inf)
            row_max = jnp.max(scores, axis=-1, keepdims=True)
            total = jnp.sum(jnp.exp(scores - row_max), axis=-1, keepdims=True)
            prob = jnp.exp(scores - (row_max + jnp.log(total)))
            probs[b * heads + h] = prob
            context[rows, columns] = dot(prob.astype(BF16), qkv[2, rows, columns]).astype(BF16)

    def fc1_block(i):
        fc1_load(i).wait()

        def fc1_tile(j):
            columns = tile_of(i * (block // TILE) + j, TILE)
            value, derivative = gelu_parts(dot(mlp_in[...], w1[:, columns]))
            act[:, columns] = value.astype(BF16)
            slope[:, columns] = derivative

        loop(block // TILE, fc1_tile)

    loop(blocks, fc1_block)
    out_load.wait()
    fc2_load.wait()

    def out_tile(owner, j):
        columns = tile_of(owner * (part // TILE) + j, TILE)
        total = dot(context[...], wo[:, columns]) + dot(act[...], w2[:, columns])
        term[owner, :, tile_of(j, TILE)] = total.astype(BF16)

    go_load.wait()

    @pl.when(section == 0)
    def _():
        each_chunk(0, out_tile)
        reduce(0, 0, True)
        to_other_section(0)
        finish_sends(0)
        from_own_section(0, other)
        from_other_section(1, full)

        def gradient_rows(i):
            rows = tile_of(i, row_tile)
            normed, _, inv_std = row_norm(other[rows, :].astype(F32))
            dx = row_norm_backward(full[rows, :].astype(F32), normed, inv_std)
            gbv[rows, :] = (gbv[rows, :].astype(F32) + dx).astype(BF16)

        loop(row_tiles, gradient_rows)
        finish_back(1)

    def d_hidden_tile(i):
        columns = tile_of(i, TILE)
        d_act = dot_nt(gbv[...], w2[columns, :])
        dh[:, columns] = (d_act * slope[:, columns]).astype(BF16)

    loop(hidden_width // TILE, d_hidden_tile)

    def d_context_head(h):
        dctx[:, tile_of(h, HEAD)] = dot_nt(gbv[...], wo[tile_of(h, HEAD), :]).astype(BF16)

    loop(heads, d_context_head)

    for b in range(batch):
        rows = pl.ds(b * length, length)
        cosine, sine = tables[rows, :LANES], tables[rows, LANES:]
        for h in range(heads):
            columns = pl.ds(h * HEAD, HEAD)
            queries, keys, values = (qkv[k, rows, columns] for k in range(3))
            d_context = dctx[rows, columns]
            prob = probs[b * heads + h]
            d_values = dot_tn(prob.astype(BF16), d_context)
            d_probs = dot_nt(d_context, values)
            delta = jnp.sum(prob * d_probs, axis=-1, keepdims=True)
            d_scores = (prob * (d_probs - delta) * scale).astype(BF16)
            for k, gradient in ((0, dot(d_scores, keys)), (1, dot_tn(d_scores, queries))):
                first = unrotated(gradient[:, :LANES], cosine, sine)
                dproj[k, rows, pl.ds(h * HEAD, LANES)] = first.astype(BF16)
                dproj[k, rows, pl.ds(h * HEAD + LANES, HEAD - LANES)] = gradient[:, LANES:].astype(
                    BF16
                )
            dproj[2, rows, columns] = d_values.astype(BF16)

    def gradient_tile(owner, j):
        columns = tile_of(owner * (part // TILE) + j, TILE)
        d_attn = dot_nt(dproj[0], w3[0, columns, :])
        d_attn = d_attn + dot_nt(dproj[1], w3[1, columns, :])
        d_attn = d_attn + dot_nt(dproj[2], w3[2, columns, :])
        d_mlp = dot_nt(dh[...], w1[columns, :])
        normed = (xv[:, columns].astype(F32) - means[...]) * inv_stds[...]
        total = d_attn * gains[0:1, columns] + d_mlp * gains[1:2, columns]
        term[owner, :, tile_of(j, TILE)] = total.astype(BF16)
        vectors[0:1, columns] = jnp.sum(d_attn * normed, axis=0, keepdims=True)
        vectors[1:2, columns] = jnp.sum(d_mlp * normed, axis=0, keepdims=True)
        vectors[2:3, columns] = jnp.sum(d_attn, axis=0, keepdims=True)
        vectors[3:4, columns] = jnp.sum(d_mlp, axis=0, keepdims=True)

    each_chunk(1, gradient_tile)

    outs = [(xv, x_out), (act, act_out), (context, context_out), (dh, dh_out), (dproj, dproj_out), (gbv, gb_out)]
    stores = [pltpu.make_async_copy(a, b, store.at[i]) for i, (a, b) in enumerate(outs)]
    for copy in stores:
        copy.start()

    def input_gradient():
        def rows_of(i):
            rows = tile_of(i, row_tile)
            inv_std = inv_stds[rows, :]
            normed = (xv[rows, :].astype(F32) - means[rows, :]) * inv_std
            dx = row_norm_backward(full[rows, :].astype(F32), normed, inv_std)
            slope[rows, :] = gbv[rows, :].astype(F32) + dx

        loop(row_tiles, rows_of)

    @pl.when(section == 0)
    def _():
        reduce(1, 2, False)
        within_section(2, full)
        finish_sends(1)
        input_gradient()

    @pl.when(section == 1)
    def _():
        finish_back(0)
        reduce(1, 1, False)
        to_other_section(1)
        finish_sends(1)
        each_chunk(0, out_tile)
        from_own_section(1, full)
        input_gradient()
        reduce(0, 3, True)
        within_section(3, other)
        finish_sends(0)

    last = [
        pltpu.make_async_copy(other, layer_out, store.at[6]),
        pltpu.make_async_copy(slope, input_grad, store.at[7]),
    ]
    for copy in last:
        copy.start()
    for copy in stores + last:
        copy.wait()


def chain(block_input, grad_output, segment_ids, weights):
    w_qkv, w_out, w_fc1, w_fc2, gains, biases = weights
    batch, length, width = block_input.shape
    tokens = batch * length
    count = lax.axis_size("tensor")
    inner, hidden = w_qkv.shape[2], w_fc1.shape[1]
    part = width // count
    heads = inner // HEAD
    anywhere, vmem = pl.BlockSpec(memory_space=pl.ANY), pl.BlockSpec(memory_space=pltpu.VMEM)
    like = jax.ShapeDtypeStruct
    wide, narrow = (tokens, width), (tokens, inner)
    dma = pltpu.SemaphoreType.DMA
    return pl.pallas_call(
        functools.partial(chain_kernel, count, batch),
        out_shape=[
            like(wide, BF16),
            like(wide, F32),
            like((4, width), F32),
            like(wide, BF16),
            like((tokens, hidden), BF16),
            like(narrow, BF16),
            like((tokens, hidden), BF16),
            like((3, tokens, inner), BF16),
            like(wide, BF16),
        ],
        in_specs=[anywhere, anywhere, vmem, vmem] + [anywhere] * 4 + [vmem, vmem],
        out_specs=[anywhere, anywhere, vmem] + [anywhere] * 6,
        scratch_shapes=[
            pltpu.VMEM((3, width, inner), BF16),
            pltpu.VMEM((inner, width), BF16),
            pltpu.VMEM((width, hidden), BF16),
            pltpu.VMEM((hidden, width), BF16),
            pltpu.VMEM(wide, BF16),
            pltpu.VMEM(wide, BF16),
            pltpu.VMEM(wide, BF16),
            pltpu.VMEM(wide, BF16),
            pltpu.VMEM(wide, BF16),
            pltpu.VMEM((3, tokens, inner), BF16),
            pltpu.VMEM(narrow, BF16),
            pltpu.VMEM((batch * heads, length, length), F32),
            pltpu.VMEM((tokens, hidden), BF16),
            pltpu.VMEM((tokens, hidden), F32),
            pltpu.VMEM((tokens, hidden), BF16),
            pltpu.VMEM(narrow, BF16),
            pltpu.VMEM((3, tokens, inner), BF16),
            pltpu.VMEM((tokens, 1), F32),
            pltpu.VMEM((tokens, 1), F32),
            pltpu.VMEM((tokens, 2 * LANES), F32),
            pltpu.VMEM((count, tokens, part), BF16),
            pltpu.VMEM((2, count, tokens, part), BF16),
            pltpu.VMEM((4, count, tokens, part), BF16),
            pltpu.VMEM(wide, BF16),
            dma((11,)),
            dma((8,)),
            dma((2, count)),
            dma((2, count)),
            dma((4, count)),
            dma((4, count)),
            dma((2, count)),
            dma((2, count)),
        ],
        compiler_params=pltpu.CompilerParams(
            collective_id=0, has_side_effects=True, vmem_limit_bytes=67_043_328
        ),
        name="chain",
    )(
        block_input.reshape(wide),
        grad_output.reshape(wide),
        segment_ids.reshape(tokens, 1),
        segment_ids,
        jnp.transpose(w_qkv, (1, 0, 2)),
        w_out,
        w_fc1,
        w_fc2,
        gains,
        biases,
    )


def shards(
    block_input, grad_output, segment_ids, w_qkv, w_out, w_fc1, w_fc2, norm_gains, norm_biases
):
    batch, length, width = block_input.shape
    dp_count = lax.axis_size("dp")
    weights = (w_qkv[0], w_out[0], w_fc1[0], w_fc2[0], norm_gains[0], norm_biases[0])
    (layer_out, input_grads, vectors, inputs, activated, context, d_hidden, d_proj, grad_b) = chain(
        block_input, grad_output, segment_ids, weights
    )

    def gathered(value, axis=0):
        return lax.all_gather(value, "dp", axis=axis, tiled=True)

    def sliced(value):
        return lax.all_to_all(value, "dp", split_axis=1, concat_axis=0, tiled=True)

    mine = width // dp_count
    start = lax.axis_index("dp") * mine
    gains = lax.dynamic_slice_in_dim(norm_gains[0], start, mine, 1)
    biases = lax.dynamic_slice_in_dim(norm_biases[0], start, mine, 1)
    _, row_mean, inv_std = row_norm(inputs.astype(F32))
    rows = gathered(jnp.concatenate([row_mean, inv_std], axis=1))
    normed = (sliced(inputs).astype(F32) - rows[:, :1]) * rows[:, 1:]
    attn_in = (normed * gains[0] + biases[0]).astype(BF16)
    mlp_in = (normed * gains[1] + biases[1]).astype(BF16)
    grads_mine = sliced(grad_b)
    g_fc2 = dot(gathered(activated).T, grads_mine)
    g_out = dot(gathered(context).T, grads_mine)
    g_fc1 = dot(mlp_in.T, gathered(d_hidden))
    d_proj = gathered(d_proj, 1)
    g_qkv = jnp.stack([dot(attn_in.T, d_proj[k]) for k in range(3)], axis=1)
    summed = lax.psum(lax.psum_scatter(vectors, "dp", scatter_dimension=1, tiled=True), "tensor")
    shape = (1, batch, length, width)
    return (
        layer_out.reshape(shape),
        input_grads.reshape(shape),
        g_qkv[None],
        g_out[None],
        g_fc1[None],
        g_fc2[None],
        summed[None, :2],
        summed[None, 2:],
    )


def solution(mesh):
    return jax.shard_map(
        shards,
        mesh=mesh,
        in_specs=(
            P("dp", None, None),
            P("dp", None, None),
            P("dp", None),
            P("section", None, None, "tensor"),
            P("section", "tensor", None),
            P("section", None, "tensor"),
            P("section", "tensor", None),
            P("section", None, None),
            P("section", None, None),
        ),
        out_specs=(
            P("section", "dp", None, None),
            P("section", "dp", None, None),
            P("section", "dp", None, "tensor"),
            P("section", "tensor", "dp"),
            P("section", "dp", "tensor"),
            P("section", "tensor", "dp"),
            P("section", None, "dp"),
            P("section", None, "dp"),
        ),
        check_vma=False,
    )
```

```python
import functools
import math

import jax
import jax.numpy as jnp
from jax import lax
from jax.experimental import pallas as pl
from jax.experimental.pallas import tpu as pltpu
from jax.sharding import PartitionSpec as P

HEAD = 256
ROT = 64
LANES = 128
TILE = 256
NORM_EPSILON = 1e-05
MESH = pl.DeviceIdType.MESH
BF16 = jnp.bfloat16
F32 = jnp.float32


def partner(index, step, count):
    if count & (count - 1):
        return lax.rem(index + step, count), lax.rem(index + count - step, count)
    bit = 1
    while bit < count:
        index = index + ((step // bit) % 2) * (bit - 2 * bit * ((index // bit) % 2))
        bit *= 2
    return index, index


def loop(count, body, unroll=1):
    lax.fori_loop(0, count, lambda i, carry: (body(i), carry)[1], 0, unroll=unroll)


def tile_of(i, size):
    return pl.ds(pl.multiple_of(i * size, size), size)


def dot(left, right):
    return jnp.dot(left, right, preferred_element_type=jnp.float32)


def dot_nt(left, right):
    return lax.dot_general(left, right, (((1,), (1,)), ((), ())), preferred_element_type=jnp.float32)


def dot_tn(left, right):
    return lax.dot_general(left, right, (((0,), (0,)), ((), ())), preferred_element_type=jnp.float32)


def gelu_parts(hidden):
    normal_cdf = 0.5 * (1.0 + lax.erf(hidden * (1.0 / math.sqrt(2.0))))
    density = jnp.exp(-0.5 * hidden * hidden) * (1.0 / math.sqrt(2.0 * math.pi))
    return (hidden * normal_cdf, normal_cdf + hidden * density)


def lanes_of(shape):
    return lax.broadcasted_iota(jnp.int32, shape, len(shape) - 1)


def rotated(tile, cosine, sine):
    half = ROT // 2
    left, right = pltpu.roll(tile, LANES - half, 1), pltpu.roll(tile, half, 1)
    lane = lanes_of(tile.shape)
    turned = jnp.where(lane < half, -left, right)
    return tile * cosine + turned * sine


def unrotated(tile, cosine, sine):
    half = ROT // 2
    scaled = tile * sine
    left, right = pltpu.roll(scaled, LANES - half, 1), pltpu.roll(scaled, half, 1)
    lane = lanes_of(tile.shape)
    turned = jnp.where(lane < half, left, jnp.where(lane < ROT, -right, 0.0))
    return tile * cosine + turned


def row_norm(values):
    mean = jnp.mean(values, axis=-1, keepdims=True)
    centred = values - mean
    inv_std = lax.rsqrt(jnp.mean(centred * centred, axis=-1, keepdims=True) + NORM_EPSILON)
    return centred * inv_std, mean, inv_std


def row_norm_backward(summed, normed, inv_std):
    return inv_std * (
        summed
        - jnp.mean(summed, axis=-1, keepdims=True)
        - normed * jnp.mean(summed * normed, axis=-1, keepdims=True)
    )


def chain_kernel(count, batch, *refs):
    (
        x_hbm, go_hbm, seg_col, seg_row, w3_hbm, wo_hbm, w1_hbm, w2_hbm, gains, biases,
        layer_out, input_grad, totals, x_all, gb_all, context_all, dproj_all, act_all, dh_all, stats_all,
        slope_all,
        w3, wo, w1, w2, xv, other, gbv, attn_in, mlp_in, qkv, context, probs, act, slope, dh, dctx,
        dproj, means, inv_stds, tables, term, arrived, parts, full, act_rest, slope_rest,
        vectors, plane_vectors, slices,
        load, store, send, recv, part_send, part_recv, back_send, back_recv,
        line_send, line_recv, plane_send, plane_recv, rest_load, rest_store, sum_send, sum_recv,
        slice_send, slice_recv,
    ) = refs
    section, me = lax.axis_index("section"), lax.axis_index("tensor")
    row, rows_count = lax.axis_index("dp"), lax.axis_size("dp")
    tokens, width = xv.shape
    length = tokens // batch
    heads = qkv.shape[2] // HEAD
    hidden_width = act.shape[1]
    part = width // count
    row_tile = 32 if tokens % 32 == 0 else 16
    row_tiles = tokens // row_tile
    scale = 1.0 / math.sqrt(HEAD)

    qkv_loads = [pltpu.make_async_copy(w3_hbm.at[k], w3.at[k], load.at[k]) for k in range(3)]
    blocks = 4
    block = hidden_width // blocks

    def fc1_load(i):
        columns = tile_of(i, block)
        return pltpu.make_async_copy(w1_hbm.at[:, columns], w1.at[:, columns], load.at[3 + i])

    out_load = pltpu.make_async_copy(wo_hbm, wo, load.at[7])
    fc2_load = pltpu.make_async_copy(w2_hbm, w2, load.at[8])
    x_load = pltpu.make_async_copy(x_hbm, xv, load.at[9])
    go_load = pltpu.make_async_copy(go_hbm, gbv, load.at[10])

    @pl.when(section == 0)
    def _():
        x_load.start()

    for copy in qkv_loads:
        copy.start()
    for i in range(blocks):
        fc1_load(i).start()
    out_load.start()
    fc2_load.start()
    go_load.start()

    def at(section, index):
        return {"section": section, "tensor": index}

    steps = list(range(1, count))
    barrier = pltpu.get_barrier_semaphore()
    for step in range(count):
        peer = partner(me, step, count)[0]
        pl.semaphore_signal(barrier, inc=1, device_id=at(1 - section, peer), device_id_type=MESH)
        if step:
            pl.semaphore_signal(barrier, inc=1, device_id=at(section, peer), device_id_type=MESH)

    for step in range(1, rows_count):
        pl.semaphore_signal(
            barrier,
            inc=1,
            device_id={"dp": lax.rem(row + step, rows_count)},
            device_id_type=MESH,
        )

    flows = (x_all, gb_all, context_all, dproj_all)

    def line_copy(flow, origin, up, own=None):
        place = flows[flow].at[origin, me] if flow < 2 else flows[flow].at[origin]
        return pltpu.make_async_remote_copy(
            src_ref=place if own is None else own,
            dst_ref=place,
            send_sem=line_send.at[flow, int(up), origin],
            recv_sem=line_recv.at[flow, origin],
            device_id={"dp": row + (1 if up else -1)},
            device_id_type=MESH,
        )

    def plane_copy(flow, origin, step):
        peer = partner(me, step, count)[0]
        return pltpu.make_async_remote_copy(
            src_ref=flows[flow].at[origin, me],
            dst_ref=flows[flow].at[origin, me],
            send_sem=plane_send.at[flow, origin, step],
            recv_sem=plane_recv.at[flow, origin, step],
            device_id=at(section, peer),
            device_id_type=MESH,
        )

    def send_plane(flow, origin):
        for step in steps[::-1]:
            plane_copy(flow, origin, step).start()

    def start_flow(flow, own):
        if flow < 2:
            own = own.at[:, tile_of(me, part)]

        @pl.when(row + 1 < rows_count)
        def _():
            line_copy(flow, row, True, own).start()

        @pl.when(row >= 1)
        def _():
            line_copy(flow, row, False, own).start()

    def hop(flow, third, plane=True):
        def one(hops):
            @pl.when(row >= hops)
            def _():
                origin = row - hops
                line_copy(flow, origin, True).wait_recv()

                @pl.when(row + 1 < rows_count)
                def _():
                    line_copy(flow, origin, True).start()

                if flow < 2 and plane:
                    send_plane(flow, origin)

            @pl.when(row + hops < rows_count)
            def _():
                origin = row + hops
                line_copy(flow, origin, False).wait_recv()

                @pl.when(row >= 1)
                def _():
                    line_copy(flow, origin, False).start()

                if flow < 2 and plane:
                    send_plane(flow, origin)

        low, high = (1 + (rows_count - 1) * k // 3 for k in (third - 1, third))
        loop(high - low, lambda i: one(low + i))

    def others(body):
        def one(i):
            hops = 1 + i // 2
            origin = row + hops * (1 - 2 * lax.rem(i, 2))

            @pl.when((origin >= 0) & (origin < rows_count))
            def _():
                body(origin)

        loop(2 * (rows_count - 1), one)

    def finish_flow(flow):
        def one(origin):
            @pl.when((origin <= row) & (row + 1 < rows_count))
            def _():
                line_copy(flow, origin, True).wait_send()

            @pl.when((origin >= row) & (row >= 1))
            def _():
                line_copy(flow, origin, False).wait_send()

            if flow < 2:

                @pl.when(origin != row)
                def _():
                    for step in steps:
                        plane_copy(flow, origin, step).wait_send()

        loop(rows_count, one)

    def own_stores(flow, own):
        return [
            pltpu.make_async_copy(
                own.at[:, pl.ds(i * part, part)], flows[flow].at[row, i], store.at[flow * count + i]
            )
            for i in range(count)
        ]

    def scatter(kind, step):
        peer = partner(me, step, count)[0]
        return pltpu.make_async_remote_copy(
            src_ref=term.at[peer],
            dst_ref=arrived.at[kind, step],
            send_sem=send.at[kind, step],
            recv_sem=recv.at[kind, step],
            device_id=at(section, peer),
            device_id_type=MESH,
        )

    def gather(number, step, target):
        peer = partner(me, step, count)[0]
        return pltpu.make_async_remote_copy(
            src_ref=parts.at[number, 0],
            dst_ref=parts.at[number, step],
            send_sem=part_send.at[number, step],
            recv_sem=part_recv.at[number, step],
            device_id=at(target, peer),
            device_id_type=MESH,
        )

    def back(number, step):
        return pltpu.make_async_remote_copy(
            src_ref=parts.at[number, step],
            dst_ref=parts.at[number, step],
            send_sem=back_send.at[number, step],
            recv_sem=back_recv.at[number, step],
            device_id=at(1 - section, me),
            device_id_type=MESH,
        )

    def place(number, step, target):
        owner = partner(me, step, count)[1]
        target[:, tile_of(owner, part)] = parts[number, step]

    def reduce(kind, number, with_input):
        for step in steps:
            scatter(kind, step).wait_recv()

        def rows_of(i):
            rows = tile_of(i, row_tile)
            total = term[me, rows, :].astype(F32)
            if with_input:
                total = total + xv[rows, tile_of(me, part)].astype(F32)
            for step in steps:
                total = total + arrived[kind, step, rows, :].astype(F32)
            parts[number, 0, rows, :] = total.astype(BF16)

        loop(row_tiles, rows_of)

    def finish_sends(kind):
        for step in steps:
            scatter(kind, step).wait_send()

    def to_other_section(number):
        for step in steps[::-1] + [0]:
            gather(number, step, 1 - section).start()

    def from_own_section(number, target):
        place(number, 0, target)
        for step in steps:
            back(number, step).wait_recv()
            place(number, step, target)
        for step in [0] + steps:
            gather(number, step, 1 - section).wait_send()

    def from_other_section(number, target):
        gather(number, 0, 1 - section).wait_recv()
        place(number, 0, target)
        for step in steps:
            gather(number, step, 1 - section).wait_recv()
            back(number, step).start()
            place(number, step, target)

    def finish_back(number):
        for step in steps:
            back(number, step).wait_send()

    def start_within(number):
        for step in steps[::-1]:
            gather(number, step, section).start()

    def finish_within(number, target):
        place(number, 0, target)
        for step in steps:
            gather(number, step, section).wait_recv()
            place(number, step, target)
        for step in steps:
            gather(number, step, section).wait_send()

    def each_chunk(kind, compute):
        def chunk(i):
            step = count - 1 - i
            owner = partner(me, step, count)[0]
            loop(part // TILE, lambda j: compute(owner, j))

            @pl.when(step > 0)
            def _():
                scatter(kind, step).start()

        loop(count, chunk)

    lane = lanes_of((1, LANES)).astype(F32)
    exponent = jnp.where(lane < ROT // 2, lane, lane - ROT // 2)
    frequency = jnp.exp(exponent * (-2.0 * math.log(10000.0) / ROT))
    for b in range(batch):
        rows = pl.ds(b * length, length)
        earlier = (seg_row[b : b + 1, :] < seg_col[rows, :]).astype(F32)
        number_of = jnp.sum(earlier, axis=1, keepdims=True)
        index = lax.broadcasted_iota(jnp.int32, (length, 1), 0).astype(F32)
        angles = (index - number_of) * frequency
        inside = lanes_of((length, LANES)) < ROT
        tables[rows, :LANES] = jnp.where(inside, jnp.cos(angles), 1.0)
        tables[rows, LANES:] = jnp.where(inside, jnp.sin(angles), 0.0)

    def allowed_of(b):
        row = lax.broadcasted_iota(jnp.int32, (length, length), 0)
        column = lax.broadcasted_iota(jnp.int32, (length, length), 1)
        same = seg_row[b : b + 1, :] == seg_col[pl.ds(b * length, length), :]
        return same & (column <= row)

    def d_context_head(h):
        dctx[:, tile_of(h, HEAD)] = dot_nt(gbv[...], wo[tile_of(h, HEAD), :]).astype(BF16)

    pl.semaphore_wait(barrier, 2 * count - 1 + rows_count - 1)

    @pl.when(section == 0)
    def _():
        x_load.wait()

    @pl.when(section == 1)
    def _():
        go_load.wait()
        start_flow(1, gbv)
        out_load.wait()
        loop(heads, d_context_head)
        fc2_load.wait()

        def d_act_tile(i):
            columns = tile_of(i, TILE)
            slope[:, columns] = dot_nt(gbv[...], w2[columns, :])

        loop(hidden_width // TILE, d_act_tile)
        for third in (1, 2, 3):
            hop(1, third, plane=False)
        from_other_section(0, xv)

    start_flow(0, xv)
    for copy in own_stores(0, xv):
        copy.start()

    def norm_rows(i):
        rows = tile_of(i, row_tile)
        normed, mean, inv_std = row_norm(xv[rows, :].astype(F32))
        means[rows, :] = mean
        inv_stds[rows, :] = inv_std
        attn_in[rows, :] = (normed * gains[0:1, :] + biases[0:1, :]).astype(BF16)
        mlp_in[rows, :] = (normed * gains[1:2, :] + biases[1:2, :]).astype(BF16)

    loop(row_tiles, norm_rows)

    def rotary_head(i):
        which, h = i // heads, lax.rem(i, heads)
        tile = dot(attn_in[...], w3[which, :, tile_of(h, HEAD)])
        first = rotated(tile[:, :LANES], tables[:, :LANES], tables[:, LANES:])
        qkv[which, :, pl.ds(pl.multiple_of(h * HEAD, HEAD), LANES)] = first.astype(BF16)
        qkv[which, :, pl.ds(pl.multiple_of(h * HEAD + LANES, LANES), HEAD - LANES)] = tile[
            :, LANES:
        ].astype(BF16)

    def value_head(h):
        qkv[2, :, tile_of(h, HEAD)] = dot(attn_in[...], w3[2, :, tile_of(h, HEAD)]).astype(BF16)

    qkv_loads[0].wait()
    qkv_loads[1].wait()
    loop(2 * heads, rotary_head)
    qkv_loads[2].wait()
    loop(heads, value_head)
    hop(0, 1)

    @pl.when(section == 1)
    def _():
        others(lambda origin: send_plane(1, origin))

    for b in range(batch):
        rows = pl.ds(b * length, length)
        allowed = allowed_of(b)
        for h in range(heads):
            columns = pl.ds(h * HEAD, HEAD)
            scores = dot_nt(qkv[0, rows, columns], qkv[1, rows, columns]) * scale
            scores = jnp.where(allowed, scores, -jnp.inf)
            row_max = jnp.max(scores, axis=-1, keepdims=True)
            total = jnp.sum(jnp.exp(scores - row_max), axis=-1, keepdims=True)
            prob = jnp.exp(scores - (row_max + jnp.log(total)))
            probs[b * heads + h] = prob
            context[rows, columns] = dot(prob.astype(BF16), qkv[2, rows, columns]).astype(BF16)

    start_flow(2, context)
    hop(0, 2)

    def fc1_block(i):
        fc1_load(i).wait()

        def fc1_tile(j):
            columns = tile_of(i * (block // TILE) + j, TILE)
            value, derivative = gelu_parts(dot(mlp_in[...], w1[:, columns]))
            act[:, columns] = value.astype(BF16)

            @pl.when(section == 0)
            def _():
                slope[:, columns] = derivative

            @pl.when(section == 1)
            def _():
                dh[:, columns] = (slope[:, columns] * derivative).astype(BF16)

        loop(block // TILE, fc1_tile)

    loop(blocks, fc1_block)
    hop(0, 3)

    @pl.when(section == 0)
    def _():
        out_load.wait()
        fc2_load.wait()
        go_load.wait()

    tiles = hidden_width // TILE

    def act_store(origin, i):
        columns = tile_of(i, TILE)
        return pltpu.make_async_copy(
            act_rest.at[:, columns], act_all.at[origin, :, columns], rest_store.at[0, i]
        )

    def dh_store(origin, i):
        columns = tile_of(i, TILE)
        return pltpu.make_async_copy(
            act_rest.at[:, columns], dh_all.at[origin, :, columns], rest_store.at[0, i]
        )

    def slope_store(origin, i):
        columns = tile_of(i, TILE)
        return pltpu.make_async_copy(
            slope_rest.at[:, columns], slope_all.at[origin, :, columns], rest_store.at[1, i]
        )

    def load_block(flow, origin):
        for step in steps:
            plane_copy(flow, origin, step).wait_recv()
        copies = [
            pltpu.make_async_copy(
                flows[flow].at[origin, i], attn_in.at[:, pl.ds(i * part, part)], rest_load.at[i]
            )
            for i in range(count)
        ]
        for copy in copies:
            copy.start()
        return copies

    def rest_forward(origin):
        for copy in load_block(0, origin):
            copy.wait()

        def norm_rows(i):
            rows = tile_of(i, row_tile)
            normed, mean, inv_std = row_norm(attn_in[rows, :].astype(F32))
            first = lanes_of((row_tile, LANES)) == 0
            stats_all[origin, rows, :] = jnp.where(first, mean, inv_std)
            mlp_in[rows, :] = (normed * gains[1:2, :] + biases[1:2, :]).astype(BF16)

        loop(row_tiles, norm_rows)

        def tile(i):
            columns = tile_of(i, TILE)
            value, derivative = gelu_parts(dot(mlp_in[...], w1[:, columns]))
            act_rest[:, columns] = value.astype(BF16)
            slope_rest[:, columns] = derivative
            act_store(origin, i).start()
            slope_store(origin, i).start()

        loop(tiles, tile)

        def wait(i):
            act_store(origin, i).wait()
            slope_store(origin, i).wait()

        loop(tiles, wait)

    def rest_backward(origin):
        copies = load_block(1, origin)
        slope_load = pltpu.make_async_copy(slope_all.at[origin], slope_rest, rest_load.at[count])
        slope_load.start()
        for copy in copies + [slope_load]:
            copy.wait()

        def tile(i):
            columns = tile_of(i, TILE)
            d_act = dot_nt(attn_in[...], w2[columns, :])
            act_rest[:, columns] = (d_act * slope_rest[:, columns]).astype(BF16)
            dh_store(origin, i).start()

        loop(tiles, tile)
        loop(tiles, lambda i: dh_store(origin, i).wait())

    def out_tile(owner, j):
        columns = tile_of(owner * (part // TILE) + j, TILE)
        total = dot(context[...], wo[:, columns]) + dot(act[...], w2[:, columns])
        term[owner, :, tile_of(j, TILE)] = total.astype(BF16)

    @pl.when(section == 0)
    def _():
        each_chunk(0, out_tile)
        reduce(0, 0, True)
        to_other_section(0)
        finish_sends(0)
        hop(2, 1)
        others(rest_forward)
        hop(2, 2)
        hop(2, 3)
        from_own_section(0, other)
        from_other_section(1, full)

        def gradient_rows(i):
            rows = tile_of(i, row_tile)
            normed, _, inv_std = row_norm(other[rows, :].astype(F32))
            dx = row_norm_backward(full[rows, :].astype(F32), normed, inv_std)
            gbv[rows, :] = (gbv[rows, :].astype(F32) + dx).astype(BF16)

        loop(row_tiles, gradient_rows)
        start_flow(1, gbv)
        finish_back(1)

        def d_hidden_tile(i):
            columns = tile_of(i, TILE)
            d_act = dot_nt(gbv[...], w2[columns, :])
            dh[:, columns] = (d_act * slope[:, columns]).astype(BF16)

        loop(hidden_width // TILE, d_hidden_tile)
        loop(heads, d_context_head)
        hop(1, 1)


    for b in range(batch):
        rows = pl.ds(b * length, length)
        cosine, sine = tables[rows, :LANES], tables[rows, LANES:]
        for h in range(heads):
            columns = pl.ds(h * HEAD, HEAD)
            queries, keys, values = (qkv[k, rows, columns] for k in range(3))
            d_context = dctx[rows, columns]
            prob = probs[b * heads + h]
            d_values = dot_tn(prob.astype(BF16), d_context)
            d_probs = dot_nt(d_context, values)
            delta = jnp.sum(prob * d_probs, axis=-1, keepdims=True)
            d_scores = (prob * (d_probs - delta) * scale).astype(BF16)
            for k, gradient in ((0, dot(d_scores, keys)), (1, dot_tn(d_scores, queries))):
                first = unrotated(gradient[:, :LANES], cosine, sine)
                dproj[k, rows, pl.ds(h * HEAD, LANES)] = first.astype(BF16)
                dproj[k, rows, pl.ds(h * HEAD + LANES, HEAD - LANES)] = gradient[:, LANES:].astype(
                    BF16
                )
            dproj[2, rows, columns] = d_values.astype(BF16)

    start_flow(3, dproj)

    @pl.when(section == 0)
    def _():
        hop(1, 2)

    @pl.when(section == 1)
    def _():
        hop(2, 1)

    def gradient_tile(owner, j):
        columns = tile_of(owner * (part // TILE) + j, TILE)
        d_attn = dot_nt(dproj[0], w3[0, columns, :])
        d_attn = d_attn + dot_nt(dproj[1], w3[1, columns, :])
        d_attn = d_attn + dot_nt(dproj[2], w3[2, columns, :])
        d_mlp = dot_nt(dh[...], w1[columns, :])
        normed = (xv[:, columns].astype(F32) - means[...]) * inv_stds[...]
        total = d_attn * gains[0:1, columns] + d_mlp * gains[1:2, columns]
        term[owner, :, tile_of(j, TILE)] = total.astype(BF16)
        vectors[0:1, columns] = jnp.sum(d_attn * normed, axis=0, keepdims=True)
        vectors[1:2, columns] = jnp.sum(d_mlp * normed, axis=0, keepdims=True)
        vectors[2:3, columns] = jnp.sum(d_attn, axis=0, keepdims=True)
        vectors[3:4, columns] = jnp.sum(d_mlp, axis=0, keepdims=True)

    each_chunk(1, gradient_tile)

    outs = [
        (act, act_all.at[row]),
        (context, context_all.at[row]),
        (dh, dh_all.at[row]),
        (dproj, dproj_all.at[row]),
    ]
    stores = own_stores(1, gbv)
    stores += [
        pltpu.make_async_copy(a, b, store.at[2 * count + i]) for i, (a, b) in enumerate(outs)
    ]
    for copy in stores:
        copy.start()

    def sum_copy(step):
        peer = partner(me, step, count)[0]
        return pltpu.make_async_remote_copy(
            src_ref=vectors,
            dst_ref=plane_vectors.at[step],
            send_sem=sum_send.at[step],
            recv_sem=sum_recv.at[step],
            device_id=at(section, peer),
            device_id_type=MESH,
        )

    mine = width // rows_count

    def slice_copy(step):
        target = lax.rem(row + step, rows_count)
        return pltpu.make_async_remote_copy(
            src_ref=plane_vectors.at[0, :, tile_of(target, mine)],
            dst_ref=slices.at[step],
            send_sem=slice_send.at[step],
            recv_sem=slice_recv.at[step],
            device_id={"dp": target},
            device_id_type=MESH,
        )

    for step in steps:
        sum_copy(step).start()

    def sum_plane():
        total = vectors[...]
        for step in steps:
            sum_copy(step).wait_recv()
            total = total + plane_vectors[step]
        plane_vectors[0] = total
        for step in range(1, rows_count):
            slice_copy(step).start()

    def sum_line():
        total = plane_vectors[0, :, tile_of(row, mine)]
        for step in range(1, rows_count):
            slice_copy(step).wait_recv()
            total = total + slices[step]
        totals[...] = total
        for step in range(1, rows_count):
            slice_copy(step).wait_send()
        for step in steps:
            sum_copy(step).wait_send()

    def own_stats(i):
        rows = tile_of(i, row_tile)
        first = lanes_of((row_tile, LANES)) == 0
        stats_all[row, rows, :] = jnp.where(first, means[rows, :], inv_stds[rows, :])

    loop(row_tiles, own_stats)

    def input_gradient():
        def rows_of(i):
            rows = tile_of(i, row_tile)
            inv_std = inv_stds[rows, :]
            normed = (xv[rows, :].astype(F32) - means[rows, :]) * inv_std
            dx = row_norm_backward(full[rows, :].astype(F32), normed, inv_std)
            slope[rows, :] = gbv[rows, :].astype(F32) + dx

        loop(row_tiles, rows_of)

    @pl.when(section == 0)
    def _():
        hop(1, 3)
        reduce(1, 2, False)
        start_within(2)
        hop(3, 1)
        others(rest_backward)
        finish_within(2, full)
        finish_sends(1)
        input_gradient()
        sum_plane()
        hop(3, 2)
        hop(3, 3)

    @pl.when(section == 1)
    def _():
        finish_back(0)
        reduce(1, 1, False)
        to_other_section(1)
        finish_sends(1)
        hop(2, 2)
        each_chunk(0, out_tile)
        hop(2, 3)
        hop(3, 1)
        others(rest_forward)
        from_own_section(1, full)
        input_gradient()
        reduce(0, 3, True)
        start_within(3)
        hop(3, 2)
        others(rest_backward)
        finish_within(3, other)
        finish_sends(0)
        sum_plane()
        hop(3, 3)

    sum_line()
    last = [
        pltpu.make_async_copy(other, layer_out, store.at[2 * count + 4]),
        pltpu.make_async_copy(slope, input_grad, store.at[2 * count + 5]),
    ]
    for copy in last:
        copy.start()
    for copy in own_stores(0, xv) + stores + last:
        copy.wait()
    for flow in range(4):
        finish_flow(flow)


def chain(block_input, grad_output, segment_ids, weights):
    w_qkv, w_out, w_fc1, w_fc2, gains, biases = weights
    batch, length, width = block_input.shape
    tokens = batch * length
    count = lax.axis_size("tensor")
    inner, hidden = w_qkv.shape[2], w_fc1.shape[1]
    part = width // count
    heads = inner // HEAD
    anywhere, vmem = pl.BlockSpec(memory_space=pl.ANY), pl.BlockSpec(memory_space=pltpu.VMEM)
    like = jax.ShapeDtypeStruct
    rows_count = lax.axis_size("dp")
    wide, narrow = (tokens, width), (tokens, inner)
    dma = pltpu.SemaphoreType.DMA
    return pl.pallas_call(
        functools.partial(chain_kernel, count, batch),
        out_shape=[
            like(wide, BF16),
            like(wide, F32),
            like((4, width // rows_count), F32),
            like((rows_count, count, tokens, part), BF16),
            like((rows_count, count, tokens, part), BF16),
            like((rows_count, tokens, inner), BF16),
            like((rows_count, 3, tokens, inner), BF16),
            like((rows_count, tokens, hidden), BF16),
            like((rows_count, tokens, hidden), BF16),
            like((rows_count, tokens, LANES), F32),
            like((rows_count, tokens, hidden), F32),
        ],
        in_specs=[anywhere, anywhere, vmem, vmem] + [anywhere] * 4 + [vmem, vmem],
        out_specs=[anywhere, anywhere, vmem] + [anywhere] * 6 + [vmem, anywhere],
        scratch_shapes=[
            pltpu.VMEM((3, width, inner), BF16),
            pltpu.VMEM((inner, width), BF16),
            pltpu.VMEM((width, hidden), BF16),
            pltpu.VMEM((hidden, width), BF16),
            pltpu.VMEM(wide, BF16),
            pltpu.VMEM(wide, BF16),
            pltpu.VMEM(wide, BF16),
            pltpu.VMEM(wide, BF16),
            pltpu.VMEM(wide, BF16),
            pltpu.VMEM((3, tokens, inner), BF16),
            pltpu.VMEM(narrow, BF16),
            pltpu.VMEM((batch * heads, length, length), F32),
            pltpu.VMEM((tokens, hidden), BF16),
            pltpu.VMEM((tokens, hidden), F32),
            pltpu.VMEM((tokens, hidden), BF16),
            pltpu.VMEM(narrow, BF16),
            pltpu.VMEM((3, tokens, inner), BF16),
            pltpu.VMEM((tokens, 1), F32),
            pltpu.VMEM((tokens, 1), F32),
            pltpu.VMEM((tokens, 2 * LANES), F32),
            pltpu.VMEM((count, tokens, part), BF16),
            pltpu.VMEM((2, count, tokens, part), BF16),
            pltpu.VMEM((4, count, tokens, part), BF16),
            pltpu.VMEM(wide, BF16),
            pltpu.VMEM((tokens, hidden), BF16),
            pltpu.VMEM((tokens, hidden), F32),
            pltpu.VMEM((4, width), F32),
            pltpu.VMEM((count, 4, width), F32),
            pltpu.VMEM((rows_count, 4, width // rows_count), F32),
            dma((11,)),
            dma((2 * count + 6,)),
            dma((2, count)),
            dma((2, count)),
            dma((4, count)),
            dma((4, count)),
            dma((2, count)),
            dma((2, count)),
            dma((4, 2, rows_count)),
            dma((4, rows_count)),
            dma((2, rows_count, count)),
            dma((2, rows_count, count)),
            dma((count + 1,)),
            dma((2, hidden // TILE)),
            dma((count,)),
            dma((count,)),
            dma((rows_count,)),
            dma((rows_count,)),
        ],
        compiler_params=pltpu.CompilerParams(
            collective_id=0, has_side_effects=True, vmem_limit_bytes=67_043_328
        ),
        name="chain",
    )(
        block_input.reshape(wide),
        grad_output.reshape(wide),
        segment_ids.reshape(tokens, 1),
        segment_ids,
        jnp.transpose(w_qkv, (1, 0, 2)),
        w_out,
        w_fc1,
        w_fc2,
        gains,
        biases,
    )


def shards(
    block_input, grad_output, segment_ids, w_qkv, w_out, w_fc1, w_fc2, norm_gains, norm_biases
):
    batch, length, width = block_input.shape
    dp_count, tensor_count = lax.axis_size("dp"), lax.axis_size("tensor")
    weights = (w_qkv[0], w_out[0], w_fc1[0], w_fc2[0], norm_gains[0], norm_biases[0])
    (layer_out, input_grads, summed, x_all, gb_all, context, d_proj, activated, d_hidden, stats, _) = chain(
        block_input, grad_output, segment_ids, weights
    )
    mine, part = width // dp_count, width // tensor_count
    start = lax.axis_index("dp") * mine

    def sliced(value):
        chunk = lax.dynamic_index_in_dim(value, start // part, 1, keepdims=False)
        return lax.dynamic_slice_in_dim(chunk, start % part, mine, 2).reshape(-1, mine)

    def flat(value):
        return value.reshape(-1, value.shape[-1])

    gains = lax.dynamic_slice_in_dim(norm_gains[0], start, mine, 1)
    biases = lax.dynamic_slice_in_dim(norm_biases[0], start, mine, 1)
    stats = flat(stats)
    normed = (sliced(x_all).astype(F32) - stats[:, :1]) * stats[:, 1:2]
    attn_in = (normed * gains[0] + biases[0]).astype(BF16)
    mlp_in = (normed * gains[1] + biases[1]).astype(BF16)
    grads_mine = sliced(gb_all)
    g_fc2 = dot(flat(activated).T, grads_mine)
    g_out = dot(flat(context).T, grads_mine)
    g_fc1 = dot(mlp_in.T, flat(d_hidden))
    g_qkv = jnp.stack([dot(attn_in.T, flat(d_proj[:, k])) for k in range(3)], axis=1)
    shape = (1, batch, length, width)
    return (
        layer_out.reshape(shape),
        input_grads.reshape(shape),
        g_qkv[None],
        g_out[None],
        g_fc1[None],
        g_fc2[None],
        summed[None, :2],
        summed[None, 2:],
    )


def solution(mesh):
    return jax.shard_map(
        shards,
        mesh=mesh,
        in_specs=(
            P("dp", None, None),
            P("dp", None, None),
            P("dp", None),
            P("section", None, None, "tensor"),
            P("section", "tensor", None),
            P("section", None, "tensor"),
            P("section", "tensor", None),
            P("section", None, None),
            P("section", None, None),
        ),
        out_specs=(
            P("section", "dp", None, None),
            P("section", "dp", None, None),
            P("section", "dp", None, "tensor"),
            P("section", "tensor", "dp"),
            P("section", "dp", "tensor"),
            P("section", "tensor", "dp"),
            P("section", None, "dp"),
            P("section", None, "dp"),
        ),
        check_vma=False,
    )
```

```python
import functools
import math

import jax
import jax.numpy as jnp
from jax import lax
from jax.experimental import pallas as pl
from jax.experimental.pallas import tpu as pltpu
from jax.sharding import PartitionSpec as P

HEAD = 256
ROT = 64
LANES = 128
TILE = 256
NORM_EPSILON = 1e-05
MESH = pl.DeviceIdType.MESH
BF16 = jnp.bfloat16
F32 = jnp.float32


def partner(index, step, count):
    if count & (count - 1):
        return lax.rem(index + step, count), lax.rem(index + count - step, count)
    bit = 1
    while bit < count:
        index = index + ((step // bit) % 2) * (bit - 2 * bit * ((index // bit) % 2))
        bit *= 2
    return index, index


def loop(count, body, unroll=1):
    lax.fori_loop(0, count, lambda i, carry: (body(i), carry)[1], 0, unroll=unroll)


def tile_of(i, size):
    return pl.ds(pl.multiple_of(i * size, size), size)


def dot(left, right):
    return jnp.dot(left, right, preferred_element_type=jnp.float32)


def dot_nt(left, right):
    return lax.dot_general(left, right, (((1,), (1,)), ((), ())), preferred_element_type=jnp.float32)


def dot_tn(left, right):
    return lax.dot_general(left, right, (((0,), (0,)), ((), ())), preferred_element_type=jnp.float32)


def gelu_parts(hidden):
    normal_cdf = 0.5 * (1.0 + lax.erf(hidden * (1.0 / math.sqrt(2.0))))
    density = jnp.exp(-0.5 * hidden * hidden) * (1.0 / math.sqrt(2.0 * math.pi))
    return (hidden * normal_cdf, normal_cdf + hidden * density)


def lanes_of(shape):
    return lax.broadcasted_iota(jnp.int32, shape, len(shape) - 1)


def rotated(tile, cosine, sine):
    half = ROT // 2
    left, right = pltpu.roll(tile, LANES - half, 1), pltpu.roll(tile, half, 1)
    lane = lanes_of(tile.shape)
    turned = jnp.where(lane < half, -left, right)
    return tile * cosine + turned * sine


def unrotated(tile, cosine, sine):
    half = ROT // 2
    scaled = tile * sine
    left, right = pltpu.roll(scaled, LANES - half, 1), pltpu.roll(scaled, half, 1)
    lane = lanes_of(tile.shape)
    turned = jnp.where(lane < half, left, jnp.where(lane < ROT, -right, 0.0))
    return tile * cosine + turned


def row_norm(values):
    mean = jnp.mean(values, axis=-1, keepdims=True)
    centred = values - mean
    inv_std = lax.rsqrt(jnp.mean(centred * centred, axis=-1, keepdims=True) + NORM_EPSILON)
    return centred * inv_std, mean, inv_std


def row_norm_backward(summed, normed, inv_std):
    return inv_std * (
        summed
        - jnp.mean(summed, axis=-1, keepdims=True)
        - normed * jnp.mean(summed * normed, axis=-1, keepdims=True)
    )


def chain_kernel(count, batch, *refs):
    (
        x_hbm, go_hbm, seg_row, w3_hbm, wo_hbm, w1_hbm, w2_hbm, gains, biases,
        layer_out, input_grad, totals, x_all, gb_all, context_all, dproj_all, act_all, dh_all, stats_all,
        slope_all, relay_x, qkv_all,
        w3, wo, w1, w2, xv, other, gbv, attn_in, mlp_in, qkv, context, probs, act, slope, dh, dctx,
        dproj, means, inv_stds, tables, term, arrived, parts, full, act_rest, slope_rest,
        vectors, plane_vectors, slices, segments, qkv_rest, dproj_rest, context_rest,
        load, store, send, recv, part_send, part_recv, back_send, back_recv,
        line_send, line_recv, plane_send, plane_recv, rest_load, rest_store, sum_send, sum_recv,
        slice_send, slice_recv, engine_send, segment_send, segment_recv,
    ) = refs
    section, me = lax.axis_index("section"), lax.axis_index("tensor")
    row, rows_count = lax.axis_index("dp"), lax.axis_size("dp")
    tokens, width = xv.shape
    length = tokens // batch
    heads = qkv.shape[2] // HEAD
    hidden_width = act.shape[1]
    part = width // count
    row_tile = 32 if tokens % 32 == 0 else 16
    row_tiles = tokens // row_tile
    scale = 1.0 / math.sqrt(HEAD)

    qkv_loads = [pltpu.make_async_copy(w3_hbm.at[k], w3.at[k], load.at[k]) for k in range(3)]
    blocks = 4
    block = hidden_width // blocks

    def fc1_load(i):
        columns = tile_of(i, block)
        return pltpu.make_async_copy(w1_hbm.at[:, columns], w1.at[:, columns], load.at[3 + i])

    out_load = pltpu.make_async_copy(wo_hbm, wo, load.at[7])
    fc2_load = pltpu.make_async_copy(w2_hbm, w2, load.at[8])
    x_load = pltpu.make_async_copy(x_hbm, xv, load.at[9])
    go_load = pltpu.make_async_copy(go_hbm, gbv, load.at[10])

    @pl.when(section == 0)
    def _():
        x_load.start()

    for copy in qkv_loads:
        copy.start()
    for i in range(blocks):
        fc1_load(i).start()
    out_load.start()
    fc2_load.start()
    go_load.start()

    def at(section, index):
        return {"section": section, "tensor": index}

    steps = list(range(1, count))
    barrier = pltpu.get_barrier_semaphore()
    for step in range(count):
        peer = partner(me, step, count)[0]
        pl.semaphore_signal(barrier, inc=1, device_id=at(1 - section, peer), device_id_type=MESH)
        if step:
            pl.semaphore_signal(barrier, inc=1, device_id=at(section, peer), device_id_type=MESH)

    for step in range(1, rows_count):
        pl.semaphore_signal(
            barrier,
            inc=1,
            device_id={"dp": lax.rem(row + step, rows_count)},
            device_id_type=MESH,
        )

    flows = (x_all, gb_all, context_all, dproj_all, relay_x)

    def line_copy(flow, origin, up, own=None):
        place = flows[flow].at[origin, me] if flow < 2 else flows[flow].at[origin]
        return pltpu.make_async_remote_copy(
            src_ref=place if own is None else own,
            dst_ref=place,
            send_sem=line_send.at[flow, int(up), origin],
            recv_sem=line_recv.at[flow, origin],
            device_id={"dp": row + (1 if up else -1)},
            device_id_type=MESH,
        )

    def plane_copy(flow, origin, step):
        peer = partner(me, step, count)[0]
        return pltpu.make_async_remote_copy(
            src_ref=flows[flow].at[origin, me],
            dst_ref=flows[flow].at[origin, me],
            send_sem=plane_send.at[flow, origin, step],
            recv_sem=plane_recv.at[flow, origin, step],
            device_id=at(section, peer),
            device_id_type=MESH,
        )

    balanced = count == 4
    direct_steps = [1, 2] if balanced else steps

    def send_plane(flow, origin):
        for step in direct_steps[::-1]:
            plane_copy(flow, origin, step).start()

    def half_copy(flow, origin, half):
        owner = partner(me, 1 + half, count)[1]
        place = flows[flow].at[origin, owner, pl.ds(half * (tokens // 2), tokens // 2), :]
        return pltpu.make_async_remote_copy(
            src_ref=place,
            dst_ref=place,
            send_sem=plane_send.at[flow, origin, 3 * half],
            recv_sem=plane_recv.at[flow, origin, 3 * half],
            device_id=at(section, partner(me, 2 - half, count)[0]),
            device_id_type=MESH,
        )

    def relay_plane(flow, origin):
        if balanced:
            for step in direct_steps:
                plane_copy(flow, origin, step).wait_recv()
            for half in range(2):
                half_copy(flow, origin, half).start()

    def wait_plane(flow, origin):
        if balanced:
            for half in range(2):
                half_copy(flow, origin, half).wait_recv()
        else:
            for step in steps:
                plane_copy(flow, origin, step).wait_recv()

    def send_plane_of(flow):
        return lambda origin: send_plane(flow, origin)

    def relay_plane_of(flow):
        return lambda origin: relay_plane(flow, origin)

    def engine_copy(origin, step):
        peer = partner(me, step, count)[0]
        return pltpu.make_async_remote_copy(
            src_ref=relay_x.at[origin],
            dst_ref=x_all.at[origin, me],
            send_sem=engine_send.at[origin, step],
            recv_sem=plane_recv.at[0, origin, step],
            device_id=at(1 - section, peer),
            device_id_type=MESH,
        )

    def send_engine(origin):
        for step in steps[::-1] + [0]:
            engine_copy(origin, step).start()

    def start_flow(flow, own):
        if flow in (0, 1, 4):
            own = own.at[:, tile_of(me, part)]

        @pl.when(row + 1 < rows_count)
        def _():
            line_copy(flow, row, True, own).start()

        @pl.when(row >= 1)
        def _():
            line_copy(flow, row, False, own).start()

    def hop(flow, third, after=lambda origin: None):
        def one(hops):
            @pl.when(row >= hops)
            def _():
                origin = row - hops
                line_copy(flow, origin, True).wait_recv()

                @pl.when(row + 1 < rows_count)
                def _():
                    line_copy(flow, origin, True).start()

                after(origin)

            @pl.when(row + hops < rows_count)
            def _():
                origin = row + hops
                line_copy(flow, origin, False).wait_recv()

                @pl.when(row >= 1)
                def _():
                    line_copy(flow, origin, False).start()

                after(origin)

        low, high = (1 + (rows_count - 1) * k // 3 for k in (third - 1, third))
        loop(high - low, lambda i: one(low + i))

    def thirds(third, body):
        def one(i):
            hops = 1 + i // 2
            origin = row + hops * (1 - 2 * lax.rem(i, 2))

            @pl.when((origin >= 0) & (origin < rows_count))
            def _():
                body(origin)

        low, high = (2 * ((rows_count - 1) * k // 3) for k in (third, third + 1))
        loop(high - low, lambda i: one(low + i))

    def others(body, after=(), after_one=None):
        def one(i):
            hops = 1 + i // 2
            origin = row + hops * (1 - 2 * lax.rem(i, 2))

            @pl.when((origin >= 0) & (origin < rows_count))
            def _():
                body(origin)

            if after_one is not None:
                pl.when(i == 0)(after_one)
            for third, action in enumerate(after):
                pl.when(i == 2 * ((rows_count - 1) * (third + 1) // 3) - 1)(action)

        loop(2 * (rows_count - 1), one)

    def finish_flow(flow):
        def one(origin):
            @pl.when((origin <= row) & (row + 1 < rows_count))
            def _():
                line_copy(flow, origin, True).wait_send()

            @pl.when((origin >= row) & (row >= 1))
            def _():
                line_copy(flow, origin, False).wait_send()

            @pl.when(origin != row)
            def _():
                if flow < 2:
                    for step in direct_steps:
                        plane_copy(flow, origin, step).wait_send()
                    if balanced:
                        for half in range(2):
                            half_copy(flow, origin, half).wait_send()
                if flow == 4:
                    for step in [0] + steps:
                        engine_copy(origin, step).wait_send()

        loop(rows_count, one)

    def own_stores(flow, own):
        return [
            pltpu.make_async_copy(
                own.at[:, pl.ds(i * part, part)], flows[flow].at[row, i], store.at[flow * count + i]
            )
            for i in range(count)
        ]

    def scatter(kind, step):
        peer = partner(me, step, count)[0]
        return pltpu.make_async_remote_copy(
            src_ref=term.at[peer],
            dst_ref=arrived.at[kind, step],
            send_sem=send.at[kind, step],
            recv_sem=recv.at[kind, step],
            device_id=at(section, peer),
            device_id_type=MESH,
        )

    def gather(number, step, target):
        peer = partner(me, step, count)[0]
        return pltpu.make_async_remote_copy(
            src_ref=parts.at[number, 0],
            dst_ref=parts.at[number, step],
            send_sem=part_send.at[number, step],
            recv_sem=part_recv.at[number, step],
            device_id=at(target, peer),
            device_id_type=MESH,
        )

    def back(number, step):
        return pltpu.make_async_remote_copy(
            src_ref=parts.at[number, step],
            dst_ref=parts.at[number, step],
            send_sem=back_send.at[number, step],
            recv_sem=back_recv.at[number, step],
            device_id=at(1 - section, me),
            device_id_type=MESH,
        )

    def place(number, step, target):
        owner = partner(me, step, count)[1]
        target[:, tile_of(owner, part)] = parts[number, step]

    def reduce(kind, number, with_input):
        for step in steps:
            scatter(kind, step).wait_recv()

        def rows_of(i):
            rows = tile_of(i, row_tile)
            total = term[me, rows, :].astype(F32)
            if with_input:
                total = total + xv[rows, tile_of(me, part)].astype(F32)
            for step in steps:
                total = total + arrived[kind, step, rows, :].astype(F32)
            parts[number, 0, rows, :] = total.astype(BF16)

        loop(row_tiles, rows_of)

    def finish_sends(kind):
        for step in steps:
            scatter(kind, step).wait_send()

    def to_other_section(number):
        for step in steps[::-1] + [0]:
            gather(number, step, 1 - section).start()

    def from_own_section(number, target):
        place(number, 0, target)
        for step in steps:
            back(number, step).wait_recv()
            place(number, step, target)
        for step in [0] + steps:
            gather(number, step, 1 - section).wait_send()

    def from_other_section(number, target):
        gather(number, 0, 1 - section).wait_recv()
        place(number, 0, target)
        for step in steps:
            gather(number, step, 1 - section).wait_recv()
            back(number, step).start()
            place(number, step, target)

    def finish_back(number):
        for step in steps:
            back(number, step).wait_send()

    def start_within(number):
        for step in steps[::-1]:
            gather(number, step, section).start()

    def finish_within(number, target):
        place(number, 0, target)
        for step in steps:
            gather(number, step, section).wait_recv()
            place(number, step, target)
        for step in steps:
            gather(number, step, section).wait_send()

    def each_chunk(kind, compute, between=None):
        def chunk(i):
            step = count - 1 - i
            owner = partner(me, step, count)[0]
            loop(part // TILE, lambda j: compute(owner, j))

            @pl.when(step > 0)
            def _():
                scatter(kind, step).start()

            if between is not None:
                pl.when(i == count // 2 - 1)(between)

        loop(count, chunk)

    lane = lanes_of((1, LANES)).astype(F32)
    exponent = jnp.where(lane < ROT // 2, lane, lane - ROT // 2)
    frequency = jnp.exp(exponent * (-2.0 * math.log(10000.0) / ROT))
    row_index = lax.broadcasted_iota(jnp.int32, (length, length), 0)
    column_index = lax.broadcasted_iota(jnp.int32, (length, length), 1)

    def segments_of(values):
        across = values.astype(F32)
        down = jnp.sum(jnp.where(row_index == column_index, across, 0.0), axis=1, keepdims=True)
        return across, down

    def fill_tables(slot, values_of):
        for b in range(batch):
            rows = pl.ds(b * length, length)
            across, down = segments_of(values_of(b))
            number_of = jnp.sum((across < down).astype(F32), axis=1, keepdims=True)
            index = lax.broadcasted_iota(jnp.int32, (length, 1), 0).astype(F32)
            angles = (index - number_of) * frequency
            inside = lanes_of((length, LANES)) < ROT
            tables[slot, rows, :LANES] = jnp.where(inside, jnp.cos(angles), 1.0)
            tables[slot, rows, LANES:] = jnp.where(inside, jnp.sin(angles), 0.0)

    fill_tables(row, lambda b: seg_row[b : b + 1, :])

    def softmax(projected, values, b, h):
        rows, columns = tile_of(b, length), tile_of(h, HEAD)
        across, down = segments_of(values)
        allowed = (across == down) & (column_index <= row_index)
        scores = dot_nt(projected[0, rows, columns], projected[1, rows, columns]) * scale
        scores = jnp.where(allowed, scores, -jnp.inf)
        row_max = jnp.max(scores, axis=-1, keepdims=True)
        total = jnp.sum(jnp.exp(scores - row_max), axis=-1, keepdims=True)
        return jnp.exp(scores - (row_max + jnp.log(total)))

    def attend(prob, projected, target, b, h):
        rows, columns = tile_of(b, length), tile_of(h, HEAD)
        target[rows, columns] = dot(prob.astype(BF16), projected[2, rows, columns]).astype(BF16)

    def attend_backward(prob, projected, slot, target, b, h):
        rows, columns = tile_of(b, length), tile_of(h, HEAD)
        cosine, sine = tables[slot, rows, :LANES], tables[slot, rows, LANES:]
        queries, keys, values = (projected[k, rows, columns] for k in range(3))
        d_context = dctx[rows, columns]
        d_values = dot_tn(prob.astype(BF16), d_context)
        d_probs = dot_nt(d_context, values)
        delta = jnp.sum(prob * d_probs, axis=-1, keepdims=True)
        d_scores = (prob * (d_probs - delta) * scale).astype(BF16)
        for k, gradient in ((0, dot(d_scores, keys)), (1, dot_tn(d_scores, queries))):
            first = unrotated(gradient[:, :LANES], cosine, sine)
            start = pl.multiple_of(h * HEAD, HEAD)
            target[k, rows, pl.ds(start, LANES)] = first.astype(BF16)
            start = pl.multiple_of(h * HEAD + LANES, LANES)
            target[k, rows, pl.ds(start, HEAD - LANES)] = gradient[:, LANES:].astype(BF16)
        target[2, rows, columns] = d_values.astype(BF16)

    def each_pair(body):
        def row_of(b):
            for h in range(heads):
                body(b, h)

        loop(batch, row_of)

    def project(projected, slot):
        def rotary_head(i):
            which, h = i // heads, lax.rem(i, heads)
            tile = dot(attn_in[...], w3[which, :, tile_of(h, HEAD)])
            first = rotated(tile[:, :LANES], tables[slot, :, :LANES], tables[slot, :, LANES:])
            start = pl.multiple_of(h * HEAD, HEAD)
            projected[which, :, pl.ds(start, LANES)] = first.astype(BF16)
            start = pl.multiple_of(h * HEAD + LANES, LANES)
            projected[which, :, pl.ds(start, HEAD - LANES)] = tile[:, LANES:].astype(BF16)

        def value_head(h):
            columns = tile_of(h, HEAD)
            projected[2, :, columns] = dot(attn_in[...], w3[2, :, columns]).astype(BF16)

        loop(2 * heads, rotary_head)
        loop(heads, value_head)

    def segment_copy(step):
        return pltpu.make_async_remote_copy(
            src_ref=seg_row,
            dst_ref=segments.at[row],
            send_sem=segment_send.at[step],
            recv_sem=segment_recv.at[step],
            device_id={"dp": lax.rem(row + step, rows_count)},
            device_id_type=MESH,
        )

    def d_context_head(h):
        dctx[:, tile_of(h, HEAD)] = dot_nt(gbv[...], wo[tile_of(h, HEAD), :]).astype(BF16)

    pl.semaphore_wait(barrier, 2 * count - 1 + rows_count - 1)
    for step in range(1, rows_count):
        segment_copy(step).start()

    @pl.when(section == 0)
    def _():
        x_load.wait()

    @pl.when(section == 1)
    def _():
        start_flow(4, x_hbm)
        go_load.wait()
        out_load.wait()
        loop(heads, d_context_head)
        hop(4, 1, send_engine)
        fc2_load.wait()

        def d_act_tile(i):
            columns = tile_of(i, TILE)
            slope[:, columns] = dot_nt(gbv[...], w2[columns, :])

        loop(hidden_width // TILE, d_act_tile)
        hop(4, 2)
        hop(4, 3)
        start_flow(1, gbv)
        hop(1, 1)
        hop(1, 2)
        from_other_section(0, xv)
        start_flow(0, xv)
        thirds(1, send_engine)
        thirds(2, send_engine)

    for copy in own_stores(0, xv):
        copy.start()

    def norm_rows(i):
        rows = tile_of(i, row_tile)
        normed, mean, inv_std = row_norm(xv[rows, :].astype(F32))
        means[rows, :] = mean
        inv_stds[rows, :] = inv_std
        attn_in[rows, :] = (normed * gains[0:1, :] + biases[0:1, :]).astype(BF16)
        mlp_in[rows, :] = (normed * gains[1:2, :] + biases[1:2, :]).astype(BF16)

    loop(row_tiles, norm_rows)

    for copy in qkv_loads:
        copy.wait()
    project(qkv, row)

    def own_attention(b, h):
        prob = softmax(qkv, seg_row[pl.ds(b, 1), :], b, h)
        probs[b * heads + h] = prob
        attend(prob, qkv, context, b, h)

    each_pair(own_attention)

    @pl.when(section == 1)
    def _():
        hop(0, 1, send_plane_of(0))


    def fc1_block(i):
        fc1_load(i).wait()

        def fc1_tile(j):
            columns = tile_of(i * (block // TILE) + j, TILE)
            value, derivative = gelu_parts(dot(mlp_in[...], w1[:, columns]))
            act[:, columns] = value.astype(BF16)

            @pl.when(section == 0)
            def _():
                slope[:, columns] = derivative

            @pl.when(section == 1)
            def _():
                dh[:, columns] = (slope[:, columns] * derivative).astype(BF16)

        loop(block // TILE, fc1_tile)

    loop(blocks, fc1_block)

    @pl.when(section == 1)
    def _():
        hop(0, 2, send_plane_of(0))
        thirds(0, relay_plane_of(0))

    @pl.when(section == 0)
    def _():
        out_load.wait()
        fc2_load.wait()
        go_load.wait()

    tiles = hidden_width // TILE

    def act_store(origin, i):
        columns = tile_of(i, TILE)
        return pltpu.make_async_copy(
            act_rest.at[:, columns], act_all.at[origin, :, columns], rest_store.at[0, i]
        )

    def dh_store(origin, i):
        columns = tile_of(i, TILE)
        return pltpu.make_async_copy(
            act_rest.at[:, columns], dh_all.at[origin, :, columns], rest_store.at[0, i]
        )

    def slope_store(origin, i):
        columns = tile_of(i, TILE)
        return pltpu.make_async_copy(
            slope_rest.at[:, columns], slope_all.at[origin, :, columns], rest_store.at[1, i]
        )

    def load_block(flow, origin):
        if flow == 0:

            @pl.when(section == 0)
            def _():
                for step in [0] + steps:
                    engine_copy(origin, step).wait_recv()

            pl.when(section == 1)(lambda: wait_plane(flow, origin))
        else:
            wait_plane(flow, origin)

        copies = [
            pltpu.make_async_copy(
                flows[flow].at[origin, i], attn_in.at[:, pl.ds(i * part, part)], rest_load.at[i]
            )
            for i in range(count)
        ]
        for copy in copies:
            copy.start()
        return copies

    def attention_stores(origin):
        return [
            pltpu.make_async_copy(qkv_rest, qkv_all.at[origin], rest_load.at[count + 1]),
            pltpu.make_async_copy(context_rest, context_all.at[origin], rest_load.at[count + 2]),
        ]

    def rest_forward(origin):
        for copy in load_block(0, origin):
            copy.wait()

        def norm_rows(i):
            rows = tile_of(i, row_tile)
            normed, mean, inv_std = row_norm(attn_in[rows, :].astype(F32))
            first = lanes_of((row_tile, LANES)) == 0
            stats_all[origin, rows, :] = jnp.where(first, mean, inv_std)
            mlp_in[rows, :] = (normed * gains[1:2, :] + biases[1:2, :]).astype(BF16)
            attn_in[rows, :] = (normed * gains[0:1, :] + biases[0:1, :]).astype(BF16)

        loop(row_tiles, norm_rows)

        @pl.when(section == 0)
        def _():
            fill_tables(origin, lambda b: segments[origin, b : b + 1, :])
            project(qkv_rest, origin)

            def attention(b, h):
                prob = softmax(qkv_rest, segments[origin, pl.ds(b, 1), :], b, h)
                attend(prob, qkv_rest, context_rest, b, h)

            each_pair(attention)
            for copy in attention_stores(origin):
                copy.start()

        def tile(i):
            columns = tile_of(i, TILE)
            value, derivative = gelu_parts(dot(mlp_in[...], w1[:, columns]))
            act_rest[:, columns] = value.astype(BF16)
            slope_rest[:, columns] = derivative
            act_store(origin, i).start()
            slope_store(origin, i).start()

        loop(tiles, tile)

        def wait(i):
            act_store(origin, i).wait()
            slope_store(origin, i).wait()

        loop(tiles, wait)

        @pl.when(section == 0)
        def _():
            for copy in attention_stores(origin):
                copy.wait()

    def rest_backward(origin):
        copies = load_block(1, origin)
        slope_load = pltpu.make_async_copy(slope_all.at[origin], slope_rest, rest_load.at[count])
        slope_load.start()
        for copy in copies + [slope_load]:
            copy.wait()

        def tile(i):
            columns = tile_of(i, TILE)
            d_act = dot_nt(attn_in[...], w2[columns, :])
            act_rest[:, columns] = (d_act * slope_rest[:, columns]).astype(BF16)
            dh_store(origin, i).start()

        qkv_load = pltpu.make_async_copy(qkv_all.at[origin], qkv_rest, rest_load.at[count + 1])
        dproj_store = pltpu.make_async_copy(
            dproj_rest, dproj_all.at[origin], rest_load.at[count + 2]
        )
        pl.when(section == 0)(qkv_load.start)
        loop(tiles, tile)

        @pl.when(section == 0)
        def _():
            qkv_load.wait()

            def head(h):
                columns = tile_of(h, HEAD)
                dctx[:, columns] = dot_nt(attn_in[...], wo[columns, :]).astype(BF16)

            loop(heads, head)

            def attention(b, h):
                prob = softmax(qkv_rest, segments[origin, pl.ds(b, 1), :], b, h)
                attend_backward(prob, qkv_rest, origin, dproj_rest, b, h)

            each_pair(attention)
            dproj_store.start()
            dproj_store.wait()

        loop(tiles, lambda i: dh_store(origin, i).wait())

    def out_tile(owner, j):
        columns = tile_of(owner * (part // TILE) + j, TILE)
        total = dot(context[...], wo[:, columns]) + dot(act[...], w2[:, columns])
        term[owner, :, tile_of(j, TILE)] = total.astype(BF16)

    @pl.when(section == 0)
    def _():
        each_chunk(0, out_tile)
        reduce(0, 0, True)
        to_other_section(0)
        finish_sends(0)
        for step in range(1, rows_count):
            segment_copy(step).wait_recv()
        others(rest_forward)
        from_own_section(0, other)
        from_other_section(1, full)

        def gradient_rows(i):
            rows = tile_of(i, row_tile)
            normed, _, inv_std = row_norm(other[rows, :].astype(F32))
            dx = row_norm_backward(full[rows, :].astype(F32), normed, inv_std)
            gbv[rows, :] = (gbv[rows, :].astype(F32) + dx).astype(BF16)

        loop(row_tiles, gradient_rows)
        start_flow(1, gbv)
        finish_back(1)

        def d_hidden_tile(i):
            columns = tile_of(i, TILE)
            d_act = dot_nt(gbv[...], w2[columns, :])
            dh[:, columns] = (d_act * slope[:, columns]).astype(BF16)

        loop(hidden_width // TILE, d_hidden_tile)
        loop(heads, d_context_head)
        hop(1, 1, send_plane_of(1))


    each_pair(lambda b, h: attend_backward(probs[b * heads + h], qkv, row, dproj, b, h))

    @pl.when(section == 1)
    def _():
        start_flow(3, dproj)
        hop(1, 3)

    def gradient_tile(owner, j):
        columns = tile_of(owner * (part // TILE) + j, TILE)
        d_attn = dot_nt(dproj[0], w3[0, columns, :])
        d_attn = d_attn + dot_nt(dproj[1], w3[1, columns, :])
        d_attn = d_attn + dot_nt(dproj[2], w3[2, columns, :])
        d_mlp = dot_nt(dh[...], w1[columns, :])
        normed = (xv[:, columns].astype(F32) - means[...]) * inv_stds[...]
        total = d_attn * gains[0:1, columns] + d_mlp * gains[1:2, columns]
        term[owner, :, tile_of(j, TILE)] = total.astype(BF16)
        vectors[0:1, columns] = jnp.sum(d_attn * normed, axis=0, keepdims=True)
        vectors[1:2, columns] = jnp.sum(d_mlp * normed, axis=0, keepdims=True)
        vectors[2:3, columns] = jnp.sum(d_attn, axis=0, keepdims=True)
        vectors[3:4, columns] = jnp.sum(d_mlp, axis=0, keepdims=True)

    def second_hop():
        @pl.when(section == 0)
        def _():
            hop(1, 2, send_plane_of(1))
            thirds(0, relay_plane_of(1))

    each_chunk(1, gradient_tile, second_hop)

    outs = [
        (act, act_all.at[row]),
        (context, context_all.at[row]),
        (dh, dh_all.at[row]),
        (dproj, dproj_all.at[row]),
    ]
    stores = own_stores(1, gbv)
    stores += [
        pltpu.make_async_copy(a, b, store.at[2 * count + i]) for i, (a, b) in enumerate(outs)
    ]
    for copy in stores:
        copy.start()

    def sum_copy(step):
        peer = partner(me, step, count)[0]
        return pltpu.make_async_remote_copy(
            src_ref=vectors,
            dst_ref=plane_vectors.at[step],
            send_sem=sum_send.at[step],
            recv_sem=sum_recv.at[step],
            device_id=at(section, peer),
            device_id_type=MESH,
        )

    mine = width // rows_count

    def slice_copy(step):
        target = lax.rem(row + step, rows_count)
        return pltpu.make_async_remote_copy(
            src_ref=plane_vectors.at[0, :, tile_of(target, mine)],
            dst_ref=slices.at[step],
            send_sem=slice_send.at[step],
            recv_sem=slice_recv.at[step],
            device_id={"dp": target},
            device_id_type=MESH,
        )

    for step in steps:
        sum_copy(step).start()

    def sum_plane():
        total = vectors[...]
        for step in steps:
            sum_copy(step).wait_recv()
            total = total + plane_vectors[step]
        plane_vectors[0] = total
        for step in range(1, rows_count):
            slice_copy(step).start()

    def sum_line():
        total = plane_vectors[0, :, tile_of(row, mine)]
        for step in range(1, rows_count):
            slice_copy(step).wait_recv()
            total = total + slices[step]
        totals[...] = total
        for step in range(1, rows_count):
            slice_copy(step).wait_send()
        for step in steps:
            sum_copy(step).wait_send()

    def own_stats(i):
        rows = tile_of(i, row_tile)
        first = lanes_of((row_tile, LANES)) == 0
        stats_all[row, rows, :] = jnp.where(first, means[rows, :], inv_stds[rows, :])

    loop(row_tiles, own_stats)

    def input_gradient():
        def rows_of(i):
            rows = tile_of(i, row_tile)
            inv_std = inv_stds[rows, :]
            normed = (xv[rows, :].astype(F32) - means[rows, :]) * inv_std
            dx = row_norm_backward(full[rows, :].astype(F32), normed, inv_std)
            slope[rows, :] = gbv[rows, :].astype(F32) + dx

        loop(row_tiles, rows_of)

    @pl.when(section == 0)
    def _():
        hop(1, 3, send_plane_of(1))

        def after_first():
            thirds(2, relay_plane_of(1))
            reduce(1, 2, False)
            start_within(2)

        others(rest_backward, [after_first], lambda: thirds(1, relay_plane_of(1)))
        finish_within(2, full)
        finish_sends(1)
        input_gradient()
        sum_plane()

    @pl.when(section == 1)
    def _():
        finish_back(0)
        reduce(1, 1, False)
        to_other_section(1)
        hop(0, 3, send_plane_of(0))
        thirds(1, relay_plane_of(0))
        finish_sends(1)
        hop(3, 1)

        def after_first():
            thirds(2, relay_plane_of(0))
            from_own_section(1, full)

        def after_second():
            for third in range(3):
                thirds(third, send_plane_of(1))

        others(rest_forward, [after_first, after_second])
        start_flow(2, context)
        hop(3, 2)
        input_gradient()
        each_chunk(0, out_tile)
        for third in range(3):
            thirds(third, relay_plane_of(1))
        hop(2, 1)
        hop(3, 3)
        others(rest_backward, [lambda: hop(2, 2), lambda: hop(2, 3)])
        reduce(0, 3, True)
        start_within(3)
        sum_plane()
        finish_within(3, other)
        finish_sends(0)

    sum_line()
    last = [
        pltpu.make_async_copy(other, layer_out, store.at[2 * count + 4]),
        pltpu.make_async_copy(slope, input_grad, store.at[2 * count + 5]),
    ]
    for copy in last:
        copy.start()
    for copy in own_stores(0, xv) + stores + last:
        copy.wait()
    finish_flow(1)

    @pl.when(section == 1)
    def _():
        for step in range(1, rows_count):
            segment_copy(step).wait_recv()
        for flow in (0, 2, 3, 4):
            finish_flow(flow)

    for step in range(1, rows_count):
        segment_copy(step).wait_send()


def chain(block_input, grad_output, segment_ids, weights):
    w_qkv, w_out, w_fc1, w_fc2, gains, biases = weights
    batch, length, width = block_input.shape
    tokens = batch * length
    count = lax.axis_size("tensor")
    inner, hidden = w_qkv.shape[2], w_fc1.shape[1]
    part = width // count
    heads = inner // HEAD
    anywhere, vmem = pl.BlockSpec(memory_space=pl.ANY), pl.BlockSpec(memory_space=pltpu.VMEM)
    like = jax.ShapeDtypeStruct
    rows_count = lax.axis_size("dp")
    wide, narrow = (tokens, width), (tokens, inner)
    dma = pltpu.SemaphoreType.DMA
    return pl.pallas_call(
        functools.partial(chain_kernel, count, batch),
        out_shape=[
            like(wide, BF16),
            like(wide, F32),
            like((4, width // rows_count), F32),
            like((rows_count, count, tokens, part), BF16),
            like((rows_count, count, tokens, part), BF16),
            like((rows_count, tokens, inner), BF16),
            like((rows_count, 3, tokens, inner), BF16),
            like((rows_count, tokens, hidden), BF16),
            like((rows_count, tokens, hidden), BF16),
            like((rows_count, tokens, LANES), F32),
            like((rows_count, tokens, hidden), F32),
            like((rows_count, tokens, part), BF16),
            like((rows_count, 3, tokens, inner), BF16),
        ],
        in_specs=[anywhere, anywhere, vmem] + [anywhere] * 4 + [vmem, vmem],
        out_specs=[anywhere, anywhere, vmem] + [anywhere] * 6 + [vmem, anywhere, anywhere, anywhere],
        scratch_shapes=[
            pltpu.VMEM((3, width, inner), BF16),
            pltpu.VMEM((inner, width), BF16),
            pltpu.VMEM((width, hidden), BF16),
            pltpu.VMEM((hidden, width), BF16),
            pltpu.VMEM(wide, BF16),
            pltpu.VMEM(wide, BF16),
            pltpu.VMEM(wide, BF16),
            pltpu.VMEM(wide, BF16),
            pltpu.VMEM(wide, BF16),
            pltpu.VMEM((3, tokens, inner), BF16),
            pltpu.VMEM(narrow, BF16),
            pltpu.VMEM((batch * heads, length, length), F32),
            pltpu.VMEM((tokens, hidden), BF16),
            pltpu.VMEM((tokens, hidden), F32),
            pltpu.VMEM((tokens, hidden), BF16),
            pltpu.VMEM(narrow, BF16),
            pltpu.VMEM((3, tokens, inner), BF16),
            pltpu.VMEM((tokens, 1), F32),
            pltpu.VMEM((tokens, 1), F32),
            pltpu.VMEM((rows_count, tokens, 2 * LANES), F32),
            pltpu.VMEM((count, tokens, part), BF16),
            pltpu.VMEM((2, count, tokens, part), BF16),
            pltpu.VMEM((4, count, tokens, part), BF16),
            pltpu.VMEM(wide, BF16),
            pltpu.VMEM((tokens, hidden), BF16),
            pltpu.VMEM((tokens, hidden), F32),
            pltpu.VMEM((4, width), F32),
            pltpu.VMEM((count, 4, width), F32),
            pltpu.VMEM((rows_count, 4, width // rows_count), F32),
            pltpu.VMEM((rows_count, batch, length), jnp.int32),
            pltpu.VMEM((3, tokens, inner), BF16),
            pltpu.VMEM((3, tokens, inner), BF16),
            pltpu.VMEM(narrow, BF16),
            dma((11,)),
            dma((2 * count + 6,)),
            dma((2, count)),
            dma((2, count)),
            dma((4, count)),
            dma((4, count)),
            dma((2, count)),
            dma((2, count)),
            dma((5, 2, rows_count)),
            dma((5, rows_count)),
            dma((2, rows_count, count)),
            dma((2, rows_count, count)),
            dma((count + 3,)),
            dma((2, hidden // TILE)),
            dma((count,)),
            dma((count,)),
            dma((rows_count,)),
            dma((rows_count,)),
            dma((rows_count, count)),
            dma((rows_count,)),
            dma((rows_count,)),
        ],
        compiler_params=pltpu.CompilerParams(
            collective_id=0, has_side_effects=True, vmem_limit_bytes=67_043_328
        ),
        name="chain",
    )(
        block_input.reshape(wide),
        grad_output.reshape(wide),
        segment_ids,
        jnp.transpose(w_qkv, (1, 0, 2)),
        w_out,
        w_fc1,
        w_fc2,
        gains,
        biases,
    )


def weight_kernel(*refs):
    (
        x_all, gb_all, stats, context_all, dproj_all, act_all, dh_all, gains, biases,
        g_qkv, g_out, g_fc1, g_fc2,
        x_mine, gb_mine, context, dproj, act, attn_t, mlp_t, r_qkv, r_out, r_fc1, r_fc2,
        load, act_load, dh_load, store,
    ) = refs
    blocks, tokens, mine = x_mine.shape
    rows = blocks * tokens
    part = x_all.shape[3]
    inner, hidden = context.shape[2], act.shape[2]
    start = lax.axis_index("dp") * mine
    chunk, offset = start // part, pl.multiple_of(lax.rem(start, part), LANES)
    piece = hidden // 4

    def slice_of(source):
        return source.at[:, chunk, :, pl.ds(offset, mine)]

    def piece_load(source, target, sems, i):
        columns = pl.ds(i * piece, piece)
        return pltpu.make_async_copy(source.at[:, :, columns], target.at[:, :, columns], sems.at[i])

    gb_load = pltpu.make_async_copy(slice_of(gb_all), gb_mine, load.at[0])
    x_load = pltpu.make_async_copy(slice_of(x_all), x_mine, load.at[1])
    context_load = pltpu.make_async_copy(context_all, context, load.at[2])
    dproj_load = pltpu.make_async_copy(dproj_all, dproj, load.at[3])
    act_loads = [piece_load(act_all, act, act_load, i) for i in range(4)]
    dh_loads = [piece_load(dh_all, act, dh_load, i) for i in range(4)]
    for copy in [gb_load, context_load] + act_loads + [x_load, dproj_load]:
        copy.start()

    def transposed_rows(i):
        columns = tile_of(i, LANES)
        mean = stats[:, :, 0:1].reshape(rows, 1)
        inv_std = stats[:, :, 1:2].reshape(rows, 1)
        normed = (x_mine[:, :, columns].reshape(rows, LANES).astype(F32) - mean) * inv_std
        whole = tile_of(chunk * (part // LANES) + offset // LANES + i, LANES)
        for j, target in enumerate((attn_t, mlp_t)):
            scaled = normed * gains[j : j + 1, whole] + biases[j : j + 1, whole]
            target[columns, :] = scaled.astype(BF16).T

    def out_copy(source, target, index):
        return pltpu.make_async_copy(source, target, store.at[index])

    gb_load.wait()
    context_load.wait()
    gb_rows = gb_mine[...].reshape(rows, mine)

    def out_tile(i):
        tile = tile_of(i, TILE)
        r_out[tile, :] = dot_tn(context[:, :, tile].reshape(rows, TILE), gb_rows)

    loop(inner // TILE, out_tile)
    copies = [out_copy(r_out, g_out, 0)]
    copies[0].start()

    def fc2_copy(i):
        tile = tile_of(i, TILE)
        return out_copy(r_fc2.at[tile, :], g_fc2.at[tile, :], 1 + i)

    def fc2_tile(i):
        tile = tile_of(i, TILE)
        r_fc2[tile, :] = dot_tn(act[:, :, tile].reshape(rows, TILE), gb_mine[...].reshape(rows, mine))
        fc2_copy(i).start()

    per = piece // TILE
    for i in range(4):
        act_loads[i].wait()
        loop(per, lambda j: fc2_tile(i * per + j))
        dh_loads[i].start()
    x_load.wait()
    loop(mine // LANES, transposed_rows)

    def fc1_copy(i):
        tile = tile_of(i, TILE)
        return out_copy(r_fc1.at[:, tile], g_fc1.at[:, tile], 1 + hidden // TILE + i)

    def fc1_tile(i):
        tile = tile_of(i, TILE)
        r_fc1[:, tile] = dot(mlp_t[...], act[:, :, tile].reshape(rows, TILE))
        fc1_copy(i).start()

    for copy in dh_loads:
        copy.wait()
    loop(hidden // TILE, fc1_tile)
    dproj_load.wait()
    per = inner // TILE

    def qkv_copy(i):
        which, tile = i // per, tile_of(lax.rem(i, per), TILE)
        return out_copy(r_qkv.at[which, :, tile], g_qkv.at[which, :, tile], 1 + 2 * (hidden // TILE) + i)

    def qkv_tile(i):
        which, tile = i // per, tile_of(lax.rem(i, per), TILE)
        r_qkv[which, :, tile] = dot(attn_t[...], dproj[:, which, :, tile].reshape(rows, TILE))
        qkv_copy(i).start()

    loop(3 * per, qkv_tile)
    copies[0].wait()
    loop(hidden // TILE, lambda i: fc2_copy(i).wait())
    loop(hidden // TILE, lambda i: fc1_copy(i).wait())
    loop(3 * per, lambda i: qkv_copy(i).wait())


def weight_gradients(x_all, gb_all, stats, context_all, dproj_all, act_all, dh_all, gains, biases):
    blocks, count, tokens, part = x_all.shape
    mine = count * part // lax.axis_size("dp")
    inner, hidden = context_all.shape[2], act_all.shape[2]
    anywhere, vmem = pl.BlockSpec(memory_space=pl.ANY), pl.BlockSpec(memory_space=pltpu.VMEM)
    shapes = [(3, mine, inner), (inner, mine), (mine, hidden), (hidden, mine)]
    dma = pltpu.SemaphoreType.DMA
    return pl.pallas_call(
        weight_kernel,
        out_shape=[jax.ShapeDtypeStruct(shape, F32) for shape in shapes],
        in_specs=[anywhere, anywhere, vmem] + [anywhere] * 4 + [vmem, vmem],
        out_specs=[anywhere] * 4,
        scratch_shapes=[
            pltpu.VMEM((blocks, tokens, mine), BF16),
            pltpu.VMEM((blocks, tokens, mine), BF16),
            pltpu.VMEM((blocks, tokens, inner), BF16),
            pltpu.VMEM((blocks, 3, tokens, inner), BF16),
            pltpu.VMEM((blocks, tokens, hidden), BF16),
            pltpu.VMEM((mine, blocks * tokens), BF16),
            pltpu.VMEM((mine, blocks * tokens), BF16),
        ]
        + [pltpu.VMEM(shape, F32) for shape in shapes]
        + [
            dma((4,)),
            dma((4,)),
            dma((4,)),
            dma((1 + 2 * (hidden // TILE) + 3 * (inner // TILE),)),
        ],
        compiler_params=pltpu.CompilerParams(vmem_limit_bytes=67_043_328),
        name="weights",
    )(x_all, gb_all, stats, context_all, dproj_all, act_all, dh_all, gains, biases)


def shards(
    block_input, grad_output, segment_ids, w_qkv, w_out, w_fc1, w_fc2, norm_gains, norm_biases
):
    batch, length, width = block_input.shape
    weights = (w_qkv[0], w_out[0], w_fc1[0], w_fc2[0], norm_gains[0], norm_biases[0])
    (layer_out, input_grads, summed, x_all, gb_all, context, d_proj, activated, d_hidden, stats, *_) = chain(
        block_input, grad_output, segment_ids, weights
    )
    g_qkv, g_out, g_fc1, g_fc2 = weight_gradients(
        x_all, gb_all, stats, context, d_proj, activated, d_hidden, norm_gains[0], norm_biases[0]
    )
    shape = (1, batch, length, width)
    return (
        layer_out.reshape(shape),
        input_grads.reshape(shape),
        jnp.transpose(g_qkv, (1, 0, 2))[None],
        g_out[None],
        g_fc1[None],
        g_fc2[None],
        summed[None, :2],
        summed[None, 2:],
    )


def solution(mesh):
    return jax.shard_map(
        shards,
        mesh=mesh,
        in_specs=(
            P("dp", None, None),
            P("dp", None, None),
            P("dp", None),
            P("section", None, None, "tensor"),
            P("section", "tensor", None),
            P("section", None, "tensor"),
            P("section", "tensor", None),
            P("section", None, None),
            P("section", None, None),
        ),
        out_specs=(
            P("section", "dp", None, None),
            P("section", "dp", None, None),
            P("section", "dp", None, "tensor"),
            P("section", "tensor", "dp"),
            P("section", "dp", "tensor"),
            P("section", "tensor", "dp"),
            P("section", None, "dp"),
            P("section", None, "dp"),
        ),
        check_vma=False,
    )
```

```python
import functools
import math

import jax
import jax.numpy as jnp
from jax import lax
from jax.experimental import pallas as pl
from jax.experimental.pallas import tpu as pltpu
from jax.sharding import PartitionSpec as P

HEAD = 256
ROT = 64
LANES = 128
TILE = 256
NORM_EPSILON = 1e-05
MESH = pl.DeviceIdType.MESH
BF16 = jnp.bfloat16
F32 = jnp.float32


def partner(index, step, count):
    if count & (count - 1):
        return lax.rem(index + step, count), lax.rem(index + count - step, count)
    bit = 1
    while bit < count:
        index = index + ((step // bit) % 2) * (bit - 2 * bit * ((index // bit) % 2))
        bit *= 2
    return index, index


def loop(count, body, unroll=1):
    lax.fori_loop(0, count, lambda i, carry: (body(i), carry)[1], 0, unroll=unroll)


def tile_of(i, size):
    return pl.ds(pl.multiple_of(i * size, size), size)


def dot(left, right):
    return jnp.dot(left, right, preferred_element_type=jnp.float32)


def dot_nt(left, right):
    return lax.dot_general(left, right, (((1,), (1,)), ((), ())), preferred_element_type=jnp.float32)


def dot_tn(left, right):
    return lax.dot_general(left, right, (((0,), (0,)), ((), ())), preferred_element_type=jnp.float32)


def gelu_parts(hidden):
    normal_cdf = 0.5 * (1.0 + lax.erf(hidden * (1.0 / math.sqrt(2.0))))
    density = jnp.exp(-0.5 * hidden * hidden) * (1.0 / math.sqrt(2.0 * math.pi))
    return (hidden * normal_cdf, normal_cdf + hidden * density)


def lanes_of(shape):
    return lax.broadcasted_iota(jnp.int32, shape, len(shape) - 1)


def rotated(tile, cosine, sine):
    half = ROT // 2
    left, right = pltpu.roll(tile, LANES - half, 1), pltpu.roll(tile, half, 1)
    lane = lanes_of(tile.shape)
    turned = jnp.where(lane < half, -left, right)
    return tile * cosine + turned * sine


def unrotated(tile, cosine, sine):
    half = ROT // 2
    scaled = tile * sine
    left, right = pltpu.roll(scaled, LANES - half, 1), pltpu.roll(scaled, half, 1)
    lane = lanes_of(tile.shape)
    turned = jnp.where(lane < half, left, jnp.where(lane < ROT, -right, 0.0))
    return tile * cosine + turned


def row_norm(values):
    mean = jnp.mean(values, axis=-1, keepdims=True)
    centred = values - mean
    inv_std = lax.rsqrt(jnp.mean(centred * centred, axis=-1, keepdims=True) + NORM_EPSILON)
    return centred * inv_std, mean, inv_std


def row_norm_backward(summed, normed, inv_std):
    return inv_std * (
        summed
        - jnp.mean(summed, axis=-1, keepdims=True)
        - normed * jnp.mean(summed * normed, axis=-1, keepdims=True)
    )


def chain_kernel(count, batch, *refs):
    (
        x_hbm, go_hbm, seg_row, w3_hbm, wo_hbm, w1_hbm, w2_hbm, gains, biases,
        layer_out, input_grad, gain_grads, bias_grads, x_all, gb_all, context_all, dproj_all, act_all, dh_all, stats_out,
        slope_all, relay_x, qkv_all,
        w3, wo, w1, w2, xv, other, gbv, attn_in, mlp_in, qkv, context, probs, act, slope, dh, dctx,
        dproj, means, inv_stds, tables, term, arrived, parts, full, act_rest, slope_rest,
        stats_all, vectors, plane_vectors, slices, segments, qkv_rest, dproj_rest, context_rest,
        load, store, send, recv, part_send, part_recv, back_send, back_recv,
        line_send, line_recv, plane_send, plane_recv, rest_load, rest_store, sum_send, sum_recv,
        slice_send, slice_recv, engine_send, segment_send, segment_recv,
    ) = refs
    section, me = lax.axis_index("section"), lax.axis_index("tensor")
    row, rows_count = lax.axis_index("dp"), lax.axis_size("dp")
    tokens, width = xv.shape
    length = tokens // batch
    heads = qkv.shape[2] // HEAD
    hidden_width = act.shape[1]
    part = width // count
    row_tile = 32 if tokens % 32 == 0 else 16
    row_tiles = tokens // row_tile
    scale = 1.0 / math.sqrt(HEAD)

    qkv_loads = [pltpu.make_async_copy(w3_hbm.at[k], w3.at[k], load.at[k]) for k in range(3)]
    blocks = 4
    block = hidden_width // blocks

    def fc1_load(i):
        columns = tile_of(i, block)
        return pltpu.make_async_copy(w1_hbm.at[:, columns], w1.at[:, columns], load.at[3 + i])

    out_load = pltpu.make_async_copy(wo_hbm, wo, load.at[7])
    fc2_load = pltpu.make_async_copy(w2_hbm, w2, load.at[8])
    x_load = pltpu.make_async_copy(x_hbm, xv, load.at[9])
    go_load = pltpu.make_async_copy(go_hbm, gbv, load.at[10])

    @pl.when(section == 0)
    def _():
        x_load.start()

    go_load.start()

    def start_out_loads():
        out_load.start()
        fc2_load.start()

    pl.when(section == 1)(start_out_loads)
    for copy in qkv_loads:
        copy.start()
    for i in range(blocks):
        fc1_load(i).start()
    pl.when(section == 0)(start_out_loads)

    def at(section, index):
        return {"section": section, "tensor": index}

    steps = list(range(1, count))
    barrier = pltpu.get_barrier_semaphore()
    for step in range(count):
        peer = partner(me, step, count)[0]
        pl.semaphore_signal(barrier, inc=1, device_id=at(1 - section, peer), device_id_type=MESH)
        if step:
            pl.semaphore_signal(barrier, inc=1, device_id=at(section, peer), device_id_type=MESH)

    for step in range(1, rows_count):
        pl.semaphore_signal(
            barrier,
            inc=1,
            device_id={"dp": lax.rem(row + step, rows_count)},
            device_id_type=MESH,
        )

    flows = (x_all, gb_all, context_all, dproj_all, relay_x)

    def line_copy(flow, origin, up, own=None):
        place = flows[flow].at[origin, me] if flow < 2 else flows[flow].at[origin]
        return pltpu.make_async_remote_copy(
            src_ref=place if own is None else own,
            dst_ref=place,
            send_sem=line_send.at[flow, int(up), origin],
            recv_sem=line_recv.at[flow, origin],
            device_id={"dp": row + (1 if up else -1)},
            device_id_type=MESH,
        )

    def plane_copy(flow, origin, step):
        peer = partner(me, step, count)[0]
        return pltpu.make_async_remote_copy(
            src_ref=flows[flow].at[origin, me],
            dst_ref=flows[flow].at[origin, me],
            send_sem=plane_send.at[flow, origin, step],
            recv_sem=plane_recv.at[flow, origin, step],
            device_id=at(section, peer),
            device_id_type=MESH,
        )

    balanced = count == 4
    direct_steps = [1, 2] if balanced else steps

    def send_plane(flow, origin):
        for step in direct_steps[::-1]:
            plane_copy(flow, origin, step).start()

    def half_copy(flow, origin, half):
        owner = partner(me, 1 + half, count)[1]
        place = flows[flow].at[origin, owner, pl.ds(half * (tokens // 2), tokens // 2), :]
        return pltpu.make_async_remote_copy(
            src_ref=place,
            dst_ref=place,
            send_sem=plane_send.at[flow, origin, 3 * half],
            recv_sem=plane_recv.at[flow, origin, 3 * half],
            device_id=at(section, partner(me, 2 - half, count)[0]),
            device_id_type=MESH,
        )

    def relay_plane(flow, origin):
        if balanced:
            for step in direct_steps:
                plane_copy(flow, origin, step).wait_recv()
            for half in range(2):
                half_copy(flow, origin, half).start()

    def wait_plane(flow, origin):
        if balanced:
            for half in range(2):
                half_copy(flow, origin, half).wait_recv()
        else:
            for step in steps:
                plane_copy(flow, origin, step).wait_recv()

    def send_plane_of(flow):
        return lambda origin: send_plane(flow, origin)

    def relay_plane_of(flow):
        return lambda origin: relay_plane(flow, origin)

    def engine_copy(origin, step):
        peer = partner(me, step, count)[0]
        return pltpu.make_async_remote_copy(
            src_ref=relay_x.at[origin],
            dst_ref=x_all.at[origin, me],
            send_sem=engine_send.at[origin, step],
            recv_sem=plane_recv.at[0, origin, step],
            device_id=at(1 - section, peer),
            device_id_type=MESH,
        )

    def send_engine(origin):
        for step in steps[::-1] + [0]:
            engine_copy(origin, step).start()

    first_other = jnp.where(row == rows_count - 1, row - 1, row + 1)

    def send_engine_first(origin):
        pl.when(origin == first_other)(lambda: send_engine(origin))

    def send_engine_later(origin):
        pl.when(origin != first_other)(lambda: send_engine(origin))

    def start_flow(flow, own):
        if flow in (0, 1, 4):
            own = own.at[:, tile_of(me, part)]

        @pl.when(row + 1 < rows_count)
        def _():
            line_copy(flow, row, True, own).start()

        @pl.when(row >= 1)
        def _():
            line_copy(flow, row, False, own).start()

    near = 2 * (rows_count - 1) // 3

    def hop(flow, third, after=lambda origin: None, limit=None):
        limit = rows_count if limit is None else limit

        def one(hops):
            @pl.when(row >= hops)
            def _():
                origin = row - hops
                line_copy(flow, origin, True).wait_recv()

                @pl.when((row + 1 < rows_count) & (hops < limit))
                def _():
                    line_copy(flow, origin, True).start()

                after(origin)

            @pl.when(row + hops < rows_count)
            def _():
                origin = row + hops
                line_copy(flow, origin, False).wait_recv()

                @pl.when((row >= 1) & (hops < limit))
                def _():
                    line_copy(flow, origin, False).start()

                after(origin)

        low, high = (1 + (rows_count - 1) * k // 3 for k in (third - 1, third))
        loop(high - low, lambda i: one(low + i))

    def thirds(third, body):
        def one(i):
            hops = 1 + i // 2
            origin = row + hops * (1 - 2 * lax.rem(i, 2))

            @pl.when((origin >= 0) & (origin < rows_count))
            def _():
                body(origin)

        low, high = (2 * ((rows_count - 1) * k // 3) for k in (third, third + 1))
        loop(high - low, lambda i: one(low + i))

    def others(body, after=()):
        def one(i):
            hops = 1 + i // 2
            origin = row + hops * (1 - 2 * lax.rem(i, 2))
            above, below = rows_count - 1 - row, row
            done = jnp.minimum((i + 2) // 2, above) + jnp.minimum((i + 1) // 2, below)

            @pl.when((origin >= 0) & (origin < rows_count))
            def _():
                body(origin)
                for number, action in after:
                    pl.when(done == number)(action)

        loop(2 * (rows_count - 1), one)

    def finish_flow(flow, limit=None):
        limit = rows_count if limit is None else limit

        def one(origin):
            @pl.when((origin <= row) & (row + 1 < rows_count) & (row - origin < limit))
            def _():
                line_copy(flow, origin, True).wait_send()

            @pl.when((origin >= row) & (row >= 1) & (origin - row < limit))
            def _():
                line_copy(flow, origin, False).wait_send()

            @pl.when(origin != row)
            def _():
                if flow < 2:
                    for step in direct_steps:
                        plane_copy(flow, origin, step).wait_send()
                    if balanced:
                        for half in range(2):
                            half_copy(flow, origin, half).wait_send()
                if flow == 4:
                    for step in [0] + steps:
                        engine_copy(origin, step).wait_send()

        loop(rows_count, one)

    def own_stores(flow, own):
        return [
            pltpu.make_async_copy(
                own.at[:, pl.ds(i * part, part)], flows[flow].at[row, i], store.at[flow * count + i]
            )
            for i in range(count)
        ]

    def scatter(kind, step):
        peer = partner(me, step, count)[0]
        return pltpu.make_async_remote_copy(
            src_ref=term.at[peer],
            dst_ref=arrived.at[kind, step],
            send_sem=send.at[kind, step],
            recv_sem=recv.at[kind, step],
            device_id=at(section, peer),
            device_id_type=MESH,
        )

    def gather(number, step, target):
        peer = partner(me, step, count)[0]
        return pltpu.make_async_remote_copy(
            src_ref=parts.at[number, 0],
            dst_ref=parts.at[number, step],
            send_sem=part_send.at[number, step],
            recv_sem=part_recv.at[number, step],
            device_id=at(target, peer),
            device_id_type=MESH,
        )

    def back(number, step):
        return pltpu.make_async_remote_copy(
            src_ref=parts.at[number, step],
            dst_ref=parts.at[number, step],
            send_sem=back_send.at[number, step],
            recv_sem=back_recv.at[number, step],
            device_id=at(1 - section, me),
            device_id_type=MESH,
        )

    def place(number, step, target):
        owner = partner(me, step, count)[1]
        target[:, tile_of(owner, part)] = parts[number, step]

    def reduce(kind, number, with_input):
        for step in steps:
            scatter(kind, step).wait_recv()

        def rows_of(i):
            rows = tile_of(i, row_tile)
            total = term[me, rows, :].astype(F32)
            if with_input:
                total = total + xv[rows, tile_of(me, part)].astype(F32)
            for step in steps:
                total = total + arrived[kind, step, rows, :].astype(F32)
            parts[number, 0, rows, :] = total.astype(BF16)

        loop(row_tiles, rows_of)

    def finish_sends(kind):
        for step in steps:
            scatter(kind, step).wait_send()

    def to_other_section(number):
        for step in steps[::-1] + [0]:
            gather(number, step, 1 - section).start()

    def from_own_section(number, target):
        place(number, 0, target)
        for step in steps:
            back(number, step).wait_recv()
            place(number, step, target)
        for step in [0] + steps:
            gather(number, step, 1 - section).wait_send()

    def from_other_section(number, target):
        gather(number, 0, 1 - section).wait_recv()
        place(number, 0, target)
        for step in steps:
            gather(number, step, 1 - section).wait_recv()
            back(number, step).start()
            place(number, step, target)

    def finish_back(number):
        for step in steps:
            back(number, step).wait_send()

    def start_within(number):
        for step in steps[::-1]:
            gather(number, step, section).start()

    def finish_within(number, target):
        place(number, 0, target)
        for step in steps:
            gather(number, step, section).wait_recv()
            place(number, step, target)
        for step in steps:
            gather(number, step, section).wait_send()

    def each_chunk(kind, compute, between=None, sends=True):
        def chunk(i):
            step = count - 1 - i
            owner = partner(me, step, count)[0]
            loop(part // TILE, lambda j: compute(owner, j))

            @pl.when((step > 0) & sends)
            def _():
                scatter(kind, step).start()

            if between is not None:
                pl.when(i == count // 2 - 1)(between)

        loop(count, chunk)

    lane = lanes_of((1, LANES)).astype(F32)
    exponent = jnp.where(lane < ROT // 2, lane, lane - ROT // 2)
    frequency = jnp.exp(exponent * (-2.0 * math.log(10000.0) / ROT))
    row_index = lax.broadcasted_iota(jnp.int32, (length, length), 0)
    column_index = lax.broadcasted_iota(jnp.int32, (length, length), 1)

    def segments_of(values):
        across = values.astype(F32)
        down = jnp.sum(jnp.where(row_index == column_index, across, 0.0), axis=1, keepdims=True)
        return across, down

    def fill_tables(slot, values_of):
        for b in range(batch):
            rows = pl.ds(b * length, length)
            across, down = segments_of(values_of(b))
            number_of = jnp.sum((across < down).astype(F32), axis=1, keepdims=True)
            index = lax.broadcasted_iota(jnp.int32, (length, 1), 0).astype(F32)
            angles = (index - number_of) * frequency
            inside = lanes_of((length, LANES)) < ROT
            tables[slot, rows, :LANES] = jnp.where(inside, jnp.cos(angles), 1.0)
            tables[slot, rows, LANES:] = jnp.where(inside, jnp.sin(angles), 0.0)

    fill_tables(row, lambda b: seg_row[b : b + 1, :])

    def softmax(projected, values, b, h):
        rows, columns = tile_of(b, length), tile_of(h, HEAD)
        across, down = segments_of(values)
        allowed = (across == down) & (column_index <= row_index)
        scores = dot_nt(projected[0, rows, columns], projected[1, rows, columns]) * scale
        scores = jnp.where(allowed, scores, -jnp.inf)
        row_max = jnp.max(scores, axis=-1, keepdims=True)
        total = jnp.sum(jnp.exp(scores - row_max), axis=-1, keepdims=True)
        return jnp.exp(scores - (row_max + jnp.log(total)))

    def attend(prob, projected, target, b, h):
        rows, columns = tile_of(b, length), tile_of(h, HEAD)
        target[rows, columns] = dot(prob.astype(BF16), projected[2, rows, columns]).astype(BF16)

    def attend_backward(prob, projected, slot, target, b, h):
        rows, columns = tile_of(b, length), tile_of(h, HEAD)
        cosine, sine = tables[slot, rows, :LANES], tables[slot, rows, LANES:]
        queries, keys, values = (projected[k, rows, columns] for k in range(3))
        d_context = dctx[rows, columns]
        d_values = dot_tn(prob.astype(BF16), d_context)
        d_probs = dot_nt(d_context, values)
        delta = jnp.sum(prob * d_probs, axis=-1, keepdims=True)
        d_scores = (prob * (d_probs - delta) * scale).astype(BF16)
        for k, gradient in ((0, dot(d_scores, keys)), (1, dot_tn(d_scores, queries))):
            first = unrotated(gradient[:, :LANES], cosine, sine)
            start = pl.multiple_of(h * HEAD, HEAD)
            target[k, rows, pl.ds(start, LANES)] = first.astype(BF16)
            start = pl.multiple_of(h * HEAD + LANES, LANES)
            target[k, rows, pl.ds(start, HEAD - LANES)] = gradient[:, LANES:].astype(BF16)
        target[2, rows, columns] = d_values.astype(BF16)

    def each_pair(body):
        def row_of(b):
            for h in range(heads):
                body(b, h)

        loop(batch, row_of)

    def project(projected, slot):
        def rotary_head(i):
            which, h = i // heads, lax.rem(i, heads)
            tile = dot(attn_in[...], w3[which, :, tile_of(h, HEAD)])
            first = rotated(tile[:, :LANES], tables[slot, :, :LANES], tables[slot, :, LANES:])
            start = pl.multiple_of(h * HEAD, HEAD)
            projected[which, :, pl.ds(start, LANES)] = first.astype(BF16)
            start = pl.multiple_of(h * HEAD + LANES, LANES)
            projected[which, :, pl.ds(start, HEAD - LANES)] = tile[:, LANES:].astype(BF16)

        def value_head(h):
            columns = tile_of(h, HEAD)
            projected[2, :, columns] = dot(attn_in[...], w3[2, :, columns]).astype(BF16)

        loop(2 * heads, rotary_head)
        loop(heads, value_head)

    def segment_copy(step):
        return pltpu.make_async_remote_copy(
            src_ref=seg_row,
            dst_ref=segments.at[row],
            send_sem=segment_send.at[step],
            recv_sem=segment_recv.at[step],
            device_id={"dp": lax.rem(row + step, rows_count)},
            device_id_type=MESH,
        )

    def d_context_head(h):
        dctx[:, tile_of(h, HEAD)] = dot_nt(gbv[...], wo[tile_of(h, HEAD), :]).astype(BF16)

    def meet():
        pl.semaphore_wait(barrier, 2 * count - 1 + rows_count - 1)
        for step in range(1, rows_count):
            segment_copy(step).start()


    @pl.when(section == 0)
    def _():
        x_load.wait()

    @pl.when(section == 1)
    def _():
        meet()
        start_flow(4, x_hbm)
        go_load.wait()
        out_load.wait()
        loop(heads, d_context_head)
        hop(4, 1, send_engine_first)
        fc2_load.wait()

        def d_act_tile(i):
            columns = tile_of(i, TILE)
            slope[:, columns] = dot_nt(gbv[...], w2[columns, :])

        loop(hidden_width // TILE, d_act_tile)
        hop(4, 2)
        hop(4, 3)
        start_flow(1, gbv)
        hop(1, 1)
        hop(1, 2)
        from_other_section(0, xv)
        start_flow(0, xv)
        for third in range(3):
            thirds(third, send_engine_later)

    for copy in own_stores(0, xv):
        copy.start()

    def norm_rows(i):
        rows = tile_of(i, row_tile)
        normed, mean, inv_std = row_norm(xv[rows, :].astype(F32))
        means[rows, :] = mean
        inv_stds[rows, :] = inv_std
        attn_in[rows, :] = (normed * gains[0:1, :] + biases[0:1, :]).astype(BF16)
        mlp_in[rows, :] = (normed * gains[1:2, :] + biases[1:2, :]).astype(BF16)

    loop(row_tiles, norm_rows)

    for copy in qkv_loads:
        copy.wait()
    project(qkv, row)

    def own_attention(b, h):
        prob = softmax(qkv, seg_row[pl.ds(b, 1), :], b, h)
        probs[b * heads + h] = prob
        attend(prob, qkv, context, b, h)

    each_pair(own_attention)

    @pl.when(section == 1)
    def _():
        hop(0, 1, send_plane_of(0))


    def fc1_block(i):
        fc1_load(i).wait()

        def fc1_tile(j):
            columns = tile_of(i * (block // TILE) + j, TILE)
            value, derivative = gelu_parts(dot(mlp_in[...], w1[:, columns]))
            act[:, columns] = value.astype(BF16)

            @pl.when(section == 0)
            def _():
                slope[:, columns] = derivative

            @pl.when(section == 1)
            def _():
                dh[:, columns] = (slope[:, columns] * derivative).astype(BF16)

        loop(block // TILE, fc1_tile)

    loop(blocks, fc1_block)

    @pl.when(section == 1)
    def _():
        hop(0, 2, send_plane_of(0))

    @pl.when(section == 0)
    def _():
        out_load.wait()
        fc2_load.wait()
        go_load.wait()

    tiles = hidden_width // TILE

    def act_store(origin, i):
        columns = tile_of(i, TILE)
        return pltpu.make_async_copy(
            act_rest.at[:, columns], act_all.at[origin, :, columns], rest_store.at[0, i]
        )

    def dh_store(origin, i):
        columns = tile_of(i, TILE)
        return pltpu.make_async_copy(
            act_rest.at[:, columns], dh_all.at[origin, :, columns], rest_store.at[0, i]
        )

    def slope_store(origin, i):
        columns = tile_of(i, TILE)
        return pltpu.make_async_copy(
            slope_rest.at[:, columns], slope_all.at[origin, :, columns], rest_store.at[1, i]
        )

    def load_block(flow, origin):
        if flow == 0:

            @pl.when(section == 0)
            def _():
                for step in [0] + steps:
                    engine_copy(origin, step).wait_recv()

            pl.when(section == 1)(lambda: wait_plane(flow, origin))
        else:
            wait_plane(flow, origin)

        copies = [
            pltpu.make_async_copy(
                flows[flow].at[origin, i], attn_in.at[:, pl.ds(i * part, part)], rest_load.at[i]
            )
            for i in range(count)
        ]
        for copy in copies:
            copy.start()
        return copies

    def attention_stores(origin):
        return [
            pltpu.make_async_copy(qkv_rest, qkv_all.at[origin], rest_load.at[count + 1]),
            pltpu.make_async_copy(context_rest, context_all.at[origin], rest_load.at[count + 2]),
        ]

    def rest_forward(origin):
        for copy in load_block(0, origin):
            copy.wait()

        def norm_rows(i):
            rows = tile_of(i, row_tile)
            normed, mean, inv_std = row_norm(attn_in[rows, :].astype(F32))
            first = lanes_of((row_tile, LANES)) == 0
            stats_all[origin, rows, :] = jnp.where(first, mean, inv_std)
            mlp_in[rows, :] = (normed * gains[1:2, :] + biases[1:2, :]).astype(BF16)
            attn_in[rows, :] = (normed * gains[0:1, :] + biases[0:1, :]).astype(BF16)

        loop(row_tiles, norm_rows)

        @pl.when(section == 0)
        def _():
            fill_tables(origin, lambda b: segments[origin, b : b + 1, :])
            project(qkv_rest, origin)

            def attention(b, h):
                prob = softmax(qkv_rest, segments[origin, pl.ds(b, 1), :], b, h)
                attend(prob, qkv_rest, context_rest, b, h)

            each_pair(attention)
            for copy in attention_stores(origin):
                copy.start()

        def tile(i):
            columns = tile_of(i, TILE)
            value, derivative = gelu_parts(dot(mlp_in[...], w1[:, columns]))
            act_rest[:, columns] = value.astype(BF16)
            slope_rest[:, columns] = derivative
            act_store(origin, i).start()
            slope_store(origin, i).start()

        loop(tiles, tile)

        def wait(i):
            act_store(origin, i).wait()
            slope_store(origin, i).wait()

        loop(tiles, wait)

        @pl.when(section == 0)
        def _():
            for copy in attention_stores(origin):
                copy.wait()

    def rest_backward(origin):
        copies = load_block(1, origin)
        slope_load = pltpu.make_async_copy(slope_all.at[origin], slope_rest, rest_load.at[count])
        slope_load.start()
        for copy in copies + [slope_load]:
            copy.wait()

        def tile(i):
            columns = tile_of(i, TILE)
            d_act = dot_nt(attn_in[...], w2[columns, :])
            act_rest[:, columns] = (d_act * slope_rest[:, columns]).astype(BF16)
            dh_store(origin, i).start()

        qkv_load = pltpu.make_async_copy(qkv_all.at[origin], qkv_rest, rest_load.at[count + 1])
        dproj_store = pltpu.make_async_copy(
            dproj_rest, dproj_all.at[origin], rest_load.at[count + 2]
        )
        far = (section == 0) & ((origin - row > near) | (row - origin > near))
        pl.when(far)(qkv_load.start)
        loop(tiles, tile)

        @pl.when(far)
        def _():
            qkv_load.wait()

            def head(h):
                columns = tile_of(h, HEAD)
                dctx[:, columns] = dot_nt(attn_in[...], wo[columns, :]).astype(BF16)

            loop(heads, head)

            def attention(b, h):
                prob = softmax(qkv_rest, segments[origin, pl.ds(b, 1), :], b, h)
                attend_backward(prob, qkv_rest, origin, dproj_rest, b, h)

            each_pair(attention)
            dproj_store.start()
            dproj_store.wait()

        loop(tiles, lambda i: dh_store(origin, i).wait())

    def out_tile(owner, j):
        columns = tile_of(owner * (part // TILE) + j, TILE)
        total = dot(context[...], wo[:, columns]) + dot(act[...], w2[:, columns])
        term[owner, :, tile_of(j, TILE)] = total.astype(BF16)

    layer_store = pltpu.make_async_copy(other, layer_out, store.at[2 * count + 4])
    grad_store = pltpu.make_async_copy(slope, input_grad, store.at[2 * count + 5])
    stats_store = pltpu.make_async_copy(stats_all, stats_out, store.at[2 * count + 6])

    @pl.when(section == 0)
    def _():
        meet()
        each_chunk(0, out_tile)
        reduce(0, 0, True)
        to_other_section(0)
        finish_sends(0)
        for step in range(1, rows_count):
            segment_copy(step).wait_recv()
        others(rest_forward)
        from_own_section(0, other)
        layer_store.start()
        from_other_section(1, full)

        def gradient_rows(i):
            rows = tile_of(i, row_tile)
            normed, _, inv_std = row_norm(other[rows, :].astype(F32))
            dx = row_norm_backward(full[rows, :].astype(F32), normed, inv_std)
            gbv[rows, :] = (gbv[rows, :].astype(F32) + dx).astype(BF16)

        loop(row_tiles, gradient_rows)
        start_flow(1, gbv)
        finish_back(1)

        def d_hidden_tile(i):
            columns = tile_of(i, TILE)
            d_act = dot_nt(gbv[...], w2[columns, :])
            dh[:, columns] = (d_act * slope[:, columns]).astype(BF16)

        loop(hidden_width // TILE, d_hidden_tile)
        loop(heads, d_context_head)
        hop(1, 1, send_plane_of(1))


    each_pair(lambda b, h: attend_backward(probs[b * heads + h], qkv, row, dproj, b, h))

    @pl.when(section == 1)
    def _():
        start_flow(3, dproj)
        hop(1, 3)

    def gradient_tile(owner, j):
        columns = tile_of(owner * (part // TILE) + j, TILE)
        d_attn = dot_nt(dproj[0], w3[0, columns, :])
        d_attn = d_attn + dot_nt(dproj[1], w3[1, columns, :])
        d_attn = d_attn + dot_nt(dproj[2], w3[2, columns, :])
        d_mlp = dot_nt(dh[...], w1[columns, :])
        normed = (xv[:, columns].astype(F32) - means[...]) * inv_stds[...]
        total = d_attn * gains[0:1, columns] + d_mlp * gains[1:2, columns]
        term[owner, :, tile_of(j, TILE)] = total.astype(BF16)
        vectors[0:1, columns] = jnp.sum(d_attn * normed, axis=0, keepdims=True)
        vectors[1:2, columns] = jnp.sum(d_mlp * normed, axis=0, keepdims=True)
        vectors[2:3, columns] = jnp.sum(d_attn, axis=0, keepdims=True)
        vectors[3:4, columns] = jnp.sum(d_mlp, axis=0, keepdims=True)

    def second_hop():
        @pl.when(section == 0)
        def _():
            hop(1, 2, send_plane_of(1))

    each_chunk(1, gradient_tile, second_hop, section == 1)

    outs = [
        (act, act_all.at[row]),
        (context, context_all.at[row]),
        (dh, dh_all.at[row]),
        (dproj, dproj_all.at[row]),
    ]
    stores = own_stores(1, gbv)
    stores += [
        pltpu.make_async_copy(a, b, store.at[2 * count + i]) for i, (a, b) in enumerate(outs)
    ]
    for copy in stores:
        copy.start()

    def sum_copy(step):
        peer = partner(me, step, count)[0]
        return pltpu.make_async_remote_copy(
            src_ref=vectors,
            dst_ref=plane_vectors.at[step],
            send_sem=sum_send.at[step],
            recv_sem=sum_recv.at[step],
            device_id=at(section, peer),
            device_id_type=MESH,
        )

    mine = width // rows_count

    def slice_copy(step):
        target = lax.rem(row + step, rows_count)
        return pltpu.make_async_remote_copy(
            src_ref=plane_vectors.at[0, :, tile_of(target, mine)],
            dst_ref=slices.at[step],
            send_sem=slice_send.at[step],
            recv_sem=slice_recv.at[step],
            device_id={"dp": target},
            device_id_type=MESH,
        )

    for step in steps:
        sum_copy(step).start()

    def sum_plane():
        total = vectors[...]
        for step in steps:
            sum_copy(step).wait_recv()
            total = total + plane_vectors[step]
        plane_vectors[0] = total
        for step in range(1, rows_count):
            slice_copy(step).start()

    def sum_line():
        total = plane_vectors[0, :, tile_of(row, mine)]
        for step in range(1, rows_count):
            slice_copy(step).wait_recv()
            total = total + slices[step]
        gain_grads[...] = total[:2]
        bias_grads[...] = total[2:]
        for step in range(1, rows_count):
            slice_copy(step).wait_send()
        for step in steps:
            sum_copy(step).wait_send()

    def own_stats(i):
        rows = tile_of(i, row_tile)
        first = lanes_of((row_tile, LANES)) == 0
        stats_all[row, rows, :] = jnp.where(first, means[rows, :], inv_stds[rows, :])

    loop(row_tiles, own_stats)

    def input_gradient():
        def rows_of(i):
            rows = tile_of(i, row_tile)
            inv_std = inv_stds[rows, :]
            normed = (xv[rows, :].astype(F32) - means[rows, :]) * inv_std
            dx = row_norm_backward(full[rows, :].astype(F32), normed, inv_std)
            slope[rows, :] = gbv[rows, :].astype(F32) + dx

        loop(row_tiles, rows_of)
        grad_store.start()

    @pl.when(section == 0)
    def _():
        stats_store.start()
        thirds(0, relay_plane_of(1))
        hop(1, 3, send_plane_of(1))
        start_flow(3, dproj)
        thirds(1, relay_plane_of(1))

        def after_first():
            thirds(2, relay_plane_of(1))
            for step in steps[::-1]:
                scatter(1, step).start()
            sum_plane()
            hop(3, 1, limit=near)

        def after_second():
            reduce(1, 2, False)
            start_within(2)

        others(rest_backward, [(1, after_first), (2, after_second)])
        finish_within(2, full)
        finish_sends(1)
        input_gradient()
        hop(3, 2, limit=near)

    @pl.when(section == 1)
    def _():
        finish_back(0)
        reduce(1, 1, False)
        to_other_section(1)
        thirds(0, relay_plane_of(0))
        hop(0, 3, send_plane_of(0))
        thirds(1, relay_plane_of(0))
        finish_sends(1)
        each_chunk(0, out_tile, None, False)
        hop(3, 1)

        def after_first():
            thirds(2, relay_plane_of(0))
            from_own_section(1, full)
            for third in range(3):
                thirds(third, send_plane_of(1))
            sum_plane()

        others(rest_forward, [(1, after_first)])
        stats_store.start()
        for step in steps[::-1]:
            scatter(0, step).start()
        input_gradient()
        start_flow(2, context)
        hop(3, 2)
        for third in range(3):
            thirds(third, relay_plane_of(1))

        def after_first_backward():
            hop(2, 1)
            reduce(0, 3, True)
            start_within(3)

        others(rest_backward, [(1, after_first_backward), (2, lambda: hop(2, 2))])
        finish_within(3, other)
        layer_store.start()
        hop(3, 3)
        hop(2, 3)
        finish_sends(0)

    sum_line()
    for copy in own_stores(0, xv) + stores + [layer_store, grad_store, stats_store]:
        copy.wait()
    finish_flow(1)
    pl.when(section == 0)(lambda: finish_flow(3, near))

    @pl.when(section == 1)
    def _():
        for step in range(1, rows_count):
            segment_copy(step).wait_recv()
        for flow in (0, 2, 3, 4):
            finish_flow(flow)

    for step in range(1, rows_count):
        segment_copy(step).wait_send()


def chain(block_input, grad_output, segment_ids, weights):
    w_qkv, w_out, w_fc1, w_fc2, gains, biases = weights
    batch, length, width = block_input.shape
    tokens = batch * length
    count = lax.axis_size("tensor")
    inner, hidden = w_qkv.shape[2], w_fc1.shape[1]
    part = width // count
    heads = inner // HEAD
    anywhere, vmem = pl.BlockSpec(memory_space=pl.ANY), pl.BlockSpec(memory_space=pltpu.VMEM)
    like = jax.ShapeDtypeStruct
    rows_count = lax.axis_size("dp")
    wide, narrow = (tokens, width), (tokens, inner)
    dma = pltpu.SemaphoreType.DMA
    return pl.pallas_call(
        functools.partial(chain_kernel, count, batch),
        out_shape=[
            like(wide, BF16),
            like(wide, F32),
            like((2, width // rows_count), F32),
            like((2, width // rows_count), F32),
            like((rows_count, count, tokens, part), BF16),
            like((rows_count, count, tokens, part), BF16),
            like((rows_count, tokens, inner), BF16),
            like((rows_count, 3, tokens, inner), BF16),
            like((rows_count, tokens, hidden), BF16),
            like((rows_count, tokens, hidden), BF16),
            like((rows_count, tokens, LANES), F32),
            like((rows_count, tokens, hidden), F32),
            like((rows_count, tokens, part), BF16),
            like((rows_count, 3, tokens, inner), BF16),
        ],
        in_specs=[anywhere, anywhere, vmem] + [anywhere] * 4 + [vmem, vmem],
        out_specs=[anywhere, anywhere, vmem, vmem] + [anywhere] * 6 + [anywhere] * 4,
        scratch_shapes=[
            pltpu.VMEM((3, width, inner), BF16),
            pltpu.VMEM((inner, width), BF16),
            pltpu.VMEM((width, hidden), BF16),
            pltpu.VMEM((hidden, width), BF16),
            pltpu.VMEM(wide, BF16),
            pltpu.VMEM(wide, BF16),
            pltpu.VMEM(wide, BF16),
            pltpu.VMEM(wide, BF16),
            pltpu.VMEM(wide, BF16),
            pltpu.VMEM((3, tokens, inner), BF16),
            pltpu.VMEM(narrow, BF16),
            pltpu.VMEM((batch * heads, length, length), F32),
            pltpu.VMEM((tokens, hidden), BF16),
            pltpu.VMEM((tokens, hidden), F32),
            pltpu.VMEM((tokens, hidden), BF16),
            pltpu.VMEM(narrow, BF16),
            pltpu.VMEM((3, tokens, inner), BF16),
            pltpu.VMEM((tokens, 1), F32),
            pltpu.VMEM((tokens, 1), F32),
            pltpu.VMEM((rows_count, tokens, 2 * LANES), F32),
            pltpu.VMEM((count, tokens, part), BF16),
            pltpu.VMEM((2, count, tokens, part), BF16),
            pltpu.VMEM((4, count, tokens, part), BF16),
            pltpu.VMEM(wide, BF16),
            pltpu.VMEM((tokens, hidden), BF16),
            pltpu.VMEM((tokens, hidden), F32),
            pltpu.VMEM((rows_count, tokens, LANES), F32),
            pltpu.VMEM((4, width), F32),
            pltpu.VMEM((count, 4, width), F32),
            pltpu.VMEM((rows_count, 4, width // rows_count), F32),
            pltpu.VMEM((rows_count, batch, length), jnp.int32),
            pltpu.VMEM((3, tokens, inner), BF16),
            pltpu.VMEM((3, tokens, inner), BF16),
            pltpu.VMEM(narrow, BF16),
            dma((11,)),
            dma((2 * count + 7,)),
            dma((2, count)),
            dma((2, count)),
            dma((4, count)),
            dma((4, count)),
            dma((2, count)),
            dma((2, count)),
            dma((5, 2, rows_count)),
            dma((5, rows_count)),
            dma((2, rows_count, count)),
            dma((2, rows_count, count)),
            dma((count + 3,)),
            dma((2, hidden // TILE)),
            dma((count,)),
            dma((count,)),
            dma((rows_count,)),
            dma((rows_count,)),
            dma((rows_count, count)),
            dma((rows_count,)),
            dma((rows_count,)),
        ],
        compiler_params=pltpu.CompilerParams(
            collective_id=0, has_side_effects=True, vmem_limit_bytes=67_043_328
        ),
        name="chain",
    )(
        block_input.reshape(wide),
        grad_output.reshape(wide),
        segment_ids,
        jnp.transpose(w_qkv, (1, 0, 2)),
        w_out,
        w_fc1,
        w_fc2,
        gains,
        biases,
    )


def weight_kernel(*refs):
    (
        x_all, gb_all, stats_all, context_all, dproj_all, act_all, dh_all, gains, biases,
        layer_in, grad_in, gain_in, bias_in,
        g_qkv, g_out, g_fc1, g_fc2, layer_out, input_grad, gain_out, bias_out,
        x_mine, gb_mine, context, dproj, act, attn_t, mlp_t, r_qkv, r_out, r_fc1, r_fc2,
        layer, grad, stats, load, act_load, dh_load, store, through, gb_load, x_load,
    ) = refs
    blocks, tokens, mine = x_mine.shape
    rows = blocks * tokens
    part = x_all.shape[3]
    inner, hidden = context.shape[2], act.shape[2]
    start = lax.axis_index("dp") * mine
    chunk, offset = start // part, pl.multiple_of(lax.rem(start, part), LANES)
    piece = hidden // 4

    def slice_loads(source, target, sems):
        return [
            pltpu.make_async_copy(
                source.at[i, chunk, :, pl.ds(offset, mine)], target.at[i], sems.at[i]
            )
            for i in range(blocks)
        ]

    def piece_load(source, target, sems, i):
        columns = pl.ds(i * piece, piece)
        return pltpu.make_async_copy(source.at[:, :, columns], target.at[:, :, columns], sems.at[i])

    gb_loads = slice_loads(gb_all, gb_mine, gb_load)
    x_loads = slice_loads(x_all, x_mine, x_load)
    stats_load = pltpu.make_async_copy(stats_all, stats, load.at[0])
    context_load = pltpu.make_async_copy(context_all, context, load.at[2])
    dproj_load = pltpu.make_async_copy(dproj_all, dproj, load.at[3])
    act_loads = [piece_load(act_all, act, act_load, i) for i in range(4)]
    dh_loads = [piece_load(dh_all, act, dh_load, i) for i in range(4)]
    gain_out[...] = gain_in[...]
    bias_out[...] = bias_in[...]
    ins = [
        pltpu.make_async_copy(layer_in, layer, through.at[0]),
        pltpu.make_async_copy(grad_in, grad, through.at[1]),
    ]
    outs = [
        pltpu.make_async_copy(layer, layer_out, through.at[2]),
        pltpu.make_async_copy(grad, input_grad, through.at[3]),
    ]
    early = gb_loads + [context_load] + act_loads[:1] + x_loads + [stats_load]
    for copy in early + act_loads[1:] + [dproj_load] + ins:
        copy.start()

    def transposed_rows(i):
        columns = tile_of(i, LANES)
        mean = stats[:, :, 0:1].reshape(rows, 1)
        inv_std = stats[:, :, 1:2].reshape(rows, 1)
        normed = (x_mine[:, :, columns].reshape(rows, LANES).astype(F32) - mean) * inv_std
        whole = tile_of(chunk * (part // LANES) + offset // LANES + i, LANES)
        for j, target in enumerate((attn_t, mlp_t)):
            scaled = normed * gains[j : j + 1, whole] + biases[j : j + 1, whole]
            target[columns, :] = scaled.astype(BF16).T

    def out_copy(source, target, index):
        return pltpu.make_async_copy(source, target, store.at[index])

    for copy in gb_loads + [context_load]:
        copy.wait()
    gb_rows = gb_mine[...].reshape(rows, mine)

    def out_tile(i):
        tile = tile_of(i, TILE)
        r_out[tile, :] = dot_tn(context[:, :, tile].reshape(rows, TILE), gb_rows)

    loop(inner // TILE, out_tile)
    copies = [out_copy(r_out, g_out, 0)]
    copies[0].start()

    def fc2_copy(i):
        tile = tile_of(i, TILE)
        return out_copy(r_fc2.at[tile, :], g_fc2.at[tile, :], 1 + i)

    def fc2_tile(i):
        tile = tile_of(i, TILE)
        r_fc2[tile, :] = dot_tn(act[:, :, tile].reshape(rows, TILE), gb_mine[...].reshape(rows, mine))
        fc2_copy(i).start()

    per = piece // TILE
    for i in range(4):
        act_loads[i].wait()
        loop(per, lambda j: fc2_tile(i * per + j))
        dh_loads[i].start()
    for copy in ins:
        copy.wait()
    for copy in outs:
        copy.start()
    for copy in x_loads + [stats_load]:
        copy.wait()
    loop(mine // LANES, transposed_rows)

    def fc1_copy(i):
        tile = tile_of(i, TILE)
        return out_copy(r_fc1.at[:, tile], g_fc1.at[:, tile], 1 + hidden // TILE + i)

    def fc1_tile(i):
        tile = tile_of(i, TILE)
        r_fc1[:, tile] = dot(mlp_t[...], act[:, :, tile].reshape(rows, TILE))
        fc1_copy(i).start()

    for copy in dh_loads:
        copy.wait()
    loop(hidden // TILE, fc1_tile)
    dproj_load.wait()
    per = inner // TILE

    def qkv_copy(i):
        which, tile = i // per, tile_of(lax.rem(i, per), TILE)
        return out_copy(r_qkv.at[which, :, tile], g_qkv.at[which, :, tile], 1 + 2 * (hidden // TILE) + i)

    def qkv_tile(i):
        which, tile = i // per, tile_of(lax.rem(i, per), TILE)
        r_qkv[which, :, tile] = dot(attn_t[...], dproj[:, which, :, tile].reshape(rows, TILE))
        qkv_copy(i).start()

    loop(3 * per, qkv_tile)
    for copy in copies + outs:
        copy.wait()
    loop(hidden // TILE, lambda i: fc2_copy(i).wait())
    loop(hidden // TILE, lambda i: fc1_copy(i).wait())
    loop(3 * per, lambda i: qkv_copy(i).wait())


def weight_gradients(
    x_all, gb_all, stats, context_all, dproj_all, act_all, dh_all, gains, biases, *through
):
    blocks, count, tokens, part = x_all.shape
    mine = count * part // lax.axis_size("dp")
    inner, hidden = context_all.shape[2], act_all.shape[2]
    anywhere, vmem = pl.BlockSpec(memory_space=pl.ANY), pl.BlockSpec(memory_space=pltpu.VMEM)
    shapes = [(3, mine, inner), (inner, mine), (mine, hidden), (hidden, mine)]
    dma = pltpu.SemaphoreType.DMA
    return pl.pallas_call(
        weight_kernel,
        out_shape=[jax.ShapeDtypeStruct(shape, F32) for shape in shapes]
        + [jax.ShapeDtypeStruct(value.shape, value.dtype) for value in through],
        in_specs=[anywhere] * 7
        + [vmem, vmem, anywhere, anywhere, vmem, vmem],
        out_specs=[anywhere] * 6 + [vmem, vmem],
        scratch_shapes=[
            pltpu.VMEM((blocks, tokens, mine), BF16),
            pltpu.VMEM((blocks, tokens, mine), BF16),
            pltpu.VMEM((blocks, tokens, inner), BF16),
            pltpu.VMEM((blocks, 3, tokens, inner), BF16),
            pltpu.VMEM((blocks, tokens, hidden), BF16),
            pltpu.VMEM((mine, blocks * tokens), BF16),
            pltpu.VMEM((mine, blocks * tokens), BF16),
        ]
        + [pltpu.VMEM(shape, F32) for shape in shapes]
        + [pltpu.VMEM(value.shape, value.dtype) for value in through[:2]]
        + [pltpu.VMEM(stats.shape, F32)]
        + [
            dma((4,)),
            dma((4,)),
            dma((4,)),
            dma((1 + 2 * (hidden // TILE) + 3 * (inner // TILE),)),
            dma((4,)),
            dma((blocks,)),
            dma((blocks,)),
        ],
        compiler_params=pltpu.CompilerParams(vmem_limit_bytes=67_043_328),
        name="weights",
    )(x_all, gb_all, stats, context_all, dproj_all, act_all, dh_all, gains, biases, *through)


def shards(
    block_input, grad_output, segment_ids, w_qkv, w_out, w_fc1, w_fc2, norm_gains, norm_biases
):
    batch, length, width = block_input.shape
    weights = (w_qkv[0], w_out[0], w_fc1[0], w_fc2[0], norm_gains[0], norm_biases[0])
    (layer_out, input_grads, gain_grads, bias_grads, x_all, gb_all, context, d_proj, activated, d_hidden, stats, *_) = chain(
        block_input, grad_output, segment_ids, weights
    )
    g_qkv, g_out, g_fc1, g_fc2, layer_out, input_grads, gain_grads, bias_grads = weight_gradients(
        x_all, gb_all, stats, context, d_proj, activated, d_hidden, norm_gains[0], norm_biases[0],
        layer_out, input_grads, gain_grads, bias_grads,
    )
    shape = (1, batch, length, width)
    return (
        layer_out.reshape(shape),
        input_grads.reshape(shape),
        jnp.transpose(g_qkv, (1, 0, 2))[None],
        g_out[None],
        g_fc1[None],
        g_fc2[None],
        gain_grads[None],
        bias_grads[None],
    )


def solution(mesh):
    return jax.shard_map(
        shards,
        mesh=mesh,
        in_specs=(
            P("dp", None, None),
            P("dp", None, None),
            P("dp", None),
            P("section", None, None, "tensor"),
            P("section", "tensor", None),
            P("section", None, "tensor"),
            P("section", "tensor", None),
            P("section", None, None),
            P("section", None, None),
        ),
        out_specs=(
            P("section", "dp", None, None),
            P("section", "dp", None, None),
            P("section", "dp", None, "tensor"),
            P("section", "tensor", "dp"),
            P("section", "dp", "tensor"),
            P("section", "tensor", "dp"),
            P("section", None, "dp"),
            P("section", None, "dp"),
        ),
        check_vma=False,
    )
```

```python
import functools
import math

import jax
import jax.numpy as jnp
from jax import lax
from jax.experimental import pallas as pl
from jax.experimental.pallas import tpu as pltpu
from jax.sharding import PartitionSpec as P

HEAD = 256
ROT = 64
LANES = 128
TILE = 256
NORM_EPSILON = 1e-05
MESH = pl.DeviceIdType.MESH
BF16 = jnp.bfloat16
F32 = jnp.float32


def partner(index, step, count):
    if count & (count - 1):
        return lax.rem(index + step, count), lax.rem(index + count - step, count)
    bit = 1
    while bit < count:
        index = index + ((step // bit) % 2) * (bit - 2 * bit * ((index // bit) % 2))
        bit *= 2
    return index, index


def loop(count, body, unroll=1):
    lax.fori_loop(0, count, lambda i, carry: (body(i), carry)[1], 0, unroll=unroll)


def tile_of(i, size):
    return pl.ds(pl.multiple_of(i * size, size), size)


def dot(left, right):
    return jnp.dot(left, right, preferred_element_type=jnp.float32)


def dot_nt(left, right):
    return lax.dot_general(left, right, (((1,), (1,)), ((), ())), preferred_element_type=jnp.float32)


def dot_tn(left, right):
    return lax.dot_general(left, right, (((0,), (0,)), ((), ())), preferred_element_type=jnp.float32)


def gelu_parts(hidden):
    normal_cdf = 0.5 * (1.0 + lax.erf(hidden * (1.0 / math.sqrt(2.0))))
    density = jnp.exp(-0.5 * hidden * hidden) * (1.0 / math.sqrt(2.0 * math.pi))
    return (hidden * normal_cdf, normal_cdf + hidden * density)


def lanes_of(shape):
    return lax.broadcasted_iota(jnp.int32, shape, len(shape) - 1)


def rotated(tile, cosine, sine):
    half = ROT // 2
    left, right = pltpu.roll(tile, LANES - half, 1), pltpu.roll(tile, half, 1)
    lane = lanes_of(tile.shape)
    turned = jnp.where(lane < half, -left, right)
    return tile * cosine + turned * sine


def unrotated(tile, cosine, sine):
    half = ROT // 2
    scaled = tile * sine
    left, right = pltpu.roll(scaled, LANES - half, 1), pltpu.roll(scaled, half, 1)
    lane = lanes_of(tile.shape)
    turned = jnp.where(lane < half, left, jnp.where(lane < ROT, -right, 0.0))
    return tile * cosine + turned


def row_norm(values):
    mean = jnp.mean(values, axis=-1, keepdims=True)
    centred = values - mean
    inv_std = lax.rsqrt(jnp.mean(centred * centred, axis=-1, keepdims=True) + NORM_EPSILON)
    return centred * inv_std, mean, inv_std


def row_norm_backward(summed, normed, inv_std):
    return inv_std * (
        summed
        - jnp.mean(summed, axis=-1, keepdims=True)
        - normed * jnp.mean(summed * normed, axis=-1, keepdims=True)
    )


def chain_kernel(count, batch, *refs):
    (
        x_hbm, go_hbm, seg_row, w3_hbm, wo_hbm, w1_hbm, w2_hbm, gains, biases,
        layer_out, input_grad, gain_grads, bias_grads, x_all, gb_all, context_all, dproj_all, act_all, dh_all, stats_out,
        slope_all, relay_x, qkv_all,
        w3, wo, w1, w2, xv, other, gbv, attn_in, mlp_in, qkv, context, probs, act, slope, dh, dctx,
        dproj, means, inv_stds, tables, term, arrived, parts, full, act_rest, slope_rest,
        stats_all, vectors, plane_vectors, slices, segments, qkv_rest, dproj_rest, context_rest,
        load, store, send, recv, part_send, part_recv, back_send, back_recv,
        line_send, line_recv, plane_send, plane_recv, rest_load, rest_store, sum_send, sum_recv,
        slice_send, slice_recv, engine_send, segment_send, segment_recv,
    ) = refs
    section, me = lax.axis_index("section"), lax.axis_index("tensor")
    row, rows_count = lax.axis_index("dp"), lax.axis_size("dp")
    tokens, width = xv.shape
    length = tokens // batch
    heads = qkv.shape[2] // HEAD
    hidden_width = act.shape[1]
    part = width // count
    row_tile = 32 if tokens % 32 == 0 else 16
    row_tiles = tokens // row_tile
    scale = 1.0 / math.sqrt(HEAD)

    qkv_loads = [pltpu.make_async_copy(w3_hbm.at[k], w3.at[k], load.at[k]) for k in range(3)]
    blocks = 4
    block = hidden_width // blocks

    def fc1_load(i):
        columns = tile_of(i, block)
        return pltpu.make_async_copy(w1_hbm.at[:, columns], w1.at[:, columns], load.at[3 + i])

    out_load = pltpu.make_async_copy(wo_hbm, wo, load.at[7])
    fc2_load = pltpu.make_async_copy(w2_hbm, w2, load.at[8])
    x_load = pltpu.make_async_copy(x_hbm, xv, load.at[9])
    go_load = pltpu.make_async_copy(go_hbm, gbv, load.at[10])

    @pl.when(section == 0)
    def _():
        x_load.start()

    go_load.start()

    def start_out_loads():
        out_load.start()
        fc2_load.start()

    pl.when(section == 1)(start_out_loads)
    for copy in qkv_loads:
        copy.start()
    for i in range(blocks):
        fc1_load(i).start()
    pl.when(section == 0)(start_out_loads)

    def at(section, index):
        return {"section": section, "tensor": index}

    steps = list(range(1, count))
    barrier = pltpu.get_barrier_semaphore()
    for step in range(count):
        peer = partner(me, step, count)[0]
        pl.semaphore_signal(barrier, inc=1, device_id=at(1 - section, peer), device_id_type=MESH)
        if step:
            pl.semaphore_signal(barrier, inc=1, device_id=at(section, peer), device_id_type=MESH)

    for step in range(1, rows_count):
        pl.semaphore_signal(
            barrier,
            inc=1,
            device_id={"dp": lax.rem(row + step, rows_count)},
            device_id_type=MESH,
        )

    balanced = count == 4
    opposite = partner(me, count - 1, count)[0]
    flows = (x_all, gb_all)

    def place_of(flow, origin):
        return (
            lambda: x_all.at[origin, me],
            lambda: gb_all.at[origin, me],
            lambda: context_all.at[origin],
            lambda: dproj_all.at[origin],
            lambda: relay_x.at[origin, 0],
            lambda: gb_all.at[origin, opposite],
            lambda: relay_x.at[origin, 1],
        )[flow]()

    def line_copy(flow, origin, up, own=None):
        place = place_of(flow, origin)
        return pltpu.make_async_remote_copy(
            src_ref=place if own is None else own,
            dst_ref=place,
            send_sem=line_send.at[flow, int(up), origin],
            recv_sem=line_recv.at[flow, origin],
            device_id={"dp": row + (1 if up else -1)},
            device_id_type=MESH,
        )

    def plane_copy(flow, origin, step):
        peer = partner(me, step, count)[0]
        return pltpu.make_async_remote_copy(
            src_ref=flows[flow].at[origin, me],
            dst_ref=flows[flow].at[origin, me],
            send_sem=plane_send.at[flow, origin, step],
            recv_sem=plane_recv.at[flow, origin, step],
            device_id=at(section, peer),
            device_id_type=MESH,
        )

    direct_steps = [1, 2] if balanced else steps

    def send_plane(flow, origin):
        for step in direct_steps[::-1]:
            plane_copy(flow, origin, step).start()

    def half_copy(flow, origin, half):
        owner = partner(me, 1 + half, count)[1]
        place = flows[flow].at[origin, owner, pl.ds(half * (tokens // 2), tokens // 2), :]
        return pltpu.make_async_remote_copy(
            src_ref=place,
            dst_ref=place,
            send_sem=plane_send.at[flow, origin, 3 * half],
            recv_sem=plane_recv.at[flow, origin, 3 * half],
            device_id=at(section, partner(me, 2 - half, count)[0]),
            device_id_type=MESH,
        )

    def relay_plane(flow, origin):
        if balanced:
            for step in direct_steps:
                plane_copy(flow, origin, step).wait_recv()
            for half in range(2):
                half_copy(flow, origin, half).start()

    def wait_plane(flow, origin):
        if balanced:
            for half in range(2):
                half_copy(flow, origin, half).wait_recv()
        else:
            for step in steps:
                plane_copy(flow, origin, step).wait_recv()

    def send_plane_of(flow):
        return lambda origin: send_plane(flow, origin)

    def relay_plane_of(flow):
        return lambda origin: relay_plane(flow, origin)

    def engine_copy(origin, step):
        second = balanced and step == 3
        peer = me if second else partner(me, step, count)[0]
        return pltpu.make_async_remote_copy(
            src_ref=relay_x.at[origin, int(second)],
            dst_ref=x_all.at[origin, opposite if second else me],
            send_sem=engine_send.at[origin, step],
            recv_sem=plane_recv.at[0, origin, step],
            device_id=at(1 - section, peer),
            device_id_type=MESH,
        )

    def send_engine(origin):
        for step in steps[::-1] + [0]:
            engine_copy(origin, step).start()

    first_other = jnp.where(row == rows_count - 1, row - 1, row + 1)

    def send_engine_first(origin):
        pl.when(origin == first_other)(lambda: send_engine(origin))

    def send_engine_later(origin):
        pl.when(origin != first_other)(lambda: send_engine(origin))

    def start_flow(flow, own):
        if flow in (0, 1, 4):
            own = own.at[:, tile_of(me, part)]
        if flow in (5, 6):
            own = own.at[:, tile_of(opposite, part)]

        @pl.when(row + 1 < rows_count)
        def _():
            line_copy(flow, row, True, own).start()

        @pl.when(row >= 1)
        def _():
            line_copy(flow, row, False, own).start()

    near = 2 * (rows_count - 1) // 3

    def hop(flow, third, after=lambda origin: None, limit=None):
        limit = rows_count if limit is None else limit

        def one(hops):
            @pl.when(row >= hops)
            def _():
                origin = row - hops
                line_copy(flow, origin, True).wait_recv()

                @pl.when((row + 1 < rows_count) & (hops < limit))
                def _():
                    line_copy(flow, origin, True).start()

                after(origin)

            @pl.when(row + hops < rows_count)
            def _():
                origin = row + hops
                line_copy(flow, origin, False).wait_recv()

                @pl.when((row >= 1) & (hops < limit))
                def _():
                    line_copy(flow, origin, False).start()

                after(origin)

        low, high = (1 + (rows_count - 1) * k // 3 for k in (third - 1, third))
        loop(high - low, lambda i: one(low + i))

    def thirds(third, body):
        def one(i):
            hops = 1 + i // 2
            origin = row + hops * (1 - 2 * lax.rem(i, 2))

            @pl.when((origin >= 0) & (origin < rows_count))
            def _():
                body(origin)

        low, high = (2 * ((rows_count - 1) * k // 3) for k in (third, third + 1))
        loop(high - low, lambda i: one(low + i))

    def others(body, after=()):
        def one(i):
            hops = 1 + i // 2
            origin = row + hops * (1 - 2 * lax.rem(i, 2))
            above, below = rows_count - 1 - row, row
            done = jnp.minimum((i + 2) // 2, above) + jnp.minimum((i + 1) // 2, below)

            @pl.when((origin >= 0) & (origin < rows_count))
            def _():
                body(origin)
                for number, action in after:
                    pl.when(done == number)(action)

        loop(2 * (rows_count - 1), one)

    def finish_flow(flow, limit=None, halves=True):
        limit = rows_count if limit is None else limit

        def one(origin):
            @pl.when((origin <= row) & (row + 1 < rows_count) & (row - origin < limit))
            def _():
                line_copy(flow, origin, True).wait_send()

            @pl.when((origin >= row) & (row >= 1) & (origin - row < limit))
            def _():
                line_copy(flow, origin, False).wait_send()

            @pl.when(origin != row)
            def _():
                if flow < 2:
                    for step in direct_steps:
                        plane_copy(flow, origin, step).wait_send()
                    if balanced and halves:
                        for half in range(2):
                            half_copy(flow, origin, half).wait_send()
                if flow == 4:
                    for step in [0] + steps:
                        engine_copy(origin, step).wait_send()

        loop(rows_count, one)

    def own_stores(flow, own):
        return [
            pltpu.make_async_copy(
                own.at[:, pl.ds(i * part, part)], flows[flow].at[row, i], store.at[flow * count + i]
            )
            for i in range(count)
        ]

    def scatter(kind, step):
        peer = partner(me, step, count)[0]
        return pltpu.make_async_remote_copy(
            src_ref=term.at[peer],
            dst_ref=arrived.at[kind, step],
            send_sem=send.at[kind, step],
            recv_sem=recv.at[kind, step],
            device_id=at(section, peer),
            device_id_type=MESH,
        )

    def gather(number, step, target):
        peer = partner(me, step, count)[0]
        return pltpu.make_async_remote_copy(
            src_ref=parts.at[number, 0],
            dst_ref=parts.at[number, step],
            send_sem=part_send.at[number, step],
            recv_sem=part_recv.at[number, step],
            device_id=at(target, peer),
            device_id_type=MESH,
        )

    def back(number, step):
        return pltpu.make_async_remote_copy(
            src_ref=parts.at[number, step],
            dst_ref=parts.at[number, step],
            send_sem=back_send.at[number, step],
            recv_sem=back_recv.at[number, step],
            device_id=at(1 - section, me),
            device_id_type=MESH,
        )

    def place(number, step, target):
        owner = partner(me, step, count)[1]
        target[:, tile_of(owner, part)] = parts[number, step]

    def reduce(kind, number, with_input):
        for step in steps:
            scatter(kind, step).wait_recv()

        def rows_of(i):
            rows = tile_of(i, row_tile)
            total = term[me, rows, :].astype(F32)
            if with_input:
                total = total + xv[rows, tile_of(me, part)].astype(F32)
            for step in steps:
                total = total + arrived[kind, step, rows, :].astype(F32)
            parts[number, 0, rows, :] = total.astype(BF16)

        loop(row_tiles, rows_of)

    def finish_sends(kind):
        for step in steps:
            scatter(kind, step).wait_send()

    def to_other_section(number):
        for step in steps[::-1] + [0]:
            gather(number, step, 1 - section).start()

    def from_own_section(number, target):
        place(number, 0, target)
        for step in steps:
            back(number, step).wait_recv()
            place(number, step, target)
        for step in [0] + steps:
            gather(number, step, 1 - section).wait_send()

    def from_other_section(number, target):
        gather(number, 0, 1 - section).wait_recv()
        place(number, 0, target)
        for step in steps:
            gather(number, step, 1 - section).wait_recv()
            back(number, step).start()
            place(number, step, target)

    def finish_back(number):
        for step in steps:
            back(number, step).wait_send()

    def start_within(number):
        for step in steps[::-1]:
            gather(number, step, section).start()

    def finish_within(number, target):
        place(number, 0, target)
        for step in steps:
            gather(number, step, section).wait_recv()
            place(number, step, target)
        for step in steps:
            gather(number, step, section).wait_send()

    def each_chunk(kind, compute, between=None, sends=True):
        def chunk(i):
            step = count - 1 - i
            owner = partner(me, step, count)[0]
            loop(part // TILE, lambda j: compute(owner, j))

            @pl.when((step > 0) & sends)
            def _():
                scatter(kind, step).start()

            if between is not None:
                pl.when(i == count // 2 - 1)(between)

        loop(count, chunk)

    lane = lanes_of((1, LANES)).astype(F32)
    exponent = jnp.where(lane < ROT // 2, lane, lane - ROT // 2)
    frequency = jnp.exp(exponent * (-2.0 * math.log(10000.0) / ROT))
    row_index = lax.broadcasted_iota(jnp.int32, (length, length), 0)
    column_index = lax.broadcasted_iota(jnp.int32, (length, length), 1)

    def segments_of(values):
        across = values.astype(F32)
        down = jnp.sum(jnp.where(row_index == column_index, across, 0.0), axis=1, keepdims=True)
        return across, down

    def fill_tables(slot, values_of):
        for b in range(batch):
            rows = pl.ds(b * length, length)
            across, down = segments_of(values_of(b))
            number_of = jnp.sum((across < down).astype(F32), axis=1, keepdims=True)
            index = lax.broadcasted_iota(jnp.int32, (length, 1), 0).astype(F32)
            angles = (index - number_of) * frequency
            inside = lanes_of((length, LANES)) < ROT
            tables[slot, rows, :LANES] = jnp.where(inside, jnp.cos(angles), 1.0)
            tables[slot, rows, LANES:] = jnp.where(inside, jnp.sin(angles), 0.0)

    fill_tables(row, lambda b: seg_row[b : b + 1, :])

    def softmax(projected, values, b, h):
        rows, columns = tile_of(b, length), tile_of(h, HEAD)
        across, down = segments_of(values)
        allowed = (across == down) & (column_index <= row_index)
        scores = dot_nt(projected[0, rows, columns], projected[1, rows, columns]) * scale
        scores = jnp.where(allowed, scores, -jnp.inf)
        row_max = jnp.max(scores, axis=-1, keepdims=True)
        total = jnp.sum(jnp.exp(scores - row_max), axis=-1, keepdims=True)
        return jnp.exp(scores - (row_max + jnp.log(total)))

    def attend(prob, projected, target, b, h):
        rows, columns = tile_of(b, length), tile_of(h, HEAD)
        target[rows, columns] = dot(prob.astype(BF16), projected[2, rows, columns]).astype(BF16)

    def attend_backward(prob, projected, slot, target, b, h):
        rows, columns = tile_of(b, length), tile_of(h, HEAD)
        cosine, sine = tables[slot, rows, :LANES], tables[slot, rows, LANES:]
        queries, keys, values = (projected[k, rows, columns] for k in range(3))
        d_context = dctx[rows, columns]
        d_values = dot_tn(prob.astype(BF16), d_context)
        d_probs = dot_nt(d_context, values)
        delta = jnp.sum(prob * d_probs, axis=-1, keepdims=True)
        d_scores = (prob * (d_probs - delta) * scale).astype(BF16)
        for k, gradient in ((0, dot(d_scores, keys)), (1, dot_tn(d_scores, queries))):
            first = unrotated(gradient[:, :LANES], cosine, sine)
            start = pl.multiple_of(h * HEAD, HEAD)
            target[k, rows, pl.ds(start, LANES)] = first.astype(BF16)
            start = pl.multiple_of(h * HEAD + LANES, LANES)
            target[k, rows, pl.ds(start, HEAD - LANES)] = gradient[:, LANES:].astype(BF16)
        target[2, rows, columns] = d_values.astype(BF16)

    def each_pair(body):
        def row_of(b):
            for h in range(heads):
                body(b, h)

        loop(batch, row_of)

    def project(projected, slot):
        def rotary_head(i):
            which, h = i // heads, lax.rem(i, heads)
            tile = dot(attn_in[...], w3[which, :, tile_of(h, HEAD)])
            first = rotated(tile[:, :LANES], tables[slot, :, :LANES], tables[slot, :, LANES:])
            start = pl.multiple_of(h * HEAD, HEAD)
            projected[which, :, pl.ds(start, LANES)] = first.astype(BF16)
            start = pl.multiple_of(h * HEAD + LANES, LANES)
            projected[which, :, pl.ds(start, HEAD - LANES)] = tile[:, LANES:].astype(BF16)

        def value_head(h):
            columns = tile_of(h, HEAD)
            projected[2, :, columns] = dot(attn_in[...], w3[2, :, columns]).astype(BF16)

        loop(2 * heads, rotary_head)
        loop(heads, value_head)

    def segment_copy(step):
        return pltpu.make_async_remote_copy(
            src_ref=seg_row,
            dst_ref=segments.at[row],
            send_sem=segment_send.at[step],
            recv_sem=segment_recv.at[step],
            device_id={"dp": lax.rem(row + step, rows_count)},
            device_id_type=MESH,
        )

    def d_context_head(h):
        dctx[:, tile_of(h, HEAD)] = dot_nt(gbv[...], wo[tile_of(h, HEAD), :]).astype(BF16)

    def meet():
        pl.semaphore_wait(barrier, 2 * count - 1 + rows_count - 1)
        for step in range(1, rows_count):
            segment_copy(step).start()


    @pl.when(section == 0)
    def _():
        x_load.wait()

    @pl.when(section == 1)
    def _():
        meet()
        start_flow(4, x_hbm)
        if balanced:
            start_flow(6, x_hbm)
        go_load.wait()
        out_load.wait()
        loop(heads, d_context_head)
        if balanced:
            hop(6, 1)
        hop(4, 1, send_engine_first)
        fc2_load.wait()

        def d_act_tile(i):
            columns = tile_of(i, TILE)
            slope[:, columns] = dot_nt(gbv[...], w2[columns, :])

        loop(hidden_width // TILE, d_act_tile)
        for third in (2, 3):
            if balanced:
                hop(6, third)
            hop(4, third)
            if third == 2:
                start_flow(1, gbv)
                if balanced:
                    start_flow(5, gbv)
        hop(1, 1)
        if balanced:
            hop(5, 1)
        from_other_section(0, xv)
        start_flow(0, xv)
        for third in range(3):
            thirds(third, send_engine_later)

    for copy in own_stores(0, xv):
        copy.start()

    def norm_rows(i):
        rows = tile_of(i, row_tile)
        normed, mean, inv_std = row_norm(xv[rows, :].astype(F32))
        means[rows, :] = mean
        inv_stds[rows, :] = inv_std
        attn_in[rows, :] = (normed * gains[0:1, :] + biases[0:1, :]).astype(BF16)
        mlp_in[rows, :] = (normed * gains[1:2, :] + biases[1:2, :]).astype(BF16)

    loop(row_tiles, norm_rows)

    for copy in qkv_loads:
        copy.wait()
    project(qkv, row)

    def own_attention(b, h):
        prob = softmax(qkv, seg_row[pl.ds(b, 1), :], b, h)
        probs[b * heads + h] = prob
        attend(prob, qkv, context, b, h)

    each_pair(own_attention)

    @pl.when(section == 1)
    def _():
        hop(0, 1, send_plane_of(0))
        hop(1, 2)
        if balanced:
            hop(5, 2)


    def fc1_block(i):
        fc1_load(i).wait()

        def fc1_tile(j):
            columns = tile_of(i * (block // TILE) + j, TILE)
            value, derivative = gelu_parts(dot(mlp_in[...], w1[:, columns]))
            act[:, columns] = value.astype(BF16)

            @pl.when(section == 0)
            def _():
                slope[:, columns] = derivative

            @pl.when(section == 1)
            def _():
                dh[:, columns] = (slope[:, columns] * derivative).astype(BF16)

        loop(block // TILE, fc1_tile)

    loop(blocks, fc1_block)

    @pl.when(section == 1)
    def _():
        hop(0, 2, send_plane_of(0))

    @pl.when(section == 0)
    def _():
        out_load.wait()
        fc2_load.wait()
        go_load.wait()

    tiles = hidden_width // TILE

    def act_store(origin, i):
        columns = tile_of(i, TILE)
        return pltpu.make_async_copy(
            act_rest.at[:, columns], act_all.at[origin, :, columns], rest_store.at[0, i]
        )

    def dh_store(origin, i):
        columns = tile_of(i, TILE)
        return pltpu.make_async_copy(
            act_rest.at[:, columns], dh_all.at[origin, :, columns], rest_store.at[0, i]
        )

    def slope_store(origin, i):
        columns = tile_of(i, TILE)
        return pltpu.make_async_copy(
            slope_rest.at[:, columns], slope_all.at[origin, :, columns], rest_store.at[1, i]
        )

    def load_block(flow, origin):
        if flow == 0:

            @pl.when(section == 0)
            def _():
                for step in [0] + steps:
                    engine_copy(origin, step).wait_recv()

            pl.when(section == 1)(lambda: wait_plane(flow, origin))
        else:
            pl.when(section == 0)(lambda: wait_plane(flow, origin))

            @pl.when(section == 1)
            def _():
                for step in direct_steps:
                    plane_copy(flow, origin, step).wait_recv()

        copies = [
            pltpu.make_async_copy(
                flows[flow].at[origin, i], attn_in.at[:, pl.ds(i * part, part)], rest_load.at[i]
            )
            for i in range(count)
        ]
        for copy in copies:
            copy.start()
        return copies

    def attention_stores(origin):
        return [
            pltpu.make_async_copy(qkv_rest, qkv_all.at[origin], rest_load.at[count + 1]),
            pltpu.make_async_copy(context_rest, context_all.at[origin], rest_load.at[count + 2]),
        ]

    def rest_forward(origin):
        for copy in load_block(0, origin):
            copy.wait()

        def norm_rows(i):
            rows = tile_of(i, row_tile)
            normed, mean, inv_std = row_norm(attn_in[rows, :].astype(F32))
            first = lanes_of((row_tile, LANES)) == 0
            stats_all[origin, rows, :] = jnp.where(first, mean, inv_std)
            mlp_in[rows, :] = (normed * gains[1:2, :] + biases[1:2, :]).astype(BF16)
            attn_in[rows, :] = (normed * gains[0:1, :] + biases[0:1, :]).astype(BF16)

        loop(row_tiles, norm_rows)

        @pl.when(section == 0)
        def _():
            fill_tables(origin, lambda b: segments[origin, b : b + 1, :])
            project(qkv_rest, origin)

            def attention(b, h):
                prob = softmax(qkv_rest, segments[origin, pl.ds(b, 1), :], b, h)
                attend(prob, qkv_rest, context_rest, b, h)

            each_pair(attention)
            for copy in attention_stores(origin):
                copy.start()

        def tile(i):
            columns = tile_of(i, TILE)
            value, derivative = gelu_parts(dot(mlp_in[...], w1[:, columns]))
            act_rest[:, columns] = value.astype(BF16)
            slope_rest[:, columns] = derivative
            act_store(origin, i).start()
            slope_store(origin, i).start()

        loop(tiles, tile)

        def wait(i):
            act_store(origin, i).wait()
            slope_store(origin, i).wait()

        loop(tiles, wait)

        @pl.when(section == 0)
        def _():
            for copy in attention_stores(origin):
                copy.wait()

    def rest_backward(origin):
        copies = load_block(1, origin)
        slope_load = pltpu.make_async_copy(slope_all.at[origin], slope_rest, rest_load.at[count])
        slope_load.start()
        for copy in copies + [slope_load]:
            copy.wait()

        def tile(i):
            columns = tile_of(i, TILE)
            d_act = dot_nt(attn_in[...], w2[columns, :])
            act_rest[:, columns] = (d_act * slope_rest[:, columns]).astype(BF16)
            dh_store(origin, i).start()

        qkv_load = pltpu.make_async_copy(qkv_all.at[origin], qkv_rest, rest_load.at[count + 1])
        dproj_store = pltpu.make_async_copy(
            dproj_rest, dproj_all.at[origin], rest_load.at[count + 2]
        )
        far = (section == 0) & ((origin - row > near) | (row - origin > near))
        pl.when(far)(qkv_load.start)
        loop(tiles, tile)

        @pl.when(far)
        def _():
            qkv_load.wait()

            def head(h):
                columns = tile_of(h, HEAD)
                dctx[:, columns] = dot_nt(attn_in[...], wo[columns, :]).astype(BF16)

            loop(heads, head)

            def attention(b, h):
                prob = softmax(qkv_rest, segments[origin, pl.ds(b, 1), :], b, h)
                attend_backward(prob, qkv_rest, origin, dproj_rest, b, h)

            each_pair(attention)
            dproj_store.start()
            dproj_store.wait()

        loop(tiles, lambda i: dh_store(origin, i).wait())

    def out_tile(owner, j):
        columns = tile_of(owner * (part // TILE) + j, TILE)
        total = dot(context[...], wo[:, columns]) + dot(act[...], w2[:, columns])
        term[owner, :, tile_of(j, TILE)] = total.astype(BF16)

    layer_store = pltpu.make_async_copy(other, layer_out, store.at[2 * count + 4])
    grad_store = pltpu.make_async_copy(slope, input_grad, store.at[2 * count + 5])
    stats_store = pltpu.make_async_copy(stats_all, stats_out, store.at[2 * count + 6])

    @pl.when(section == 0)
    def _():
        meet()
        each_chunk(0, out_tile)
        reduce(0, 0, True)
        to_other_section(0)
        finish_sends(0)
        for step in range(1, rows_count):
            segment_copy(step).wait_recv()
        others(rest_forward)
        from_own_section(0, other)
        layer_store.start()
        from_other_section(1, full)

        def gradient_rows(i):
            rows = tile_of(i, row_tile)
            normed, _, inv_std = row_norm(other[rows, :].astype(F32))
            dx = row_norm_backward(full[rows, :].astype(F32), normed, inv_std)
            gbv[rows, :] = (gbv[rows, :].astype(F32) + dx).astype(BF16)

        loop(row_tiles, gradient_rows)
        start_flow(1, gbv)
        finish_back(1)

        def d_hidden_tile(i):
            columns = tile_of(i, TILE)
            d_act = dot_nt(gbv[...], w2[columns, :])
            dh[:, columns] = (d_act * slope[:, columns]).astype(BF16)

        loop(hidden_width // TILE, d_hidden_tile)
        loop(heads, d_context_head)
        hop(1, 1, send_plane_of(1))


    each_pair(lambda b, h: attend_backward(probs[b * heads + h], qkv, row, dproj, b, h))

    @pl.when(section == 1)
    def _():
        start_flow(3, dproj)

    def gradient_tile(owner, j):
        columns = tile_of(owner * (part // TILE) + j, TILE)
        d_attn = dot_nt(dproj[0], w3[0, columns, :])
        d_attn = d_attn + dot_nt(dproj[1], w3[1, columns, :])
        d_attn = d_attn + dot_nt(dproj[2], w3[2, columns, :])
        d_mlp = dot_nt(dh[...], w1[columns, :])
        normed = (xv[:, columns].astype(F32) - means[...]) * inv_stds[...]
        total = d_attn * gains[0:1, columns] + d_mlp * gains[1:2, columns]
        term[owner, :, tile_of(j, TILE)] = total.astype(BF16)
        vectors[0:1, columns] = jnp.sum(d_attn * normed, axis=0, keepdims=True)
        vectors[1:2, columns] = jnp.sum(d_mlp * normed, axis=0, keepdims=True)
        vectors[2:3, columns] = jnp.sum(d_attn, axis=0, keepdims=True)
        vectors[3:4, columns] = jnp.sum(d_mlp, axis=0, keepdims=True)

    def second_hop():
        @pl.when(section == 0)
        def _():
            hop(1, 2, send_plane_of(1))
            thirds(0, relay_plane_of(1))

    each_chunk(1, gradient_tile, second_hop, section == 1)

    outs = [
        (act, act_all.at[row]),
        (context, context_all.at[row]),
        (dh, dh_all.at[row]),
        (dproj, dproj_all.at[row]),
    ]
    stores = own_stores(1, gbv)
    stores += [
        pltpu.make_async_copy(a, b, store.at[2 * count + i]) for i, (a, b) in enumerate(outs)
    ]
    for copy in stores:
        copy.start()

    def sum_copy(step):
        peer = partner(me, step, count)[0]
        return pltpu.make_async_remote_copy(
            src_ref=vectors,
            dst_ref=plane_vectors.at[step],
            send_sem=sum_send.at[step],
            recv_sem=sum_recv.at[step],
            device_id=at(section, peer),
            device_id_type=MESH,
        )

    mine = width // rows_count

    def slice_copy(step):
        target = lax.rem(row + step, rows_count)
        return pltpu.make_async_remote_copy(
            src_ref=plane_vectors.at[0, :, tile_of(target, mine)],
            dst_ref=slices.at[step],
            send_sem=slice_send.at[step],
            recv_sem=slice_recv.at[step],
            device_id={"dp": target},
            device_id_type=MESH,
        )

    for step in steps:
        sum_copy(step).start()

    def sum_plane():
        total = vectors[...]
        for step in steps:
            sum_copy(step).wait_recv()
            total = total + plane_vectors[step]
        plane_vectors[0] = total
        for step in range(1, rows_count):
            slice_copy(step).start()

    def sum_line():
        total = plane_vectors[0, :, tile_of(row, mine)]
        for step in range(1, rows_count):
            slice_copy(step).wait_recv()
            total = total + slices[step]
        gain_grads[...] = total[:2]
        bias_grads[...] = total[2:]
        for step in range(1, rows_count):
            slice_copy(step).wait_send()
        for step in steps:
            sum_copy(step).wait_send()

    def own_stats(i):
        rows = tile_of(i, row_tile)
        first = lanes_of((row_tile, LANES)) == 0
        stats_all[row, rows, :] = jnp.where(first, means[rows, :], inv_stds[rows, :])

    loop(row_tiles, own_stats)

    def input_gradient():
        def rows_of(i):
            rows = tile_of(i, row_tile)
            inv_std = inv_stds[rows, :]
            normed = (xv[rows, :].astype(F32) - means[rows, :]) * inv_std
            dx = row_norm_backward(full[rows, :].astype(F32), normed, inv_std)
            slope[rows, :] = gbv[rows, :].astype(F32) + dx

        loop(row_tiles, rows_of)
        grad_store.start()

    @pl.when(section == 0)
    def _():
        stats_store.start()
        hop(1, 3, send_plane_of(1))
        start_flow(3, dproj)
        thirds(1, relay_plane_of(1))

        def after_first():
            thirds(2, relay_plane_of(1))
            for step in steps[::-1]:
                scatter(1, step).start()
            sum_plane()

        def after_second():
            reduce(1, 2, False)
            start_within(2)
            hop(3, 1, limit=near)

        others(rest_backward, [(1, after_first), (2, after_second)])
        finish_within(2, full)
        finish_sends(1)
        input_gradient()
        hop(3, 2, limit=near)

    @pl.when(section == 1)
    def _():
        finish_back(0)
        reduce(1, 1, False)
        to_other_section(1)
        thirds(0, relay_plane_of(0))
        hop(0, 3, send_plane_of(0))
        thirds(1, relay_plane_of(0))
        hop(3, 1)
        hop(1, 3)
        if balanced:
            hop(5, 3)
        finish_sends(1)
        each_chunk(0, out_tile, None, False)
        from_own_section(1, full)
        for step in steps[::-1]:
            scatter(0, step).start()
        sum_plane()

        def share_gradients():
            for third in range(3):
                thirds(third, send_plane_of(1))

        others(
            rest_forward, [(1, lambda: thirds(2, relay_plane_of(0))), (2, share_gradients)]
        )
        stats_store.start()
        input_gradient()
        start_flow(2, context)
        hop(3, 2)

        def after_first_backward():
            hop(2, 1)
            reduce(0, 3, True)
            start_within(3)

        others(rest_backward, [(1, after_first_backward), (2, lambda: hop(2, 2))])
        finish_within(3, other)
        layer_store.start()
        hop(3, 3)
        hop(2, 3)
        finish_sends(0)

    sum_line()
    for copy in own_stores(0, xv) + stores + [layer_store, grad_store, stats_store]:
        copy.wait()
    @pl.when(section == 0)
    def _():
        finish_flow(1)
        finish_flow(3, near)

    @pl.when(section == 1)
    def _():
        for step in range(1, rows_count):
            segment_copy(step).wait_recv()
        finish_flow(1, halves=False)
        for flow in (0, 2, 3, 4) + ((5, 6) if balanced else ()):
            finish_flow(flow)

    for step in range(1, rows_count):
        segment_copy(step).wait_send()


def chain(block_input, grad_output, segment_ids, weights):
    w_qkv, w_out, w_fc1, w_fc2, gains, biases = weights
    batch, length, width = block_input.shape
    tokens = batch * length
    count = lax.axis_size("tensor")
    inner, hidden = w_qkv.shape[2], w_fc1.shape[1]
    part = width // count
    heads = inner // HEAD
    anywhere, vmem = pl.BlockSpec(memory_space=pl.ANY), pl.BlockSpec(memory_space=pltpu.VMEM)
    like = jax.ShapeDtypeStruct
    rows_count = lax.axis_size("dp")
    wide, narrow = (tokens, width), (tokens, inner)
    dma = pltpu.SemaphoreType.DMA
    return pl.pallas_call(
        functools.partial(chain_kernel, count, batch),
        out_shape=[
            like(wide, BF16),
            like(wide, F32),
            like((2, width // rows_count), F32),
            like((2, width // rows_count), F32),
            like((rows_count, count, tokens, part), BF16),
            like((rows_count, count, tokens, part), BF16),
            like((rows_count, tokens, inner), BF16),
            like((rows_count, 3, tokens, inner), BF16),
            like((rows_count, tokens, hidden), BF16),
            like((rows_count, tokens, hidden), BF16),
            like((rows_count, tokens, LANES), F32),
            like((rows_count, tokens, hidden), F32),
            like((rows_count, 2, tokens, part), BF16),
            like((rows_count, 3, tokens, inner), BF16),
        ],
        in_specs=[anywhere, anywhere, vmem] + [anywhere] * 4 + [vmem, vmem],
        out_specs=[anywhere, anywhere, vmem, vmem] + [anywhere] * 6 + [anywhere] * 4,
        scratch_shapes=[
            pltpu.VMEM((3, width, inner), BF16),
            pltpu.VMEM((inner, width), BF16),
            pltpu.VMEM((width, hidden), BF16),
            pltpu.VMEM((hidden, width), BF16),
            pltpu.VMEM(wide, BF16),
            pltpu.VMEM(wide, BF16),
            pltpu.VMEM(wide, BF16),
            pltpu.VMEM(wide, BF16),
            pltpu.VMEM(wide, BF16),
            pltpu.VMEM((3, tokens, inner), BF16),
            pltpu.VMEM(narrow, BF16),
            pltpu.VMEM((batch * heads, length, length), F32),
            pltpu.VMEM((tokens, hidden), BF16),
            pltpu.VMEM((tokens, hidden), F32),
            pltpu.VMEM((tokens, hidden), BF16),
            pltpu.VMEM(narrow, BF16),
            pltpu.VMEM((3, tokens, inner), BF16),
            pltpu.VMEM((tokens, 1), F32),
            pltpu.VMEM((tokens, 1), F32),
            pltpu.VMEM((rows_count, tokens, 2 * LANES), F32),
            pltpu.VMEM((count, tokens, part), BF16),
            pltpu.VMEM((2, count, tokens, part), BF16),
            pltpu.VMEM((4, count, tokens, part), BF16),
            pltpu.VMEM(wide, BF16),
            pltpu.VMEM((tokens, hidden), BF16),
            pltpu.VMEM((tokens, hidden), F32),
            pltpu.VMEM((rows_count, tokens, LANES), F32),
            pltpu.VMEM((4, width), F32),
            pltpu.VMEM((count, 4, width), F32),
            pltpu.VMEM((rows_count, 4, width // rows_count), F32),
            pltpu.VMEM((rows_count, batch, length), jnp.int32),
            pltpu.VMEM((3, tokens, inner), BF16),
            pltpu.VMEM((3, tokens, inner), BF16),
            pltpu.VMEM(narrow, BF16),
            dma((11,)),
            dma((2 * count + 7,)),
            dma((2, count)),
            dma((2, count)),
            dma((4, count)),
            dma((4, count)),
            dma((2, count)),
            dma((2, count)),
            dma((7, 2, rows_count)),
            dma((7, rows_count)),
            dma((2, rows_count, count)),
            dma((2, rows_count, count)),
            dma((count + 3,)),
            dma((2, hidden // TILE)),
            dma((count,)),
            dma((count,)),
            dma((rows_count,)),
            dma((rows_count,)),
            dma((rows_count, count)),
            dma((rows_count,)),
            dma((rows_count,)),
        ],
        compiler_params=pltpu.CompilerParams(
            collective_id=0, has_side_effects=True, vmem_limit_bytes=67_043_328
        ),
        name="chain",
    )(
        block_input.reshape(wide),
        grad_output.reshape(wide),
        segment_ids,
        jnp.transpose(w_qkv, (1, 0, 2)),
        w_out,
        w_fc1,
        w_fc2,
        gains,
        biases,
    )


def weight_kernel(*refs):
    (
        x_all, gb_all, stats_all, context_all, dproj_all, act_all, dh_all, gains, biases,
        layer_in, grad_in, gain_in, bias_in,
        g_qkv, g_out, g_fc1, g_fc2, layer_out, input_grad, gain_out, bias_out,
        x_mine, gb_mine, context, dproj, act, attn_t, mlp_t, r_qkv, r_out, r_fc1, r_fc2,
        layer, grad, stats, load, act_load, dh_load, store, through, gb_load, x_load,
    ) = refs
    blocks, tokens, mine = x_mine.shape
    rows = blocks * tokens
    part = x_all.shape[3]
    inner, hidden = context.shape[2], act.shape[2]
    start = lax.axis_index("dp") * mine
    chunk, offset = start // part, pl.multiple_of(lax.rem(start, part), LANES)
    piece = hidden // 4

    def slice_loads(source, target, sems):
        return [
            pltpu.make_async_copy(
                source.at[i, chunk, :, pl.ds(offset, mine)], target.at[i], sems.at[i]
            )
            for i in range(blocks)
        ]

    def piece_load(source, target, sems, i):
        columns = pl.ds(i * piece, piece)
        return pltpu.make_async_copy(source.at[:, :, columns], target.at[:, :, columns], sems.at[i])

    gb_loads = slice_loads(gb_all, gb_mine, gb_load)
    x_loads = slice_loads(x_all, x_mine, x_load)
    stats_load = pltpu.make_async_copy(stats_all, stats, load.at[0])
    context_load = pltpu.make_async_copy(context_all, context, load.at[2])
    dproj_load = pltpu.make_async_copy(dproj_all, dproj, load.at[3])
    act_loads = [piece_load(act_all, act, act_load, i) for i in range(4)]
    dh_loads = [piece_load(dh_all, act, dh_load, i) for i in range(4)]
    gain_out[...] = gain_in[...]
    bias_out[...] = bias_in[...]
    ins = [
        pltpu.make_async_copy(layer_in, layer, through.at[0]),
        pltpu.make_async_copy(grad_in, grad, through.at[1]),
    ]
    outs = [
        pltpu.make_async_copy(layer, layer_out, through.at[2]),
        pltpu.make_async_copy(grad, input_grad, through.at[3]),
    ]
    for copy in gb_loads + [context_load]:
        copy.start()

    def transposed_rows(i):
        columns = tile_of(i, LANES)
        mean = stats[:, :, 0:1].reshape(rows, 1)
        inv_std = stats[:, :, 1:2].reshape(rows, 1)
        normed = (x_mine[:, :, columns].reshape(rows, LANES).astype(F32) - mean) * inv_std
        whole = tile_of(chunk * (part // LANES) + offset // LANES + i, LANES)
        for j, target in enumerate((attn_t, mlp_t)):
            scaled = normed * gains[j : j + 1, whole] + biases[j : j + 1, whole]
            target[columns, :] = scaled.astype(BF16).T

    def out_copy(source, target, index):
        return pltpu.make_async_copy(source, target, store.at[index])

    for copy in gb_loads + [context_load]:
        copy.wait()
    for copy in act_loads + x_loads + [stats_load, dproj_load] + ins:
        copy.start()
    gb_rows = gb_mine[...].reshape(rows, mine)

    def out_tile(i):
        tile = tile_of(i, TILE)
        r_out[tile, :] = dot_tn(context[:, :, tile].reshape(rows, TILE), gb_rows)

    loop(inner // TILE, out_tile)
    copies = [out_copy(r_out, g_out, 0)]
    copies[0].start()

    def fc2_copy(i):
        tile = tile_of(i, TILE)
        return out_copy(r_fc2.at[tile, :], g_fc2.at[tile, :], 1 + i)

    def fc2_tile(i):
        tile = tile_of(i, TILE)
        r_fc2[tile, :] = dot_tn(act[:, :, tile].reshape(rows, TILE), gb_mine[...].reshape(rows, mine))
        fc2_copy(i).start()

    per = piece // TILE
    for i in range(4):
        act_loads[i].wait()
        loop(per, lambda j: fc2_tile(i * per + j))
        dh_loads[i].start()
    for copy in ins:
        copy.wait()
    for copy in outs:
        copy.start()
    for copy in x_loads + [stats_load]:
        copy.wait()
    loop(mine // LANES, transposed_rows)

    def fc1_copy(i):
        tile = tile_of(i, TILE)
        return out_copy(r_fc1.at[:, tile], g_fc1.at[:, tile], 1 + hidden // TILE + i)

    def fc1_tile(i):
        tile = tile_of(i, TILE)
        r_fc1[:, tile] = dot(mlp_t[...], act[:, :, tile].reshape(rows, TILE))
        fc1_copy(i).start()

    for copy in dh_loads:
        copy.wait()
    loop(hidden // TILE, fc1_tile)
    dproj_load.wait()
    per = inner // TILE

    def qkv_copy(i):
        which, tile = i // per, tile_of(lax.rem(i, per), TILE)
        return out_copy(r_qkv.at[which, :, tile], g_qkv.at[which, :, tile], 1 + 2 * (hidden // TILE) + i)

    def qkv_tile(i):
        which, tile = i // per, tile_of(lax.rem(i, per), TILE)
        r_qkv[which, :, tile] = dot(attn_t[...], dproj[:, which, :, tile].reshape(rows, TILE))
        qkv_copy(i).start()

    loop(3 * per, qkv_tile)
    for copy in copies + outs:
        copy.wait()
    loop(hidden // TILE, lambda i: fc2_copy(i).wait())
    loop(hidden // TILE, lambda i: fc1_copy(i).wait())
    loop(3 * per, lambda i: qkv_copy(i).wait())


def weight_gradients(
    x_all, gb_all, stats, context_all, dproj_all, act_all, dh_all, gains, biases, *through
):
    blocks, count, tokens, part = x_all.shape
    mine = count * part // lax.axis_size("dp")
    inner, hidden = context_all.shape[2], act_all.shape[2]
    anywhere, vmem = pl.BlockSpec(memory_space=pl.ANY), pl.BlockSpec(memory_space=pltpu.VMEM)
    shapes = [(3, mine, inner), (inner, mine), (mine, hidden), (hidden, mine)]
    dma = pltpu.SemaphoreType.DMA
    return pl.pallas_call(
        weight_kernel,
        out_shape=[jax.ShapeDtypeStruct(shape, F32) for shape in shapes]
        + [jax.ShapeDtypeStruct(value.shape, value.dtype) for value in through],
        in_specs=[anywhere] * 7
        + [vmem, vmem, anywhere, anywhere, vmem, vmem],
        out_specs=[anywhere] * 6 + [vmem, vmem],
        scratch_shapes=[
            pltpu.VMEM((blocks, tokens, mine), BF16),
            pltpu.VMEM((blocks, tokens, mine), BF16),
            pltpu.VMEM((blocks, tokens, inner), BF16),
            pltpu.VMEM((blocks, 3, tokens, inner), BF16),
            pltpu.VMEM((blocks, tokens, hidden), BF16),
            pltpu.VMEM((mine, blocks * tokens), BF16),
            pltpu.VMEM((mine, blocks * tokens), BF16),
        ]
        + [pltpu.VMEM(shape, F32) for shape in shapes]
        + [pltpu.VMEM(value.shape, value.dtype) for value in through[:2]]
        + [pltpu.VMEM(stats.shape, F32)]
        + [
            dma((4,)),
            dma((4,)),
            dma((4,)),
            dma((1 + 2 * (hidden // TILE) + 3 * (inner // TILE),)),
            dma((4,)),
            dma((blocks,)),
            dma((blocks,)),
        ],
        compiler_params=pltpu.CompilerParams(vmem_limit_bytes=67_043_328),
        name="weights",
    )(x_all, gb_all, stats, context_all, dproj_all, act_all, dh_all, gains, biases, *through)


def shards(
    block_input, grad_output, segment_ids, w_qkv, w_out, w_fc1, w_fc2, norm_gains, norm_biases
):
    batch, length, width = block_input.shape
    weights = (w_qkv[0], w_out[0], w_fc1[0], w_fc2[0], norm_gains[0], norm_biases[0])
    (layer_out, input_grads, gain_grads, bias_grads, x_all, gb_all, context, d_proj, activated, d_hidden, stats, *_) = chain(
        block_input, grad_output, segment_ids, weights
    )
    g_qkv, g_out, g_fc1, g_fc2, layer_out, input_grads, gain_grads, bias_grads = weight_gradients(
        x_all, gb_all, stats, context, d_proj, activated, d_hidden, norm_gains[0], norm_biases[0],
        layer_out, input_grads, gain_grads, bias_grads,
    )
    shape = (1, batch, length, width)
    return (
        layer_out.reshape(shape),
        input_grads.reshape(shape),
        jnp.transpose(g_qkv, (1, 0, 2))[None],
        g_out[None],
        g_fc1[None],
        g_fc2[None],
        gain_grads[None],
        bias_grads[None],
    )


def solution(mesh):
    return jax.shard_map(
        shards,
        mesh=mesh,
        in_specs=(
            P("dp", None, None),
            P("dp", None, None),
            P("dp", None),
            P("section", None, None, "tensor"),
            P("section", "tensor", None),
            P("section", None, "tensor"),
            P("section", "tensor", None),
            P("section", None, None),
            P("section", None, None),
        ),
        out_specs=(
            P("section", "dp", None, None),
            P("section", "dp", None, None),
            P("section", "dp", None, "tensor"),
            P("section", "tensor", "dp"),
            P("section", "dp", "tensor"),
            P("section", "tensor", "dp"),
            P("section", None, "dp"),
            P("section", None, "dp"),
        ),
        check_vma=False,
    )
```

```python
import functools
import math

import jax
import jax.numpy as jnp
from jax import lax
from jax.experimental import pallas as pl
from jax.experimental.pallas import tpu as pltpu
from jax.sharding import PartitionSpec as P

HEAD = 256
ROT = 64
LANES = 128
TILE = 256
NORM_EPSILON = 1e-05
MESH = pl.DeviceIdType.MESH
BF16 = jnp.bfloat16
F32 = jnp.float32


def partner(index, step, count):
    if count & (count - 1):
        return lax.rem(index + step, count), lax.rem(index + count - step, count)
    bit = 1
    while bit < count:
        index = index + ((step // bit) % 2) * (bit - 2 * bit * ((index // bit) % 2))
        bit *= 2
    return index, index


def loop(count, body, unroll=1):
    lax.fori_loop(0, count, lambda i, carry: (body(i), carry)[1], 0, unroll=unroll)


def tile_of(i, size):
    return pl.ds(pl.multiple_of(i * size, size), size)


def dot(left, right):
    return jnp.dot(left, right, preferred_element_type=jnp.float32)


def dot_nt(left, right):
    return lax.dot_general(left, right, (((1,), (1,)), ((), ())), preferred_element_type=jnp.float32)


def dot_tn(left, right):
    return lax.dot_general(left, right, (((0,), (0,)), ((), ())), preferred_element_type=jnp.float32)


def gelu_parts(hidden):
    normal_cdf = 0.5 * (1.0 + lax.erf(hidden * (1.0 / math.sqrt(2.0))))
    density = jnp.exp(-0.5 * hidden * hidden) * (1.0 / math.sqrt(2.0 * math.pi))
    return (hidden * normal_cdf, normal_cdf + hidden * density)


def lanes_of(shape):
    return lax.broadcasted_iota(jnp.int32, shape, len(shape) - 1)


def rotated(tile, cosine, sine):
    half = ROT // 2
    left, right = pltpu.roll(tile, LANES - half, 1), pltpu.roll(tile, half, 1)
    lane = lanes_of(tile.shape)
    turned = jnp.where(lane < half, -left, right)
    return tile * cosine + turned * sine


def unrotated(tile, cosine, sine):
    half = ROT // 2
    scaled = tile * sine
    left, right = pltpu.roll(scaled, LANES - half, 1), pltpu.roll(scaled, half, 1)
    lane = lanes_of(tile.shape)
    turned = jnp.where(lane < half, left, jnp.where(lane < ROT, -right, 0.0))
    return tile * cosine + turned


def row_norm(values):
    mean = jnp.mean(values, axis=-1, keepdims=True)
    centred = values - mean
    inv_std = lax.rsqrt(jnp.mean(centred * centred, axis=-1, keepdims=True) + NORM_EPSILON)
    return centred * inv_std, mean, inv_std


def row_norm_backward(summed, normed, inv_std):
    return inv_std * (
        summed
        - jnp.mean(summed, axis=-1, keepdims=True)
        - normed * jnp.mean(summed * normed, axis=-1, keepdims=True)
    )


def chain_kernel(count, batch, *refs):
    (
        x_hbm, go_hbm, seg_row, w3_hbm, wo_hbm, w1_hbm, w2_hbm, gains, biases,
        layer_out, input_grad, gain_grads, bias_grads, x_all, gb_all, context_all, dproj_all, act_all, dh_all, attn_out, mlp_out,
        slope_all, relay_x, qkv_all,
        w3, wo, w1, w2, xv, other, gbv, attn_in, mlp_in, qkv, context, probs, act, slope, dh, dctx,
        dproj, means, inv_stds, tables, term, arrived, parts, full, act_rest, slope_rest,
        stats_all, x_mine, attn_t, mlp_t, vectors, plane_vectors, slices, segments, qkv_rest, dproj_rest, context_rest,
        load, store, send, recv, part_send, part_recv, back_send, back_recv,
        line_send, line_recv, plane_send, plane_recv, rest_load, rest_store, sum_send, sum_recv,
        slice_send, slice_recv, engine_send, segment_send, segment_recv, slice_load, grad_sems, sums, sum_store,
    ) = refs
    section, me = lax.axis_index("section"), lax.axis_index("tensor")
    row, rows_count = lax.axis_index("dp"), lax.axis_size("dp")
    tokens, width = xv.shape
    length = tokens // batch
    heads = qkv.shape[2] // HEAD
    hidden_width = act.shape[1]
    part = width // count
    row_tile = 32 if tokens % 32 == 0 else 16
    row_tiles = tokens // row_tile
    scale = 1.0 / math.sqrt(HEAD)

    qkv_loads = [pltpu.make_async_copy(w3_hbm.at[k], w3.at[k], load.at[k]) for k in range(3)]
    blocks = 4
    block = hidden_width // blocks

    def fc1_load(i):
        columns = tile_of(i, block)
        return pltpu.make_async_copy(w1_hbm.at[:, columns], w1.at[:, columns], load.at[3 + i])

    out_load = pltpu.make_async_copy(wo_hbm, wo, load.at[7])
    fc2_load = pltpu.make_async_copy(w2_hbm, w2, load.at[8])
    x_load = pltpu.make_async_copy(x_hbm, xv, load.at[9])
    go_load = pltpu.make_async_copy(go_hbm, gbv, load.at[10])

    @pl.when(section == 0)
    def _():
        x_load.start()

    go_load.start()

    def start_out_loads():
        out_load.start()
        fc2_load.start()

    pl.when(section == 1)(start_out_loads)
    for copy in qkv_loads:
        copy.start()
    for i in range(blocks):
        fc1_load(i).start()
    pl.when(section == 0)(start_out_loads)

    def at(section, index):
        return {"section": section, "tensor": index}

    steps = list(range(1, count))
    barrier = pltpu.get_barrier_semaphore()
    for step in range(count):
        peer = partner(me, step, count)[0]
        pl.semaphore_signal(barrier, inc=1, device_id=at(1 - section, peer), device_id_type=MESH)
        if step:
            pl.semaphore_signal(barrier, inc=1, device_id=at(section, peer), device_id_type=MESH)

    for step in range(1, rows_count):
        pl.semaphore_signal(
            barrier,
            inc=1,
            device_id={"dp": lax.rem(row + step, rows_count)},
            device_id_type=MESH,
        )

    balanced = count == 4
    opposite = partner(me, count - 1, count)[0]
    flows = (x_all, gb_all)

    def place_of(flow, origin):
        return (
            lambda: x_all.at[origin, me],
            lambda: gb_all.at[origin, me],
            lambda: context_all.at[origin],
            lambda: dproj_all.at[origin],
            lambda: relay_x.at[origin, 0],
            lambda: gb_all.at[origin, opposite],
            lambda: relay_x.at[origin, 1],
        )[flow]()

    def line_copy(flow, origin, up, own=None):
        place = place_of(flow, origin)
        return pltpu.make_async_remote_copy(
            src_ref=place if own is None else own,
            dst_ref=place,
            send_sem=line_send.at[flow, int(up), origin],
            recv_sem=line_recv.at[flow, origin],
            device_id={"dp": row + (1 if up else -1)},
            device_id_type=MESH,
        )

    def plane_copy(flow, origin, step):
        peer = partner(me, step, count)[0]
        return pltpu.make_async_remote_copy(
            src_ref=flows[flow].at[origin, me],
            dst_ref=flows[flow].at[origin, me],
            send_sem=plane_send.at[flow, origin, step],
            recv_sem=plane_recv.at[flow, origin, step],
            device_id=at(section, peer),
            device_id_type=MESH,
        )

    direct_steps = [1, 2] if balanced else steps

    def send_plane(flow, origin):
        for step in direct_steps[::-1]:
            plane_copy(flow, origin, step).start()

    def half_copy(flow, origin, half):
        owner = partner(me, 1 + half, count)[1]
        place = flows[flow].at[origin, owner, pl.ds(half * (tokens // 2), tokens // 2), :]
        return pltpu.make_async_remote_copy(
            src_ref=place,
            dst_ref=place,
            send_sem=plane_send.at[flow, origin, 3 * half],
            recv_sem=plane_recv.at[flow, origin, 3 * half],
            device_id=at(section, partner(me, 2 - half, count)[0]),
            device_id_type=MESH,
        )

    def relay_plane(flow, origin):
        if balanced:
            for step in direct_steps:
                plane_copy(flow, origin, step).wait_recv()
            for half in range(2):
                half_copy(flow, origin, half).start()

    def wait_plane(flow, origin):
        if balanced:
            for half in range(2):
                half_copy(flow, origin, half).wait_recv()
        else:
            for step in steps:
                plane_copy(flow, origin, step).wait_recv()

    def send_plane_of(flow):
        return lambda origin: send_plane(flow, origin)

    def relay_plane_of(flow):
        return lambda origin: relay_plane(flow, origin)

    def engine_copy(origin, step):
        second = balanced and step == 3
        peer = me if second else partner(me, step, count)[0]
        return pltpu.make_async_remote_copy(
            src_ref=relay_x.at[origin, int(second)],
            dst_ref=x_all.at[origin, opposite if second else me],
            send_sem=engine_send.at[origin, step],
            recv_sem=plane_recv.at[0, origin, step],
            device_id=at(1 - section, peer),
            device_id_type=MESH,
        )

    def send_engine(origin):
        for step in steps[::-1] + [0]:
            engine_copy(origin, step).start()

    first_other = jnp.where(row == rows_count - 1, row - 1, row + 1)

    def send_engine_first(origin):
        pl.when(origin == first_other)(lambda: send_engine(origin))

    def send_engine_later(origin):
        pl.when(origin != first_other)(lambda: send_engine(origin))

    def start_flow(flow, own):
        if flow in (0, 1, 4):
            own = own.at[:, tile_of(me, part)]
        if flow in (5, 6):
            own = own.at[:, tile_of(opposite, part)]

        @pl.when(row + 1 < rows_count)
        def _():
            line_copy(flow, row, True, own).start()

        @pl.when(row >= 1)
        def _():
            line_copy(flow, row, False, own).start()

    near = 2 * (rows_count - 1) // 3

    def hop(flow, third, after=lambda origin: None, limit=None):
        limit = rows_count if limit is None else limit

        def one(hops):
            @pl.when(row >= hops)
            def _():
                origin = row - hops
                line_copy(flow, origin, True).wait_recv()

                @pl.when((row + 1 < rows_count) & (hops < limit))
                def _():
                    line_copy(flow, origin, True).start()

                after(origin)

            @pl.when(row + hops < rows_count)
            def _():
                origin = row + hops
                line_copy(flow, origin, False).wait_recv()

                @pl.when((row >= 1) & (hops < limit))
                def _():
                    line_copy(flow, origin, False).start()

                after(origin)

        low, high = (1 + (rows_count - 1) * k // 3 for k in (third - 1, third))
        loop(high - low, lambda i: one(low + i))

    def thirds(third, body):
        def one(i):
            hops = 1 + i // 2
            origin = row + hops * (1 - 2 * lax.rem(i, 2))

            @pl.when((origin >= 0) & (origin < rows_count))
            def _():
                body(origin)

        low, high = (2 * ((rows_count - 1) * k // 3) for k in (third, third + 1))
        loop(high - low, lambda i: one(low + i))

    def nth_other(i):
        above, below = rows_count - 1 - row, row
        both = 2 * jnp.minimum(above, below)
        near_side = jnp.where(lax.rem(i, 2) == 0, 1 + i // 2, -(1 + i // 2))
        far_side = (1 + i - both // 2) * jnp.where(above > below, 1, -1)
        return row + jnp.where(i < both, near_side, far_side)

    def others(body, after=()):
        def one(i):
            body(nth_other(i), i)
            for number, action in after:
                pl.when(i == number - 1)(action)

        loop(rows_count - 1, one)

    def finish_flow(flow, limit=None, halves=True):
        limit = rows_count if limit is None else limit

        def one(origin):
            @pl.when((origin <= row) & (row + 1 < rows_count) & (row - origin < limit))
            def _():
                line_copy(flow, origin, True).wait_send()

            @pl.when((origin >= row) & (row >= 1) & (origin - row < limit))
            def _():
                line_copy(flow, origin, False).wait_send()

            @pl.when(origin != row)
            def _():
                if flow < 2:
                    for step in direct_steps:
                        plane_copy(flow, origin, step).wait_send()
                    if balanced and halves:
                        for half in range(2):
                            half_copy(flow, origin, half).wait_send()
                if flow == 4:
                    for step in [0] + steps:
                        engine_copy(origin, step).wait_send()

        loop(rows_count, one)

    def own_stores(flow, own):
        return [
            pltpu.make_async_copy(
                own.at[:, pl.ds(i * part, part)], flows[flow].at[row, i], store.at[flow * count + i]
            )
            for i in range(count)
        ]

    def scatter(kind, step):
        peer = partner(me, step, count)[0]
        return pltpu.make_async_remote_copy(
            src_ref=term.at[peer],
            dst_ref=arrived.at[kind, step - 1],
            send_sem=send.at[kind, step],
            recv_sem=recv.at[kind, step],
            device_id=at(section, peer),
            device_id_type=MESH,
        )

    def gather(number, step, target):
        peer = partner(me, step, count)[0]
        return pltpu.make_async_remote_copy(
            src_ref=parts.at[number, 0],
            dst_ref=parts.at[number, step],
            send_sem=part_send.at[number, step],
            recv_sem=part_recv.at[number, step],
            device_id=at(target, peer),
            device_id_type=MESH,
        )

    def back(number, step):
        return pltpu.make_async_remote_copy(
            src_ref=parts.at[number, step],
            dst_ref=parts.at[number, step],
            send_sem=back_send.at[number, step],
            recv_sem=back_recv.at[number, step],
            device_id=at(1 - section, me),
            device_id_type=MESH,
        )

    def place(number, step, target):
        owner = partner(me, step, count)[1]
        target[:, tile_of(owner, part)] = parts[number, step]

    def reduce(kind, number, with_input):
        for step in steps:
            scatter(kind, step).wait_recv()

        def rows_of(i):
            rows = tile_of(i, row_tile)
            total = term[me, rows, :].astype(F32)
            if with_input:
                total = total + xv[rows, tile_of(me, part)].astype(F32)
            for step in steps:
                total = total + arrived[kind, step - 1, rows, :].astype(F32)
            parts[number, 0, rows, :] = total.astype(BF16)

        loop(row_tiles, rows_of)

    def finish_sends(kind):
        for step in steps:
            scatter(kind, step).wait_send()

    def to_other_section(number):
        for step in steps[::-1] + [0]:
            gather(number, step, 1 - section).start()

    def from_own_section(number, target):
        place(number, 0, target)
        for step in steps:
            back(number, step).wait_recv()
            place(number, step, target)
        for step in [0] + steps:
            gather(number, step, 1 - section).wait_send()

    def from_other_section(number, target):
        gather(number, 0, 1 - section).wait_recv()
        place(number, 0, target)
        for step in steps:
            gather(number, step, 1 - section).wait_recv()
            back(number, step).start()
            place(number, step, target)

    def finish_back(number):
        for step in steps:
            back(number, step).wait_send()

    def start_within(number):
        for step in steps[::-1]:
            gather(number, step, section).start()

    def finish_within(number, target):
        place(number, 0, target)
        for step in steps:
            gather(number, step, section).wait_recv()
            place(number, step, target)
        for step in steps:
            gather(number, step, section).wait_send()

    def each_chunk(kind, compute, between=None, sends=True):
        def chunk(i):
            step = count - 1 - i
            owner = partner(me, step, count)[0]
            loop(part // TILE, lambda j: compute(owner, j))

            @pl.when((step > 0) & sends)
            def _():
                scatter(kind, step).start()

            if between is not None:
                pl.when(i == count // 2 - 1)(between)

        loop(count, chunk)

    lane = lanes_of((1, LANES)).astype(F32)
    exponent = jnp.where(lane < ROT // 2, lane, lane - ROT // 2)
    frequency = jnp.exp(exponent * (-2.0 * math.log(10000.0) / ROT))
    row_index = lax.broadcasted_iota(jnp.int32, (length, length), 0)
    column_index = lax.broadcasted_iota(jnp.int32, (length, length), 1)

    def segments_of(values):
        across = values.astype(F32)
        down = jnp.sum(jnp.where(row_index == column_index, across, 0.0), axis=1, keepdims=True)
        return across, down

    def fill_tables(slot, values_of):
        for b in range(batch):
            rows = pl.ds(b * length, length)
            across, down = segments_of(values_of(b))
            number_of = jnp.sum((across < down).astype(F32), axis=1, keepdims=True)
            index = lax.broadcasted_iota(jnp.int32, (length, 1), 0).astype(F32)
            angles = (index - number_of) * frequency
            inside = lanes_of((length, LANES)) < ROT
            tables[slot, rows, :LANES] = jnp.where(inside, jnp.cos(angles), 1.0)
            tables[slot, rows, LANES:] = jnp.where(inside, jnp.sin(angles), 0.0)

    fill_tables(0, lambda b: seg_row[b : b + 1, :])

    def softmax(projected, values, b, h):
        rows, columns = tile_of(b, length), tile_of(h, HEAD)
        across, down = segments_of(values)
        allowed = (across == down) & (column_index <= row_index)
        scores = dot_nt(projected[0, rows, columns], projected[1, rows, columns]) * scale
        scores = jnp.where(allowed, scores, -jnp.inf)
        row_max = jnp.max(scores, axis=-1, keepdims=True)
        total = jnp.sum(jnp.exp(scores - row_max), axis=-1, keepdims=True)
        return jnp.exp(scores - (row_max + jnp.log(total)))

    def attend(prob, projected, target, b, h):
        rows, columns = tile_of(b, length), tile_of(h, HEAD)
        target[rows, columns] = dot(prob.astype(BF16), projected[2, rows, columns]).astype(BF16)

    def attend_backward(prob, projected, slot, target, b, h):
        rows, columns = tile_of(b, length), tile_of(h, HEAD)
        cosine, sine = tables[slot, rows, :LANES], tables[slot, rows, LANES:]
        queries, keys, values = (projected[k, rows, columns] for k in range(3))
        d_context = dctx[rows, columns]
        d_values = dot_tn(prob.astype(BF16), d_context)
        d_probs = dot_nt(d_context, values)
        delta = jnp.sum(prob * d_probs, axis=-1, keepdims=True)
        d_scores = (prob * (d_probs - delta) * scale).astype(BF16)
        for k, gradient in ((0, dot(d_scores, keys)), (1, dot_tn(d_scores, queries))):
            first = unrotated(gradient[:, :LANES], cosine, sine)
            start = pl.multiple_of(h * HEAD, HEAD)
            target[k, rows, pl.ds(start, LANES)] = first.astype(BF16)
            start = pl.multiple_of(h * HEAD + LANES, LANES)
            target[k, rows, pl.ds(start, HEAD - LANES)] = gradient[:, LANES:].astype(BF16)
        target[2, rows, columns] = d_values.astype(BF16)

    def each_pair(body):
        def row_of(b):
            for h in range(heads):
                body(b, h)

        loop(batch, row_of)

    def project(projected, slot):
        def rotary_head(i):
            which, h = i // heads, lax.rem(i, heads)
            tile = dot(attn_in[...], w3[which, :, tile_of(h, HEAD)])
            first = rotated(tile[:, :LANES], tables[slot, :, :LANES], tables[slot, :, LANES:])
            start = pl.multiple_of(h * HEAD, HEAD)
            projected[which, :, pl.ds(start, LANES)] = first.astype(BF16)
            start = pl.multiple_of(h * HEAD + LANES, LANES)
            projected[which, :, pl.ds(start, HEAD - LANES)] = tile[:, LANES:].astype(BF16)

        def value_head(h):
            columns = tile_of(h, HEAD)
            projected[2, :, columns] = dot(attn_in[...], w3[2, :, columns]).astype(BF16)

        loop(2 * heads, rotary_head)
        loop(heads, value_head)

    def segment_copy(step):
        return pltpu.make_async_remote_copy(
            src_ref=seg_row,
            dst_ref=segments.at[row],
            send_sem=segment_send.at[step],
            recv_sem=segment_recv.at[step],
            device_id={"dp": lax.rem(row + step, rows_count)},
            device_id_type=MESH,
        )

    def d_context_head(h):
        dctx[:, tile_of(h, HEAD)] = dot_nt(gbv[...], wo[tile_of(h, HEAD), :]).astype(BF16)

    def meet():
        pl.semaphore_wait(barrier, 2 * count - 1 + rows_count - 1)
        for step in range(1, rows_count):
            segment_copy(step).start()


    @pl.when(section == 0)
    def _():
        x_load.wait()

    @pl.when(section == 1)
    def _():
        meet()
        start_flow(4, x_hbm)
        if balanced:
            start_flow(6, x_hbm)
        go_load.wait()
        out_load.wait()
        loop(heads, d_context_head)
        if balanced:
            hop(6, 1)
        hop(4, 1, send_engine_first)
        fc2_load.wait()

        def d_act_tile(i):
            columns = tile_of(i, TILE)
            slope[:, columns] = dot_nt(gbv[...], w2[columns, :])

        loop(hidden_width // TILE, d_act_tile)
        for third in (2, 3):
            if balanced:
                hop(6, third)
            hop(4, third)
            if third == 2:
                start_flow(1, gbv)
                if balanced:
                    start_flow(5, gbv)
        hop(1, 1)
        if balanced:
            hop(5, 1)
        from_other_section(0, xv)
        start_flow(0, xv)
        for third in range(3):
            thirds(third, send_engine_later)

    for copy in own_stores(0, xv):
        copy.start()

    def norm_rows(i):
        rows = tile_of(i, row_tile)
        normed, mean, inv_std = row_norm(xv[rows, :].astype(F32))
        means[rows, :] = mean
        inv_stds[rows, :] = inv_std
        attn_in[rows, :] = (normed * gains[0:1, :] + biases[0:1, :]).astype(BF16)
        mlp_in[rows, :] = (normed * gains[1:2, :] + biases[1:2, :]).astype(BF16)

    loop(row_tiles, norm_rows)

    for copy in qkv_loads:
        copy.wait()
    project(qkv, 0)

    def own_attention(b, h):
        prob = softmax(qkv, seg_row[pl.ds(b, 1), :], b, h)
        probs[b * heads + h] = prob
        attend(prob, qkv, context, b, h)

    each_pair(own_attention)

    @pl.when(section == 1)
    def _():
        hop(0, 1, send_plane_of(0))
        hop(1, 2)
        if balanced:
            hop(5, 2)


    def fc1_block(i):
        fc1_load(i).wait()

        def fc1_tile(j):
            columns = tile_of(i * (block // TILE) + j, TILE)
            value, derivative = gelu_parts(dot(mlp_in[...], w1[:, columns]))
            act[:, columns] = value.astype(BF16)

            @pl.when(section == 0)
            def _():
                slope[:, columns] = derivative

            @pl.when(section == 1)
            def _():
                dh[:, columns] = (slope[:, columns] * derivative).astype(BF16)

        loop(block // TILE, fc1_tile)

    loop(blocks, fc1_block)

    @pl.when(section == 1)
    def _():
        hop(0, 2, send_plane_of(0))

    @pl.when(section == 0)
    def _():
        out_load.wait()
        fc2_load.wait()
        go_load.wait()

    tiles = hidden_width // TILE

    def act_store(origin, i):
        columns = tile_of(i, TILE)
        return pltpu.make_async_copy(
            act_rest.at[:, columns], act_all.at[origin, :, columns], rest_store.at[0]
        )

    def dh_store(origin, i):
        columns = tile_of(i, TILE)
        return pltpu.make_async_copy(
            act_rest.at[:, columns], dh_all.at[origin, :, columns], rest_store.at[0]
        )

    def slope_store(origin, i):
        columns = tile_of(i, TILE)
        return pltpu.make_async_copy(
            slope_rest.at[:, columns], slope_all.at[origin, :, columns], rest_store.at[1]
        )

    def load_block(flow, origin):
        if flow == 0:

            @pl.when(section == 0)
            def _():
                for step in [0] + steps:
                    engine_copy(origin, step).wait_recv()

            pl.when(section == 1)(lambda: wait_plane(flow, origin))
        else:
            pl.when(section == 0)(lambda: wait_plane(flow, origin))

            @pl.when(section == 1)
            def _():
                for step in direct_steps:
                    plane_copy(flow, origin, step).wait_recv()

        copies = [
            pltpu.make_async_copy(
                flows[flow].at[origin, i], attn_in.at[:, pl.ds(i * part, part)], rest_load.at[i]
            )
            for i in range(count)
        ]
        for copy in copies:
            copy.start()
        return copies

    def attention_stores(origin):
        return [
            pltpu.make_async_copy(qkv_rest, qkv_all.at[origin], rest_load.at[count + 1]),
            pltpu.make_async_copy(context_rest, context_all.at[origin], rest_load.at[count + 2]),
        ]

    def far_of(origin):
        return (section == 0) & ((origin - row > near) | (row - origin > near))

    def rest_forward(origin, index):
        for copy in load_block(0, origin):
            copy.wait()

        def norm_rows(i):
            rows = tile_of(i, row_tile)
            normed, mean, inv_std = row_norm(attn_in[rows, :].astype(F32))
            first = lanes_of((row_tile, LANES)) == 0
            stats_all[origin, rows, :] = jnp.where(first, mean, inv_std)
            mlp_in[rows, :] = (normed * gains[1:2, :] + biases[1:2, :]).astype(BF16)
            attn_in[rows, :] = (normed * gains[0:1, :] + biases[0:1, :]).astype(BF16)

        loop(row_tiles, norm_rows)

        @pl.when(section == 0)
        def _():
            fill_tables(1, lambda b: segments[origin, b : b + 1, :])
            project(qkv_rest, 1)

            def attention(b, h):
                prob = softmax(qkv_rest, segments[origin, pl.ds(b, 1), :], b, h)
                attend(prob, qkv_rest, context_rest, b, h)

            each_pair(attention)
            for copy in attention_stores(origin):
                copy.start()

        def tile(i):
            columns = tile_of(i, TILE)
            value, derivative = gelu_parts(dot(mlp_in[...], w1[:, columns]))
            act_rest[:, columns] = value.astype(BF16)
            slope_rest[:, columns] = derivative
            act_store(origin, i).start()
            slope_store(origin, i).start()

        loop(tiles, tile)

        pltpu.make_async_copy(act_rest, act_all.at[origin], rest_store.at[0]).wait()
        pltpu.make_async_copy(slope_rest, slope_all.at[origin], rest_store.at[1]).wait()

        @pl.when(section == 0)
        def _():
            for copy in attention_stores(origin):
                copy.wait()

    def slope_load(origin):
        return pltpu.make_async_copy(slope_all.at[origin], slope_rest, rest_load.at[count])

    def rest_backward(origin, index):
        copies = load_block(1, origin)
        for copy in copies + [slope_load(origin)]:
            copy.wait()

        def tile(i):
            columns = tile_of(i, TILE)
            d_act = dot_nt(attn_in[...], w2[columns, :])
            act_rest[:, columns] = (d_act * slope_rest[:, columns]).astype(BF16)
            dh_store(origin, i).start()

        qkv_load = pltpu.make_async_copy(qkv_all.at[origin], qkv_rest, rest_load.at[count + 1])
        dproj_store = pltpu.make_async_copy(
            dproj_rest, dproj_all.at[origin], rest_load.at[count + 2]
        )
        far = far_of(origin)
        pl.when(far)(qkv_load.start)
        loop(tiles, tile)

        @pl.when(index < rows_count - 2)
        def _():
            slope_load(nth_other(index + 1)).start()

        @pl.when(far)
        def _():
            qkv_load.wait()
            fill_tables(1, lambda b: segments[origin, b : b + 1, :])

            def head(h):
                columns = tile_of(h, HEAD)
                dctx[:, columns] = dot_nt(attn_in[...], wo[columns, :]).astype(BF16)

            loop(heads, head)

            def attention(b, h):
                prob = softmax(qkv_rest, segments[origin, pl.ds(b, 1), :], b, h)
                attend_backward(prob, qkv_rest, 1, dproj_rest, b, h)

            each_pair(attention)
            dproj_store.start()
            dproj_store.wait()

        pltpu.make_async_copy(act_rest, dh_all.at[origin], rest_store.at[0]).wait()

    def out_tile(owner, j):
        columns = tile_of(owner * (part // TILE) + j, TILE)
        total = dot(context[...], wo[:, columns]) + dot(act[...], w2[:, columns])
        term[owner, :, tile_of(j, TILE)] = total.astype(BF16)

    def own_stats(i):
        rows = tile_of(i, row_tile)
        first = lanes_of((row_tile, LANES)) == 0
        stats_all[row, rows, :] = jnp.where(first, means[rows, :], inv_stds[rows, :])

    layer_store = pltpu.make_async_copy(other, layer_out, store.at[2 * count + 4])

    def grad_store(i):
        rows = tile_of(i, row_tile)
        return pltpu.make_async_copy(slope.at[rows, :], input_grad.at[rows, :], grad_sems.at[0])

    transposed_stores = [
        pltpu.make_async_copy(attn_t, attn_out, store.at[2 * count + 6]),
        pltpu.make_async_copy(mlp_t, mlp_out, store.at[2 * count + 7]),
    ]
    width_mine = width // rows_count

    def transposed_inputs():
        for copy in own_stores(0, xv):
            copy.wait()
        start = row * width_mine
        chunk, offset = start // part, pl.multiple_of(lax.rem(start, part), LANES)
        loads = [
            pltpu.make_async_copy(
                x_all.at[i, chunk, :, pl.ds(offset, width_mine)], x_mine.at[i], slice_load.at[i]
            )
            for i in range(rows_count)
        ]
        for copy in loads:
            copy.start()
        for copy in loads:
            copy.wait()
        all_tokens = rows_count * tokens

        def columns_of(i):
            columns = tile_of(i, LANES)
            mean = stats_all[:, :, 0:1].reshape(all_tokens, 1)
            inv_std = stats_all[:, :, 1:2].reshape(all_tokens, 1)
            values = x_mine[:, :, columns].reshape(all_tokens, LANES).astype(F32)
            normed = (values - mean) * inv_std
            whole = tile_of(start // LANES + i, LANES)
            for j, target in enumerate((attn_t, mlp_t)):
                scaled = normed * gains[j : j + 1, whole] + biases[j : j + 1, whole]
                target[columns, :] = scaled.astype(BF16).T

        loop(width_mine // LANES, columns_of)
        for copy in transposed_stores:
            copy.start()


    @pl.when(section == 0)
    def _():
        meet()
        each_chunk(0, out_tile)
        reduce(0, 0, True)
        to_other_section(0)
        finish_sends(0)
        for step in range(1, rows_count):
            segment_copy(step).wait_recv()
        others(rest_forward)
        from_own_section(0, other)
        layer_store.start()
        from_other_section(1, full)

        def gradient_rows(i):
            rows = tile_of(i, row_tile)
            normed, _, inv_std = row_norm(other[rows, :].astype(F32))
            dx = row_norm_backward(full[rows, :].astype(F32), normed, inv_std)
            gbv[rows, :] = (gbv[rows, :].astype(F32) + dx).astype(BF16)

        loop(row_tiles, gradient_rows)
        start_flow(1, gbv)
        finish_back(1)

        def d_hidden_tile(i):
            columns = tile_of(i, TILE)
            d_act = dot_nt(gbv[...], w2[columns, :])
            dh[:, columns] = (d_act * slope[:, columns]).astype(BF16)

        loop(hidden_width // TILE, d_hidden_tile)
        loop(heads, d_context_head)


    each_pair(lambda b, h: attend_backward(probs[b * heads + h], qkv, 0, dproj, b, h))

    @pl.when(section == 0)
    def _():
        hop(1, 1, send_plane_of(1))

    @pl.when(section == 1)
    def _():
        start_flow(3, dproj)

    def gradient_tile(owner, j):
        columns = tile_of(owner * (part // TILE) + j, TILE)
        d_attn = dot_nt(dproj[0], w3[0, columns, :])
        d_attn = d_attn + dot_nt(dproj[1], w3[1, columns, :])
        d_attn = d_attn + dot_nt(dproj[2], w3[2, columns, :])
        d_mlp = dot_nt(dh[...], w1[columns, :])
        normed = (xv[:, columns].astype(F32) - means[...]) * inv_stds[...]
        total = d_attn * gains[0:1, columns] + d_mlp * gains[1:2, columns]
        term[owner, :, tile_of(j, TILE)] = total.astype(BF16)
        vectors[0:1, columns] = jnp.sum(d_attn * normed, axis=0, keepdims=True)
        vectors[1:2, columns] = jnp.sum(d_mlp * normed, axis=0, keepdims=True)
        vectors[2:3, columns] = jnp.sum(d_attn, axis=0, keepdims=True)
        vectors[3:4, columns] = jnp.sum(d_mlp, axis=0, keepdims=True)

    def second_hop():
        @pl.when(section == 0)
        def _():
            thirds(0, relay_plane_of(1))
            hop(1, 2, send_plane_of(1))

    each_chunk(1, gradient_tile, second_hop, section == 1)

    outs = [
        (act, act_all.at[row]),
        (context, context_all.at[row]),
        (dh, dh_all.at[row]),
        (dproj, dproj_all.at[row]),
    ]
    stores = own_stores(1, gbv)
    stores += [
        pltpu.make_async_copy(a, b, store.at[2 * count + i]) for i, (a, b) in enumerate(outs)
    ]
    for copy in stores:
        copy.start()

    def sum_copy(step):
        peer = partner(me, step, count)[0]
        return pltpu.make_async_remote_copy(
            src_ref=vectors,
            dst_ref=plane_vectors.at[step],
            send_sem=sum_send.at[step],
            recv_sem=sum_recv.at[step],
            device_id=at(section, peer),
            device_id_type=MESH,
        )

    mine = width // rows_count

    def slice_copy(step):
        target = lax.rem(row + step, rows_count)
        return pltpu.make_async_remote_copy(
            src_ref=plane_vectors.at[0, :, tile_of(target, mine)],
            dst_ref=slices.at[step],
            send_sem=slice_send.at[step],
            recv_sem=slice_recv.at[step],
            device_id={"dp": target},
            device_id_type=MESH,
        )

    for step in steps:
        sum_copy(step).start()

    def sum_plane():
        total = vectors[...]
        for step in steps:
            sum_copy(step).wait_recv()
            total = total + plane_vectors[step]
        plane_vectors[0] = total
        for step in range(1, rows_count):
            slice_copy(step).start()

    sum_stores = [
        pltpu.make_async_copy(sums.at[0], gain_grads, sum_store.at[0]),
        pltpu.make_async_copy(sums.at[1], bias_grads, sum_store.at[1]),
    ]

    def sum_line():
        total = plane_vectors[0, :, tile_of(row, mine)]
        for step in range(1, rows_count):
            slice_copy(step).wait_recv()
            total = total + slices[step]
        sums[0] = total[:2]
        sums[1] = total[2:]
        for copy in sum_stores:
            copy.start()
        for step in range(1, rows_count):
            slice_copy(step).wait_send()
        for step in steps:
            sum_copy(step).wait_send()


    def input_gradient():
        def rows_of(i):
            rows = tile_of(i, row_tile)
            inv_std = inv_stds[rows, :]
            normed = (xv[rows, :].astype(F32) - means[rows, :]) * inv_std
            dx = row_norm_backward(full[rows, :].astype(F32), normed, inv_std)
            slope[rows, :] = gbv[rows, :].astype(F32) + dx
            grad_store(i).start()

        loop(row_tiles, rows_of)

    @pl.when(section == 0)
    def _():
        slope_load(nth_other(0)).start()
        loop(row_tiles, own_stats)
        transposed_inputs()
        hop(1, 3, send_plane_of(1))
        start_flow(3, dproj)
        at_end = (row == 0) | (row == rows_count - 1)
        pl.when(at_end)(lambda: thirds(1, relay_plane_of(1)))

        def after_first():
            pl.when(jnp.logical_not(at_end))(lambda: thirds(1, relay_plane_of(1)))
            thirds(2, relay_plane_of(1))
            for step in steps[::-1]:
                scatter(1, step).start()
            sum_plane()

        def after_second():
            reduce(1, 2, False)
            start_within(2)
            hop(3, 1, limit=near)
            sum_line()

        others(rest_backward, [(1, after_first), (2, after_second)])
        finish_within(2, full)
        finish_sends(1)
        input_gradient()
        hop(3, 2, limit=near)

    @pl.when(section == 1)
    def _():
        finish_back(0)
        reduce(1, 1, False)
        to_other_section(1)
        thirds(0, relay_plane_of(0))
        hop(0, 3, send_plane_of(0))
        thirds(1, relay_plane_of(0))
        finish_sends(1)
        each_chunk(0, out_tile, None, False)
        hop(3, 1)
        hop(1, 3)
        if balanced:
            hop(5, 3)
        start_flow(2, context)
        loop(row_tiles, own_stats)
        from_own_section(1, full)
        for step in steps[::-1]:
            scatter(0, step).start()
        sum_plane()

        def share_gradients():
            for third in range(3):
                thirds(third, send_plane_of(1))
            hop(3, 2)
            hop(2, 1)

        others(
            rest_forward, [(1, lambda: thirds(2, relay_plane_of(0))), (2, share_gradients)]
        )
        slope_load(nth_other(0)).start()
        input_gradient()

        def after_second():
            transposed_inputs()
            reduce(0, 2, True)
            start_within(2)
            sum_line()
            hop(2, 2)

        others(rest_backward, [(2, after_second)])
        finish_within(2, other)
        layer_store.start()
        hop(3, 3)
        hop(2, 3)
        finish_sends(0)

    for copy in stores + [layer_store] + transposed_stores + sum_stores:
        copy.wait()
    pltpu.make_async_copy(slope, input_grad, grad_sems.at[0]).wait()
    @pl.when(section == 0)
    def _():
        finish_flow(1)
        finish_flow(3, near)

    @pl.when(section == 1)
    def _():
        for step in range(1, rows_count):
            segment_copy(step).wait_recv()
        finish_flow(1, halves=False)
        for flow in (0, 2, 3, 4) + ((5, 6) if balanced else ()):
            finish_flow(flow)

    for step in range(1, rows_count):
        segment_copy(step).wait_send()


def chain(attn_input, grad_output, segment_ids, weights):
    w_qkv, w_out, w_fc1, w_fc2, gains, biases = weights
    batch, length, width = attn_input.shape
    tokens = batch * length
    count = lax.axis_size("tensor")
    inner, hidden = w_qkv.shape[2], w_fc1.shape[1]
    part = width // count
    heads = inner // HEAD
    anywhere, vmem = pl.BlockSpec(memory_space=pl.ANY), pl.BlockSpec(memory_space=pltpu.VMEM)
    like = jax.ShapeDtypeStruct
    rows_count = lax.axis_size("dp")
    wide, narrow = (tokens, width), (tokens, inner)
    dma = pltpu.SemaphoreType.DMA
    return pl.pallas_call(
        functools.partial(chain_kernel, count, batch),
        out_shape=[
            like(wide, BF16),
            like(wide, F32),
            like((2, width // rows_count), F32),
            like((2, width // rows_count), F32),
            like((rows_count, count, tokens, part), BF16),
            like((rows_count, count, tokens, part), BF16),
            like((rows_count, tokens, inner), BF16),
            like((rows_count, 3, tokens, inner), BF16),
            like((rows_count, tokens, hidden), BF16),
            like((rows_count, tokens, hidden), BF16),
            like((width // rows_count, rows_count * tokens), BF16),
            like((width // rows_count, rows_count * tokens), BF16),
            like((rows_count, tokens, hidden), F32),
            like((rows_count, 2, tokens, part), BF16),
            like((rows_count, 3, tokens, inner), BF16),
        ],
        in_specs=[anywhere, anywhere, vmem] + [anywhere] * 4 + [vmem, vmem],
        out_specs=[anywhere] * 10 + [anywhere] * 5,
        scratch_shapes=[
            pltpu.VMEM((3, width, inner), BF16),
            pltpu.VMEM((inner, width), BF16),
            pltpu.VMEM((width, hidden), BF16),
            pltpu.VMEM((hidden, width), BF16),
            pltpu.VMEM(wide, BF16),
            pltpu.VMEM(wide, BF16),
            pltpu.VMEM(wide, BF16),
            pltpu.VMEM(wide, BF16),
            pltpu.VMEM(wide, BF16),
            pltpu.VMEM((3, tokens, inner), BF16),
            pltpu.VMEM(narrow, BF16),
            pltpu.VMEM((batch * heads, length, length), F32),
            pltpu.VMEM((tokens, hidden), BF16),
            pltpu.VMEM((tokens, hidden), F32),
            pltpu.VMEM((tokens, hidden), BF16),
            pltpu.VMEM(narrow, BF16),
            pltpu.VMEM((3, tokens, inner), BF16),
            pltpu.VMEM((tokens, 1), F32),
            pltpu.VMEM((tokens, 1), F32),
            pltpu.VMEM((2, tokens, 2 * LANES), F32),
            pltpu.VMEM((count, tokens, part), BF16),
            pltpu.VMEM((2, count - 1, tokens, part), BF16),
            pltpu.VMEM((3, count, tokens, part), BF16),
            pltpu.VMEM(wide, BF16),
            pltpu.VMEM((tokens, hidden), BF16),
            pltpu.VMEM((tokens, hidden), F32),
            pltpu.VMEM((rows_count, tokens, LANES), F32),
            pltpu.VMEM((rows_count, tokens, width // rows_count), BF16),
            pltpu.VMEM((width // rows_count, rows_count * tokens), BF16),
            pltpu.VMEM((width // rows_count, rows_count * tokens), BF16),
            pltpu.VMEM((4, width), F32),
            pltpu.VMEM((count, 4, width), F32),
            pltpu.VMEM((rows_count, 4, width // rows_count), F32),
            pltpu.VMEM((rows_count, batch, length), jnp.int32),
            pltpu.VMEM((3, tokens, inner), BF16),
            pltpu.VMEM((3, tokens, inner), BF16),
            pltpu.VMEM(narrow, BF16),
            dma((11,)),
            dma((2 * count + 8,)),
            dma((2, count)),
            dma((2, count)),
            dma((4, count)),
            dma((4, count)),
            dma((2, count)),
            dma((2, count)),
            dma((7, 2, rows_count)),
            dma((7, rows_count)),
            dma((2, rows_count, count)),
            dma((2, rows_count, count)),
            dma((count + 3,)),
            dma((2,)),
            dma((count,)),
            dma((count,)),
            dma((rows_count,)),
            dma((rows_count,)),
            dma((rows_count, count)),
            dma((rows_count,)),
            dma((rows_count,)),
            dma((rows_count,)),
            dma((1,)),
            pltpu.VMEM((2, 2, width // rows_count), F32),
            dma((2,)),
        ],
        compiler_params=pltpu.CompilerParams(
            collective_id=0, has_side_effects=True, vmem_limit_bytes=67_043_328
        ),
        name="chain",
    )(
        attn_input.reshape(wide),
        grad_output.reshape(wide),
        segment_ids,
        jnp.transpose(w_qkv, (1, 0, 2)),
        w_out,
        w_fc1,
        w_fc2,
        gains,
        biases,
    )


def weight_kernel(*refs):
    (
        gb_all, attn_in, mlp_in, context_all, dproj_all, act_all, dh_all,
        layer_in, grad_in, gain_in, bias_in,
        g_qkv, g_out, g_fc1, g_fc2, layer_out, input_grad, gain_out, bias_out,
        gb_mine, context, dproj, act, attn_t, mlp_t, r_qkv, r_out, r_fc1, r_fc2,
        layer, grad, load, act_load, dh_load, store, through, gb_load,
    ) = refs
    blocks, tokens, mine = gb_mine.shape
    rows = blocks * tokens
    part = gb_all.shape[3]
    inner, hidden = context.shape[2], act.shape[2]
    start = lax.axis_index("dp") * mine
    chunk, offset = start // part, pl.multiple_of(lax.rem(start, part), LANES)
    piece = hidden // 4

    def slice_loads(source, target, sems):
        return [
            pltpu.make_async_copy(
                source.at[i, chunk, :, pl.ds(offset, mine)], target.at[i], sems.at[i]
            )
            for i in range(blocks)
        ]

    def piece_load(source, target, sems, i):
        columns = pl.ds(i * piece, piece)
        return pltpu.make_async_copy(source.at[:, :, columns], target.at[:, :, columns], sems.at[i])

    gb_loads = slice_loads(gb_all, gb_mine, gb_load)
    in_loads = [
        pltpu.make_async_copy(attn_in, attn_t, load.at[0]),
        pltpu.make_async_copy(mlp_in, mlp_t, load.at[1]),
    ]
    context_load = pltpu.make_async_copy(context_all, context, load.at[2])
    dproj_load = pltpu.make_async_copy(dproj_all, dproj, load.at[3])
    act_loads = [piece_load(act_all, act, act_load, i) for i in range(4)]
    dh_loads = [piece_load(dh_all, act, dh_load, i) for i in range(4)]
    gain_out[...] = gain_in[...]
    bias_out[...] = bias_in[...]
    ins = [
        pltpu.make_async_copy(layer_in, layer, through.at[0]),
        pltpu.make_async_copy(grad_in, grad, through.at[1]),
    ]
    outs = [
        pltpu.make_async_copy(layer, layer_out, through.at[2]),
        pltpu.make_async_copy(grad, input_grad, through.at[3]),
    ]
    for copy in gb_loads + [context_load]:
        copy.start()

    def out_copy(source, target, index):
        return pltpu.make_async_copy(source, target, store.at[index])

    for copy in gb_loads + [context_load]:
        copy.wait()
    for copy in act_loads + in_loads[1:]:
        copy.start()
    gb_rows = gb_mine[...].reshape(rows, mine)

    def out_tile(i):
        tile = tile_of(i, TILE)
        r_out[tile, :] = dot_tn(context[:, :, tile].reshape(rows, TILE), gb_rows)

    loop(inner // TILE, out_tile)
    copies = [out_copy(r_out, g_out, 0)]
    copies[0].start()

    def fc2_copy(i):
        tile = tile_of(i, TILE)
        return out_copy(r_fc2.at[tile, :], g_fc2.at[tile, :], 1 + i)

    def fc2_tile(i):
        tile = tile_of(i, TILE)
        r_fc2[tile, :] = dot_tn(act[:, :, tile].reshape(rows, TILE), gb_mine[...].reshape(rows, mine))
        fc2_copy(i).start()

    per = piece // TILE
    for i in range(4):
        act_loads[i].wait()
        loop(per, lambda j: fc2_tile(i * per + j))
        dh_loads[i].start()
    for copy in [dproj_load] + in_loads[:1] + ins:
        copy.start()

    def fc1_copy(i):
        tile = tile_of(i, TILE)
        return out_copy(r_fc1.at[:, tile], g_fc1.at[:, tile], 1 + hidden // TILE + i)

    def fc1_tile(i):
        tile = tile_of(i, TILE)
        r_fc1[:, tile] = dot(mlp_t[...], act[:, :, tile].reshape(rows, TILE))
        fc1_copy(i).start()

    in_loads[1].wait()
    for i in range(4):
        dh_loads[i].wait()
        loop(per, lambda j: fc1_tile(i * per + j))
    dproj_load.wait()
    in_loads[0].wait()
    for copy in ins:
        copy.wait()
    for copy in outs:
        copy.start()
    per = inner // TILE

    def qkv_copy(i):
        which, tile = i // per, tile_of(lax.rem(i, per), TILE)
        return out_copy(r_qkv.at[which, :, tile], g_qkv.at[which, :, tile], 1 + 2 * (hidden // TILE) + i)

    def qkv_tile(i):
        which, tile = i // per, tile_of(lax.rem(i, per), TILE)
        r_qkv[which, :, tile] = dot(attn_t[...], dproj[:, which, :, tile].reshape(rows, TILE))
        qkv_copy(i).start()

    loop(3 * per, qkv_tile)
    for copy in copies + outs:
        copy.wait()
    loop(hidden // TILE, lambda i: fc2_copy(i).wait())
    loop(hidden // TILE, lambda i: fc1_copy(i).wait())
    loop(3 * per, lambda i: qkv_copy(i).wait())


def weight_gradients(
    gb_all, attn_in, mlp_in, context_all, dproj_all, act_all, dh_all, *through
):
    blocks, count, tokens, part = gb_all.shape
    mine = count * part // lax.axis_size("dp")
    inner, hidden = context_all.shape[2], act_all.shape[2]
    anywhere, vmem = pl.BlockSpec(memory_space=pl.ANY), pl.BlockSpec(memory_space=pltpu.VMEM)
    shapes = [(3, mine, inner), (inner, mine), (mine, hidden), (hidden, mine)]
    dma = pltpu.SemaphoreType.DMA
    return pl.pallas_call(
        weight_kernel,
        out_shape=[jax.ShapeDtypeStruct(shape, F32) for shape in shapes]
        + [jax.ShapeDtypeStruct(value.shape, value.dtype) for value in through],
        in_specs=[anywhere] * 7
        + [anywhere, anywhere, vmem, vmem],
        out_specs=[anywhere] * 6 + [vmem, vmem],
        scratch_shapes=[
            pltpu.VMEM((blocks, tokens, mine), BF16),
            pltpu.VMEM((blocks, tokens, inner), BF16),
            pltpu.VMEM((blocks, 3, tokens, inner), BF16),
            pltpu.VMEM((blocks, tokens, hidden), BF16),
            pltpu.VMEM((mine, blocks * tokens), BF16),
            pltpu.VMEM((mine, blocks * tokens), BF16),
        ]
        + [pltpu.VMEM(shape, F32) for shape in shapes]
        + [pltpu.VMEM(value.shape, value.dtype) for value in through[:2]]
        + [
            dma((4,)),
            dma((4,)),
            dma((4,)),
            dma((1 + 2 * (hidden // TILE) + 3 * (inner // TILE),)),
            dma((4,)),
            dma((blocks,)),
        ],
        compiler_params=pltpu.CompilerParams(vmem_limit_bytes=67_043_328),
        name="weights",
    )(gb_all, attn_in, mlp_in, context_all, dproj_all, act_all, dh_all, *through)


def shards(
    block_input, grad_output, segment_ids, w_qkv, w_out, w_fc1, w_fc2, norm_gains, norm_biases
):
    batch, length, width = block_input.shape
    weights = (w_qkv[0], w_out[0], w_fc1[0], w_fc2[0], norm_gains[0], norm_biases[0])
    (
        layer_out, input_grads, gain_grads, bias_grads, _, gb_all, context, d_proj, activated,
        d_hidden, attn_in, mlp_in, *_,
    ) = chain(block_input, grad_output, segment_ids, weights)
    g_qkv, g_out, g_fc1, g_fc2, layer_out, input_grads, gain_grads, bias_grads = weight_gradients(
        gb_all, attn_in, mlp_in, context, d_proj, activated, d_hidden,
        layer_out, input_grads, gain_grads, bias_grads,
    )
    shape = (1, batch, length, width)
    return (
        layer_out.reshape(shape),
        input_grads.reshape(shape),
        jnp.transpose(g_qkv, (1, 0, 2))[None],
        g_out[None],
        g_fc1[None],
        g_fc2[None],
        gain_grads[None],
        bias_grads[None],
    )


def solution(mesh):
    return jax.shard_map(
        shards,
        mesh=mesh,
        in_specs=(
            P("dp", None, None),
            P("dp", None, None),
            P("dp", None),
            P("section", None, None, "tensor"),
            P("section", "tensor", None),
            P("section", None, "tensor"),
            P("section", "tensor", None),
            P("section", None, None),
            P("section", None, None),
        ),
        out_specs=(
            P("section", "dp", None, None),
            P("section", "dp", None, None),
            P("section", "dp", None, "tensor"),
            P("section", "tensor", "dp"),
            P("section", "dp", "tensor"),
            P("section", "tensor", "dp"),
            P("section", None, "dp"),
            P("section", None, "dp"),
        ),
        check_vma=False,
    )
```

```python
import functools
import math

import jax
import jax.numpy as jnp
from jax import lax
from jax.experimental import pallas as pl
from jax.experimental.pallas import tpu as pltpu
from jax.sharding import PartitionSpec as P

HEAD = 256
ROT = 64
LANES = 128
TILE = 256
NORM_EPSILON = 1e-05
MESH = pl.DeviceIdType.MESH
BF16 = jnp.bfloat16
F32 = jnp.float32


def partner(index, step, count):
    if count & (count - 1):
        return lax.rem(index + step, count), lax.rem(index + count - step, count)
    bit = 1
    while bit < count:
        index = index + ((step // bit) % 2) * (bit - 2 * bit * ((index // bit) % 2))
        bit *= 2
    return index, index


def loop(count, body, unroll=1):
    lax.fori_loop(0, count, lambda i, carry: (body(i), carry)[1], 0, unroll=unroll)


def tile_of(i, size):
    return pl.ds(pl.multiple_of(i * size, size), size)


def dot(left, right):
    return jnp.dot(left, right, preferred_element_type=jnp.float32)


def dot_nt(left, right):
    return lax.dot_general(left, right, (((1,), (1,)), ((), ())), preferred_element_type=jnp.float32)


def dot_tn(left, right):
    return lax.dot_general(left, right, (((0,), (0,)), ((), ())), preferred_element_type=jnp.float32)


def gelu_parts(hidden):
    normal_cdf = 0.5 * (1.0 + lax.erf(hidden * (1.0 / math.sqrt(2.0))))
    density = jnp.exp(-0.5 * hidden * hidden) * (1.0 / math.sqrt(2.0 * math.pi))
    return (hidden * normal_cdf, normal_cdf + hidden * density)


def lanes_of(shape):
    return lax.broadcasted_iota(jnp.int32, shape, len(shape) - 1)


def rotated(tile, cosine, sine):
    half = ROT // 2
    left, right = pltpu.roll(tile, LANES - half, 1), pltpu.roll(tile, half, 1)
    lane = lanes_of(tile.shape)
    turned = jnp.where(lane < half, -left, right)
    return tile * cosine + turned * sine


def unrotated(tile, cosine, sine):
    half = ROT // 2
    scaled = tile * sine
    left, right = pltpu.roll(scaled, LANES - half, 1), pltpu.roll(scaled, half, 1)
    lane = lanes_of(tile.shape)
    turned = jnp.where(lane < half, left, jnp.where(lane < ROT, -right, 0.0))
    return tile * cosine + turned


def row_norm(values):
    mean = jnp.mean(values, axis=-1, keepdims=True)
    centred = values - mean
    inv_std = lax.rsqrt(jnp.mean(centred * centred, axis=-1, keepdims=True) + NORM_EPSILON)
    return centred * inv_std, mean, inv_std


def row_norm_backward(summed, normed, inv_std):
    return inv_std * (
        summed
        - jnp.mean(summed, axis=-1, keepdims=True)
        - normed * jnp.mean(summed * normed, axis=-1, keepdims=True)
    )


def chain_kernel(count, batch, *refs):
    (
        x_hbm, go_hbm, seg_row, w3_hbm, wo_hbm, w1_hbm, w2_hbm, gains, biases,
        layer_out, input_grad, gain_grads, bias_grads, x_all, gb_all, context_all, dproj_all, act_all, dh_all, attn_out, mlp_out,
        slope_all, relay_x, qkv_all,
        w3, wo, w1, w2, xv, other, gbv, attn_in, mlp_in, qkv, context, probs, act, slope, dh, dctx,
        dproj, means, inv_stds, tables, term, arrived, parts, full, act_rest, slope_rest,
        stats_all, x_mine, attn_t, mlp_t, vectors, plane_vectors, slices, segments, qkv_rest, dproj_rest, context_rest,
        load, store, send, recv, part_send, part_recv, back_send, back_recv,
        line_send, line_recv, plane_send, plane_recv, rest_load, rest_store, sum_send, sum_recv,
        slice_send, slice_recv, engine_send, segment_send, segment_recv, slice_load, grad_sems, sums, sum_store,
    ) = refs
    section, me = lax.axis_index("section"), lax.axis_index("tensor")
    row, rows_count = lax.axis_index("dp"), lax.axis_size("dp")
    tokens, width = xv.shape
    length = tokens // batch
    heads = qkv.shape[2] // HEAD
    hidden_width = act.shape[1]
    part = width // count
    row_tile = 32 if tokens % 32 == 0 else 16
    row_tiles = tokens // row_tile
    scale = 1.0 / math.sqrt(HEAD)

    qkv_loads = [pltpu.make_async_copy(w3_hbm.at[k], w3.at[k], load.at[k]) for k in range(3)]
    blocks = 4
    block = hidden_width // blocks

    def fc1_load(i):
        columns = tile_of(i, block)
        return pltpu.make_async_copy(w1_hbm.at[:, columns], w1.at[:, columns], load.at[3 + i])

    out_load = pltpu.make_async_copy(wo_hbm, wo, load.at[7])
    fc2_load = pltpu.make_async_copy(w2_hbm, w2, load.at[8])
    x_load = pltpu.make_async_copy(x_hbm, xv, load.at[9])
    go_load = pltpu.make_async_copy(go_hbm, gbv, load.at[10])

    @pl.when(section == 0)
    def _():
        x_load.start()

    go_load.start()

    def start_out_loads():
        out_load.start()
        fc2_load.start()

    pl.when(section == 1)(start_out_loads)
    for copy in qkv_loads:
        copy.start()
    for i in range(blocks):
        fc1_load(i).start()
    pl.when(section == 0)(start_out_loads)

    def at(section, index):
        return {"section": section, "tensor": index}

    steps = list(range(1, count))
    barrier = pltpu.get_barrier_semaphore()
    for step in range(count):
        peer = partner(me, step, count)[0]
        pl.semaphore_signal(barrier, inc=1, device_id=at(1 - section, peer), device_id_type=MESH)
        if step:
            pl.semaphore_signal(barrier, inc=1, device_id=at(section, peer), device_id_type=MESH)

    for step in range(1, rows_count):
        pl.semaphore_signal(
            barrier,
            inc=1,
            device_id={"dp": lax.rem(row + step, rows_count)},
            device_id_type=MESH,
        )

    balanced = count == 4
    opposite = partner(me, count - 1, count)[0]
    flows = (x_all, gb_all)

    def place_of(flow, origin):
        return (
            lambda: x_all.at[origin, me],
            lambda: gb_all.at[origin, me],
            lambda: context_all.at[origin],
            lambda: dproj_all.at[origin],
            lambda: relay_x.at[origin, 0],
            lambda: gb_all.at[origin, opposite],
            lambda: relay_x.at[origin, 1],
        )[flow]()

    def line_copy(flow, origin, up, own=None):
        place = place_of(flow, origin)
        return pltpu.make_async_remote_copy(
            src_ref=place if own is None else own,
            dst_ref=place,
            send_sem=line_send.at[flow, origin if up else jnp.where(origin == row, rows_count, origin)],
            recv_sem=line_recv.at[flow, origin],
            device_id={"dp": row + (1 if up else -1)},
            device_id_type=MESH,
        )

    def plane_copy(flow, origin, step):
        peer = partner(me, step, count)[0]
        return pltpu.make_async_remote_copy(
            src_ref=flows[flow].at[origin, me],
            dst_ref=flows[flow].at[origin, me],
            send_sem=plane_send.at[flow, origin, step],
            recv_sem=plane_recv.at[flow, origin, step],
            device_id=at(section, peer),
            device_id_type=MESH,
        )

    direct_steps = [1, 2] if balanced else steps

    def send_plane(flow, origin):
        for step in direct_steps[::-1]:
            plane_copy(flow, origin, step).start()

    def half_copy(flow, origin, half):
        owner = partner(me, 1 + half, count)[1]
        place = flows[flow].at[origin, owner, pl.ds(half * (tokens // 2), tokens // 2), :]
        return pltpu.make_async_remote_copy(
            src_ref=place,
            dst_ref=place,
            send_sem=plane_send.at[flow, origin, 3 * half],
            recv_sem=plane_recv.at[flow, origin, 3 * half],
            device_id=at(section, partner(me, 2 - half, count)[0]),
            device_id_type=MESH,
        )

    def relay_plane(flow, origin):
        if balanced:
            for step in direct_steps:
                plane_copy(flow, origin, step).wait_recv()
            for half in range(2):
                half_copy(flow, origin, half).start()

    def wait_plane(flow, origin):
        if balanced:
            for half in range(2):
                half_copy(flow, origin, half).wait_recv()
        else:
            for step in steps:
                plane_copy(flow, origin, step).wait_recv()

    def send_plane_of(flow):
        return lambda origin: send_plane(flow, origin)

    def relay_plane_of(flow):
        return lambda origin: relay_plane(flow, origin)

    def engine_copy(origin, step):
        second = balanced and step == 3
        peer = me if second else partner(me, step, count)[0]
        return pltpu.make_async_remote_copy(
            src_ref=relay_x.at[origin, int(second)],
            dst_ref=x_all.at[origin, opposite if second else me],
            send_sem=engine_send.at[origin, step],
            recv_sem=plane_recv.at[0, origin, step],
            device_id=at(1 - section, peer),
            device_id_type=MESH,
        )

    def send_engine(origin):
        for step in direct_steps[::-1] + [0]:
            engine_copy(origin, step).start()

    def send_engine_second(origin):
        if balanced:
            engine_copy(origin, 3).start()

    first_other = jnp.where(row == rows_count - 1, row - 1, row + 1)

    def send_engine_first(origin):
        pl.when(origin == first_other)(lambda: send_engine(origin))

    def send_engine_first_second(origin):
        pl.when(origin == first_other)(lambda: send_engine_second(origin))

    def send_engine_later(origin):
        @pl.when(origin != first_other)
        def _():
            send_engine(origin)
            send_engine_second(origin)

    def start_flow(flow, own):
        if flow in (0, 1, 4):
            own = own.at[:, tile_of(me, part)]
        if flow in (5, 6):
            own = own.at[:, tile_of(opposite, part)]

        @pl.when(row + 1 < rows_count)
        def _():
            line_copy(flow, row, True, own).start()

        @pl.when(row >= 1)
        def _():
            line_copy(flow, row, False, own).start()

    near = 2 * (rows_count - 1) // 3

    def hop(flow, third, after=lambda origin: None, limit=None):
        limit = rows_count if limit is None else limit

        def one(hops):
            @pl.when(row >= hops)
            def _():
                origin = row - hops
                line_copy(flow, origin, True).wait_recv()

                @pl.when((row + 1 < rows_count) & (hops < limit))
                def _():
                    line_copy(flow, origin, True).start()

                after(origin)

            @pl.when(row + hops < rows_count)
            def _():
                origin = row + hops
                line_copy(flow, origin, False).wait_recv()

                @pl.when((row >= 1) & (hops < limit))
                def _():
                    line_copy(flow, origin, False).start()

                after(origin)

        low, high = (1 + (rows_count - 1) * k // 3 for k in (third - 1, third))
        loop(high - low, lambda i: one(low + i))

    def thirds(third, body):
        def one(i):
            hops = 1 + i // 2
            origin = row + hops * (1 - 2 * lax.rem(i, 2))

            @pl.when((origin >= 0) & (origin < rows_count))
            def _():
                body(origin)

        low, high = (2 * ((rows_count - 1) * k // 3) for k in (third, third + 1))
        loop(high - low, lambda i: one(low + i))

    def nth_other(i):
        above, below = rows_count - 1 - row, row
        both = 2 * jnp.minimum(above, below)
        near_side = jnp.where(lax.rem(i, 2) == 0, 1 + i // 2, -(1 + i // 2))
        far_side = (1 + i - both // 2) * jnp.where(above > below, 1, -1)
        return row + jnp.where(i < both, near_side, far_side)

    def others(body, after=()):
        def one(i):
            body(nth_other(i), i)
            for number, action in after:
                pl.when(i == number - 1)(action)

        loop(rows_count - 1, one)

    def finish_flow(flow, limit=None, halves=True):
        limit = rows_count if limit is None else limit

        def one(origin):
            @pl.when((origin <= row) & (row + 1 < rows_count) & (row - origin < limit))
            def _():
                line_copy(flow, origin, True).wait_send()

            @pl.when((origin >= row) & (row >= 1) & (origin - row < limit))
            def _():
                line_copy(flow, origin, False).wait_send()

            @pl.when(origin != row)
            def _():
                if flow < 2:
                    for step in direct_steps:
                        plane_copy(flow, origin, step).wait_send()
                    if balanced and halves:
                        for half in range(2):
                            half_copy(flow, origin, half).wait_send()
                if flow == 4:
                    for step in [0] + steps:
                        engine_copy(origin, step).wait_send()

        loop(rows_count, one)

    def own_stores(flow, own):
        return [
            pltpu.make_async_copy(
                own.at[:, pl.ds(i * part, part)], flows[flow].at[row, i], store.at[flow * count + i]
            )
            for i in range(count)
        ]

    def scatter(kind, step):
        peer = partner(me, step, count)[0]
        return pltpu.make_async_remote_copy(
            src_ref=term.at[peer],
            dst_ref=arrived.at[kind, step - 1],
            send_sem=send.at[kind, step - 1],
            recv_sem=recv.at[kind, step - 1],
            device_id=at(section, peer),
            device_id_type=MESH,
        )

    def gather(number, step, target):
        peer = partner(me, step, count)[0]
        return pltpu.make_async_remote_copy(
            src_ref=parts.at[number, 0],
            dst_ref=parts.at[number, step],
            send_sem=part_send.at[number, step],
            recv_sem=part_recv.at[number, step],
            device_id=at(target, peer),
            device_id_type=MESH,
        )

    def back(number, step):
        return pltpu.make_async_remote_copy(
            src_ref=parts.at[number, step],
            dst_ref=parts.at[number, step],
            send_sem=back_send.at[number, step],
            recv_sem=back_recv.at[number, step],
            device_id=at(1 - section, me),
            device_id_type=MESH,
        )

    def place(number, step, target):
        owner = partner(me, step, count)[1]
        target[:, tile_of(owner, part)] = parts[number, step]

    def reduce(kind, number, with_input):
        for step in steps:
            scatter(kind, step).wait_recv()

        def rows_of(i):
            rows = tile_of(i, row_tile)
            total = term[me, rows, :].astype(F32)
            if with_input:
                total = total + xv[rows, tile_of(me, part)].astype(F32)
            for step in steps:
                total = total + arrived[kind, step - 1, rows, :].astype(F32)
            parts[number, 0, rows, :] = total.astype(BF16)

        loop(row_tiles, rows_of)

    def finish_sends(kind):
        for step in steps:
            scatter(kind, step).wait_send()

    def to_other_section(number):
        for step in steps[::-1] + [0]:
            gather(number, step, 1 - section).start()

    def from_own_section(number, target):
        place(number, 0, target)
        for step in steps:
            back(number, step).wait_recv()
            place(number, step, target)
        for step in [0] + steps:
            gather(number, step, 1 - section).wait_send()

    def from_other_section(number, target):
        gather(number, 0, 1 - section).wait_recv()
        place(number, 0, target)
        for step in steps:
            gather(number, step, 1 - section).wait_recv()
            back(number, step).start()
            place(number, step, target)

    def finish_back(number):
        for step in steps:
            back(number, step).wait_send()

    def start_within(number):
        for step in steps[::-1]:
            gather(number, step, section).start()

    def finish_within(number, target):
        place(number, 0, target)
        for step in steps:
            gather(number, step, section).wait_recv()
            place(number, step, target)
        for step in steps:
            gather(number, step, section).wait_send()

    def each_chunk(kind, compute, sends=True):
        def chunk(i):
            step = count - 1 - i
            owner = partner(me, step, count)[0]
            loop(part // TILE, lambda j: compute(owner, j))

            @pl.when((step > 0) & sends)
            def _():
                scatter(kind, step).start()

        loop(count, chunk)

    lane = lanes_of((1, LANES)).astype(F32)
    exponent = jnp.where(lane < ROT // 2, lane, lane - ROT // 2)
    frequency = jnp.exp(exponent * (-2.0 * math.log(10000.0) / ROT))
    row_index = lax.broadcasted_iota(jnp.int32, (length, length), 0)
    column_index = lax.broadcasted_iota(jnp.int32, (length, length), 1)

    def segments_of(values):
        across = values.astype(F32)
        down = jnp.sum(jnp.where(row_index == column_index, across, 0.0), axis=1, keepdims=True)
        return across, down

    def fill_tables(slot, values_of):
        for b in range(batch):
            rows = pl.ds(b * length, length)
            across, down = segments_of(values_of(b))
            number_of = jnp.sum((across < down).astype(F32), axis=1, keepdims=True)
            index = lax.broadcasted_iota(jnp.int32, (length, 1), 0).astype(F32)
            angles = (index - number_of) * frequency
            inside = lanes_of((length, LANES)) < ROT
            tables[slot, rows, :LANES] = jnp.where(inside, jnp.cos(angles), 1.0)
            tables[slot, rows, LANES:] = jnp.where(inside, jnp.sin(angles), 0.0)

    fill_tables(0, lambda b: seg_row[b : b + 1, :])

    def softmax(projected, values, b, h):
        rows, columns = tile_of(b, length), tile_of(h, HEAD)
        across, down = segments_of(values)
        allowed = (across == down) & (column_index <= row_index)
        scores = dot_nt(projected[0, rows, columns], projected[1, rows, columns]) * scale
        scores = jnp.where(allowed, scores, -jnp.inf)
        row_max = jnp.max(scores, axis=-1, keepdims=True)
        total = jnp.sum(jnp.exp(scores - row_max), axis=-1, keepdims=True)
        return jnp.exp(scores - (row_max + jnp.log(total)))

    def attend(prob, projected, target, b, h):
        rows, columns = tile_of(b, length), tile_of(h, HEAD)
        target[rows, columns] = dot(prob.astype(BF16), projected[2, rows, columns]).astype(BF16)

    def attend_backward(prob, projected, slot, target, b, h):
        rows, columns = tile_of(b, length), tile_of(h, HEAD)
        cosine, sine = tables[slot, rows, :LANES], tables[slot, rows, LANES:]
        queries, keys, values = (projected[k, rows, columns] for k in range(3))
        d_context = dctx[rows, columns]
        d_values = dot_tn(prob.astype(BF16), d_context)
        d_probs = dot_nt(d_context, values)
        delta = jnp.sum(prob * d_probs, axis=-1, keepdims=True)
        d_scores = (prob * (d_probs - delta) * scale).astype(BF16)
        for k, gradient in ((0, dot(d_scores, keys)), (1, dot_tn(d_scores, queries))):
            first = unrotated(gradient[:, :LANES], cosine, sine)
            start = pl.multiple_of(h * HEAD, HEAD)
            target[k, rows, pl.ds(start, LANES)] = first.astype(BF16)
            start = pl.multiple_of(h * HEAD + LANES, LANES)
            target[k, rows, pl.ds(start, HEAD - LANES)] = gradient[:, LANES:].astype(BF16)
        target[2, rows, columns] = d_values.astype(BF16)

    def each_pair(body):
        def row_of(b):
            for h in range(heads):
                body(b, h)

        loop(batch, row_of)

    def project(projected, slot):
        def rotary_head(i):
            which, h = i // heads, lax.rem(i, heads)
            tile = dot(attn_in[...], w3[which, :, tile_of(h, HEAD)])
            first = rotated(tile[:, :LANES], tables[slot, :, :LANES], tables[slot, :, LANES:])
            start = pl.multiple_of(h * HEAD, HEAD)
            projected[which, :, pl.ds(start, LANES)] = first.astype(BF16)
            start = pl.multiple_of(h * HEAD + LANES, LANES)
            projected[which, :, pl.ds(start, HEAD - LANES)] = tile[:, LANES:].astype(BF16)

        def value_head(h):
            columns = tile_of(h, HEAD)
            projected[2, :, columns] = dot(attn_in[...], w3[2, :, columns]).astype(BF16)

        loop(2 * heads, rotary_head)
        loop(heads, value_head)

    def segment_copy(step):
        return pltpu.make_async_remote_copy(
            src_ref=seg_row,
            dst_ref=segments.at[row],
            send_sem=segment_send.at[step],
            recv_sem=segment_recv.at[step],
            device_id={"dp": lax.rem(row + step, rows_count)},
            device_id_type=MESH,
        )

    def d_context_head(h):
        dctx[:, tile_of(h, HEAD)] = dot_nt(gbv[...], wo[tile_of(h, HEAD), :]).astype(BF16)

    def meet():
        pl.semaphore_wait(barrier, 2 * count - 1 + rows_count - 1)
        for step in range(1, rows_count):
            segment_copy(step).start()


    @pl.when(section == 0)
    def _():
        x_load.wait()

    @pl.when(section == 1)
    def _():
        meet()
        start_flow(4, x_hbm)
        go_load.wait()
        out_load.wait()
        loop(heads, d_context_head)
        if balanced:
            start_flow(6, x_hbm)
        hop(4, 1, send_engine_first)
        if balanced:
            hop(6, 1, send_engine_first_second)
        fc2_load.wait()

        def d_act_tile(i):
            columns = tile_of(i, TILE)
            slope[:, columns] = dot_nt(gbv[...], w2[columns, :])

        loop(hidden_width // TILE, d_act_tile)
        for third in (2, 3):
            if balanced:
                hop(6, third)
            hop(4, third)
            if third == 2:
                start_flow(1, gbv)
                if balanced:
                    start_flow(5, gbv)
        hop(1, 1)
        if balanced:
            hop(5, 1)
        from_other_section(0, xv)
        start_flow(0, xv)
        for third in range(3):
            thirds(third, send_engine_later)

    for copy in own_stores(0, xv):
        copy.start()

    def norm_rows(i):
        rows = tile_of(i, row_tile)
        normed, mean, inv_std = row_norm(xv[rows, :].astype(F32))
        means[rows, :] = mean
        inv_stds[rows, :] = inv_std
        attn_in[rows, :] = (normed * gains[0:1, :] + biases[0:1, :]).astype(BF16)
        mlp_in[rows, :] = (normed * gains[1:2, :] + biases[1:2, :]).astype(BF16)

    loop(row_tiles, norm_rows)

    for copy in qkv_loads:
        copy.wait()
    project(qkv, 0)

    def own_attention(b, h):
        prob = softmax(qkv, seg_row[pl.ds(b, 1), :], b, h)
        probs[b * heads + h] = prob
        attend(prob, qkv, context, b, h)

    each_pair(own_attention)

    @pl.when(section == 1)
    def _():
        hop(0, 1, send_plane_of(0))
        hop(1, 2)
        if balanced:
            hop(5, 2)


    def fc1_block(i):
        fc1_load(i).wait()

        def fc1_tile(j):
            columns = tile_of(i * (block // TILE) + j, TILE)
            value, derivative = gelu_parts(dot(mlp_in[...], w1[:, columns]))
            act[:, columns] = value.astype(BF16)

            @pl.when(section == 0)
            def _():
                slope[:, columns] = derivative

            @pl.when(section == 1)
            def _():
                dh[:, columns] = (slope[:, columns] * derivative).astype(BF16)

        loop(block // TILE, fc1_tile)

    loop(blocks, fc1_block)

    @pl.when(section == 1)
    def _():
        hop(0, 2, send_plane_of(0))

    @pl.when(section == 0)
    def _():
        out_load.wait()
        fc2_load.wait()
        go_load.wait()

    tiles = hidden_width // TILE

    def act_store(origin, i):
        columns = tile_of(i, TILE)
        return pltpu.make_async_copy(
            act_rest.at[:, columns], act_all.at[origin, :, columns], rest_store.at[0]
        )

    def dh_store(origin, i):
        columns = tile_of(i, TILE)
        return pltpu.make_async_copy(
            act_rest.at[:, columns], dh_all.at[origin, :, columns], rest_store.at[0]
        )

    def slope_store(origin, i):
        columns = tile_of(i, TILE)
        return pltpu.make_async_copy(
            slope_rest.at[:, columns], slope_all.at[origin, :, columns], rest_store.at[1]
        )

    def load_block(flow, origin):
        if flow == 0:

            @pl.when(section == 0)
            def _():
                for step in [0] + steps:
                    engine_copy(origin, step).wait_recv()

            pl.when(section == 1)(lambda: wait_plane(flow, origin))
        else:
            pl.when(section == 0)(lambda: wait_plane(flow, origin))

            @pl.when(section == 1)
            def _():
                for step in direct_steps:
                    plane_copy(flow, origin, step).wait_recv()

        copies = [
            pltpu.make_async_copy(
                flows[flow].at[origin, i], attn_in.at[:, pl.ds(i * part, part)], rest_load.at[i]
            )
            for i in range(count)
        ]
        for copy in copies:
            copy.start()
        return copies

    def attention_stores(origin):
        return [
            pltpu.make_async_copy(qkv_rest, qkv_all.at[origin], rest_load.at[count + 1]),
            pltpu.make_async_copy(context_rest, context_all.at[origin], rest_load.at[count + 2]),
        ]

    def far_of(origin):
        return (section == 0) & ((origin - row > near) | (row - origin > near))

    def rest_forward(origin, index):
        for copy in load_block(0, origin):
            copy.wait()

        def norm_rows(i):
            rows = tile_of(i, row_tile)
            normed, mean, inv_std = row_norm(attn_in[rows, :].astype(F32))
            first = lanes_of((row_tile, LANES)) == 0
            stats_all[origin, rows, :] = jnp.where(first, mean, inv_std)
            mlp_in[rows, :] = (normed * gains[1:2, :] + biases[1:2, :]).astype(BF16)
            attn_in[rows, :] = (normed * gains[0:1, :] + biases[0:1, :]).astype(BF16)

        loop(row_tiles, norm_rows)

        @pl.when(section == 0)
        def _():
            fill_tables(1, lambda b: segments[origin, b : b + 1, :])
            project(qkv_rest, 1)

            def attention(b, h):
                prob = softmax(qkv_rest, segments[origin, pl.ds(b, 1), :], b, h)
                attend(prob, qkv_rest, context_rest, b, h)

            each_pair(attention)
            for copy in attention_stores(origin):
                copy.start()

        def tile(i):
            columns = tile_of(i, TILE)
            value, derivative = gelu_parts(dot(mlp_in[...], w1[:, columns]))
            act_rest[:, columns] = value.astype(BF16)
            slope_rest[:, columns] = derivative
            act_store(origin, i).start()
            slope_store(origin, i).start()

        loop(tiles, tile)

        pltpu.make_async_copy(act_rest, act_all.at[origin], rest_store.at[0]).wait()
        pltpu.make_async_copy(slope_rest, slope_all.at[origin], rest_store.at[1]).wait()

        @pl.when(section == 0)
        def _():
            for copy in attention_stores(origin):
                copy.wait()

    def slope_load(origin):
        return pltpu.make_async_copy(slope_all.at[origin], slope_rest, rest_load.at[count])

    def rest_backward(origin, index):
        copies = load_block(1, origin)
        for copy in copies + [slope_load(origin)]:
            copy.wait()

        def tile(i):
            columns = tile_of(i, TILE)
            d_act = dot_nt(attn_in[...], w2[columns, :])
            act_rest[:, columns] = (d_act * slope_rest[:, columns]).astype(BF16)
            dh_store(origin, i).start()

        qkv_load = pltpu.make_async_copy(qkv_all.at[origin], qkv_rest, rest_load.at[count + 1])
        dproj_store = pltpu.make_async_copy(
            dproj_rest, dproj_all.at[origin], rest_load.at[count + 2]
        )
        far = far_of(origin)
        pl.when(far)(qkv_load.start)
        loop(tiles, tile)

        @pl.when(index < rows_count - 2)
        def _():
            slope_load(nth_other(index + 1)).start()

        @pl.when(far)
        def _():
            qkv_load.wait()
            fill_tables(1, lambda b: segments[origin, b : b + 1, :])

            def head(h):
                columns = tile_of(h, HEAD)
                dctx[:, columns] = dot_nt(attn_in[...], wo[columns, :]).astype(BF16)

            loop(heads, head)

            def attention(b, h):
                prob = softmax(qkv_rest, segments[origin, pl.ds(b, 1), :], b, h)
                attend_backward(prob, qkv_rest, 1, dproj_rest, b, h)

            each_pair(attention)
            dproj_store.start()
            dproj_store.wait()

        pltpu.make_async_copy(act_rest, dh_all.at[origin], rest_store.at[0]).wait()

    def out_tile(owner, j):
        columns = tile_of(owner * (part // TILE) + j, TILE)
        total = dot(context[...], wo[:, columns]) + dot(act[...], w2[:, columns])
        term[owner, :, tile_of(j, TILE)] = total.astype(BF16)

    def own_stats(i):
        rows = tile_of(i, row_tile)
        first = lanes_of((row_tile, LANES)) == 0
        stats_all[row, rows, :] = jnp.where(first, means[rows, :], inv_stds[rows, :])

    layer_store = pltpu.make_async_copy(other, layer_out, store.at[2 * count + 4])

    def grad_store(i):
        rows = tile_of(i, row_tile)
        return pltpu.make_async_copy(slope.at[rows, :], input_grad.at[rows, :], grad_sems.at[0])

    transposed_stores = [
        pltpu.make_async_copy(attn_t, attn_out, store.at[2 * count + 6]),
        pltpu.make_async_copy(mlp_t, mlp_out, store.at[2 * count + 7]),
    ]
    width_mine = width // rows_count

    def transposed_inputs():
        for copy in own_stores(0, xv):
            copy.wait()
        start = row * width_mine
        chunk, offset = start // part, pl.multiple_of(lax.rem(start, part), LANES)
        loads = [
            pltpu.make_async_copy(
                x_all.at[i, chunk, :, pl.ds(offset, width_mine)], x_mine.at[i], slice_load.at[i]
            )
            for i in range(rows_count)
        ]
        for copy in loads:
            copy.start()
        for copy in loads:
            copy.wait()
        all_tokens = rows_count * tokens

        def columns_of(i):
            columns = tile_of(i, LANES)
            mean = stats_all[:, :, 0:1].reshape(all_tokens, 1)
            inv_std = stats_all[:, :, 1:2].reshape(all_tokens, 1)
            values = x_mine[:, :, columns].reshape(all_tokens, LANES).astype(F32)
            normed = (values - mean) * inv_std
            whole = tile_of(start // LANES + i, LANES)
            for j, target in enumerate((attn_t, mlp_t)):
                scaled = normed * gains[j : j + 1, whole] + biases[j : j + 1, whole]
                target[columns, :] = scaled.astype(BF16).T

        loop(width_mine // LANES, columns_of)
        for copy in transposed_stores:
            copy.start()


    @pl.when(section == 0)
    def _():
        meet()
        each_chunk(0, out_tile)
        reduce(0, 0, True)
        to_other_section(0)
        finish_sends(0)
        for step in range(1, rows_count):
            segment_copy(step).wait_recv()
        others(rest_forward)
        from_own_section(0, other)
        layer_store.start()
        from_other_section(1, full)

        def gradient_rows(i):
            rows = tile_of(i, row_tile)
            normed, _, inv_std = row_norm(other[rows, :].astype(F32))
            dx = row_norm_backward(full[rows, :].astype(F32), normed, inv_std)
            gbv[rows, :] = (gbv[rows, :].astype(F32) + dx).astype(BF16)

        loop(row_tiles, gradient_rows)
        start_flow(1, gbv)
        finish_back(1)

        def d_hidden_tile(i):
            columns = tile_of(i, TILE)
            d_act = dot_nt(gbv[...], w2[columns, :])
            dh[:, columns] = (d_act * slope[:, columns]).astype(BF16)

        loop(hidden_width // TILE, d_hidden_tile)
        loop(heads, d_context_head)


    each_pair(lambda b, h: attend_backward(probs[b * heads + h], qkv, 0, dproj, b, h))

    @pl.when(section == 0)
    def _():
        hop(1, 1, send_plane_of(1))

    @pl.when(section == 1)
    def _():
        start_flow(3, dproj)

    def gradient_tile(owner, j):
        columns = tile_of(owner * (part // TILE) + j, TILE)
        d_attn = dot_nt(dproj[0], w3[0, columns, :])
        d_attn = d_attn + dot_nt(dproj[1], w3[1, columns, :])
        d_attn = d_attn + dot_nt(dproj[2], w3[2, columns, :])
        d_mlp = dot_nt(dh[...], w1[columns, :])
        normed = (xv[:, columns].astype(F32) - means[...]) * inv_stds[...]
        total = d_attn * gains[0:1, columns] + d_mlp * gains[1:2, columns]
        term[owner, :, tile_of(j, TILE)] = total.astype(BF16)
        vectors[0:1, columns] = jnp.sum(d_attn * normed, axis=0, keepdims=True)
        vectors[1:2, columns] = jnp.sum(d_mlp * normed, axis=0, keepdims=True)
        vectors[2:3, columns] = jnp.sum(d_attn, axis=0, keepdims=True)
        vectors[3:4, columns] = jnp.sum(d_mlp, axis=0, keepdims=True)

    each_chunk(1, gradient_tile, section == 1)

    outs = [
        (act, act_all.at[row]),
        (context, context_all.at[row]),
        (dh, dh_all.at[row]),
        (dproj, dproj_all.at[row]),
    ]
    stores = own_stores(1, gbv)
    stores += [
        pltpu.make_async_copy(a, b, store.at[2 * count + i]) for i, (a, b) in enumerate(outs)
    ]
    for copy in stores:
        copy.start()

    def sum_copy(step):
        peer = partner(me, step, count)[0]
        return pltpu.make_async_remote_copy(
            src_ref=vectors,
            dst_ref=plane_vectors.at[step],
            send_sem=sum_send.at[step],
            recv_sem=sum_recv.at[step],
            device_id=at(section, peer),
            device_id_type=MESH,
        )

    mine = width // rows_count

    def slice_copy(step):
        target = lax.rem(row + step, rows_count)
        return pltpu.make_async_remote_copy(
            src_ref=plane_vectors.at[0, :, tile_of(target, mine)],
            dst_ref=slices.at[step],
            send_sem=slice_send.at[step],
            recv_sem=slice_recv.at[step],
            device_id={"dp": target},
            device_id_type=MESH,
        )

    for step in steps:
        sum_copy(step).start()

    def sum_plane():
        total = vectors[...]
        for step in steps:
            sum_copy(step).wait_recv()
            total = total + plane_vectors[step]
        plane_vectors[0] = total
        for step in range(1, rows_count):
            slice_copy(step).start()

    sum_stores = [
        pltpu.make_async_copy(sums.at[0], gain_grads, sum_store.at[0]),
        pltpu.make_async_copy(sums.at[1], bias_grads, sum_store.at[1]),
    ]

    def sum_line():
        total = plane_vectors[0, :, tile_of(row, mine)]
        for step in range(1, rows_count):
            slice_copy(step).wait_recv()
            total = total + slices[step]
        sums[0] = total[:2]
        sums[1] = total[2:]
        for copy in sum_stores:
            copy.start()
        for step in range(1, rows_count):
            slice_copy(step).wait_send()
        for step in steps:
            sum_copy(step).wait_send()


    def input_gradient():
        def rows_of(i):
            rows = tile_of(i, row_tile)
            inv_std = inv_stds[rows, :]
            normed = (xv[rows, :].astype(F32) - means[rows, :]) * inv_std
            dx = row_norm_backward(full[rows, :].astype(F32), normed, inv_std)
            slope[rows, :] = gbv[rows, :].astype(F32) + dx
            grad_store(i).start()

        loop(row_tiles, rows_of)

    @pl.when(section == 0)
    def _():
        slope_load(nth_other(0)).start()
        thirds(0, relay_plane_of(1))
        hop(1, 2, send_plane_of(1))
        loop(row_tiles, own_stats)
        transposed_inputs()
        hop(1, 3, send_plane_of(1))
        start_flow(3, dproj)
        at_end = (row == 0) | (row == rows_count - 1)
        pl.when(at_end)(lambda: thirds(1, relay_plane_of(1)))

        def after_first():
            pl.when(jnp.logical_not(at_end))(lambda: thirds(1, relay_plane_of(1)))
            thirds(2, relay_plane_of(1))
            for step in steps[::-1]:
                scatter(1, step).start()
            sum_plane()

        def after_second():
            reduce(1, 2, False)
            start_within(2)
            hop(3, 1, limit=near)
            sum_line()

        others(rest_backward, [(1, after_first), (2, after_second)])
        finish_within(2, full)
        finish_sends(1)
        input_gradient()
        hop(3, 2, limit=near)

    @pl.when(section == 1)
    def _():
        finish_back(0)
        hop(1, 3)
        if balanced:
            hop(5, 3)
        reduce(1, 1, False)
        to_other_section(1)
        thirds(0, relay_plane_of(0))
        hop(0, 3, send_plane_of(0))
        thirds(1, relay_plane_of(0))
        finish_sends(1)
        each_chunk(0, out_tile, False)
        hop(3, 1)
        start_flow(2, context)
        loop(row_tiles, own_stats)
        from_own_section(1, full)
        for step in steps[::-1]:
            scatter(0, step).start()
        sum_plane()

        def share_gradients():
            for third in range(3):
                thirds(third, send_plane_of(1))
            hop(3, 2)
            hop(2, 1)

        others(
            rest_forward, [(1, lambda: thirds(2, relay_plane_of(0))), (2, share_gradients)]
        )
        slope_load(nth_other(0)).start()
        input_gradient()

        def after_second():
            transposed_inputs()
            reduce(0, 2, True)
            start_within(2)
            sum_line()
            hop(2, 2)

        others(rest_backward, [(2, after_second)])
        finish_within(2, other)
        layer_store.start()
        hop(3, 3)
        hop(2, 3)
        finish_sends(0)

    for copy in stores + [layer_store] + transposed_stores + sum_stores:
        copy.wait()
    pltpu.make_async_copy(slope, input_grad, grad_sems.at[0]).wait()
    @pl.when(section == 0)
    def _():
        finish_flow(1)
        finish_flow(3, near)

    @pl.when(section == 1)
    def _():
        for step in range(1, rows_count):
            segment_copy(step).wait_recv()
        finish_flow(1, halves=False)
        for flow in (0, 2, 3, 4) + ((5, 6) if balanced else ()):
            finish_flow(flow)

    for step in range(1, rows_count):
        segment_copy(step).wait_send()


def chain(attn_input, grad_output, segment_ids, weights):
    w_qkv, w_out, w_fc1, w_fc2, gains, biases = weights
    batch, length, width = attn_input.shape
    tokens = batch * length
    count = lax.axis_size("tensor")
    inner, hidden = w_qkv.shape[2], w_fc1.shape[1]
    part = width // count
    heads = inner // HEAD
    anywhere, vmem = pl.BlockSpec(memory_space=pl.ANY), pl.BlockSpec(memory_space=pltpu.VMEM)
    like = jax.ShapeDtypeStruct
    rows_count = lax.axis_size("dp")
    wide, narrow = (tokens, width), (tokens, inner)
    dma = pltpu.SemaphoreType.DMA
    return pl.pallas_call(
        functools.partial(chain_kernel, count, batch),
        out_shape=[
            like(wide, BF16),
            like(wide, F32),
            like((2, width // rows_count), F32),
            like((2, width // rows_count), F32),
            like((rows_count, count, tokens, part), BF16),
            like((rows_count, count, tokens, part), BF16),
            like((rows_count, tokens, inner), BF16),
            like((rows_count, 3, tokens, inner), BF16),
            like((rows_count, tokens, hidden), BF16),
            like((rows_count, tokens, hidden), BF16),
            like((width // rows_count, rows_count * tokens), BF16),
            like((width // rows_count, rows_count * tokens), BF16),
            like((rows_count, tokens, hidden), F32),
            like((rows_count, 2, tokens, part), BF16),
            like((rows_count, 3, tokens, inner), BF16),
        ],
        in_specs=[anywhere, anywhere, vmem] + [anywhere] * 4 + [vmem, vmem],
        out_specs=[anywhere] * 10 + [anywhere] * 5,
        scratch_shapes=[
            pltpu.VMEM((3, width, inner), BF16),
            pltpu.VMEM((inner, width), BF16),
            pltpu.VMEM((width, hidden), BF16),
            pltpu.VMEM((hidden, width), BF16),
            pltpu.VMEM(wide, BF16),
            pltpu.VMEM(wide, BF16),
            pltpu.VMEM(wide, BF16),
            pltpu.VMEM(wide, BF16),
            pltpu.VMEM(wide, BF16),
            pltpu.VMEM((3, tokens, inner), BF16),
            pltpu.VMEM(narrow, BF16),
            pltpu.VMEM((batch * heads, length, length), F32),
            pltpu.VMEM((tokens, hidden), BF16),
            pltpu.VMEM((tokens, hidden), F32),
            pltpu.VMEM((tokens, hidden), BF16),
            pltpu.VMEM(narrow, BF16),
            pltpu.VMEM((3, tokens, inner), BF16),
            pltpu.VMEM((tokens, 1), F32),
            pltpu.VMEM((tokens, 1), F32),
            pltpu.VMEM((2, tokens, 2 * LANES), F32),
            pltpu.VMEM((count, tokens, part), BF16),
            pltpu.VMEM((2, count - 1, tokens, part), BF16),
            pltpu.VMEM((3, count, tokens, part), BF16),
            pltpu.VMEM(wide, BF16),
            pltpu.VMEM((tokens, hidden), BF16),
            pltpu.VMEM((tokens, hidden), F32),
            pltpu.VMEM((rows_count, tokens, LANES), F32),
            pltpu.VMEM((rows_count, tokens, width // rows_count), BF16),
            pltpu.VMEM((width // rows_count, rows_count * tokens), BF16),
            pltpu.VMEM((width // rows_count, rows_count * tokens), BF16),
            pltpu.VMEM((4, width), F32),
            pltpu.VMEM((count, 4, width), F32),
            pltpu.VMEM((rows_count, 4, width // rows_count), F32),
            pltpu.VMEM((rows_count, batch, length), jnp.int32),
            pltpu.VMEM((3, tokens, inner), BF16),
            pltpu.VMEM((3, tokens, inner), BF16),
            pltpu.VMEM(narrow, BF16),
            dma((11,)),
            dma((2 * count + 8,)),
            dma((2, count - 1)),
            dma((2, count - 1)),
            dma((3, count)),
            dma((3, count)),
            dma((2, count)),
            dma((2, count)),
            dma((7, rows_count + 1)),
            dma((7, rows_count)),
            dma((2, rows_count, count)),
            dma((2, rows_count, count)),
            dma((count + 3,)),
            dma((2,)),
            dma((count,)),
            dma((count,)),
            dma((rows_count,)),
            dma((rows_count,)),
            dma((rows_count, count)),
            dma((rows_count,)),
            dma((rows_count,)),
            dma((rows_count,)),
            dma((1,)),
            pltpu.VMEM((2, 2, width // rows_count), F32),
            dma((2,)),
        ],
        compiler_params=pltpu.CompilerParams(
            collective_id=0, has_side_effects=True, vmem_limit_bytes=67_043_328
        ),
        name="chain",
    )(
        attn_input.reshape(wide),
        grad_output.reshape(wide),
        segment_ids,
        jnp.transpose(w_qkv, (1, 0, 2)),
        w_out,
        w_fc1,
        w_fc2,
        gains,
        biases,
    )


def weight_kernel(*refs):
    (
        gb_all, attn_in, mlp_in, context_all, dproj_all, act_all, dh_all,
        layer_in, grad_in, gain_in, bias_in,
        g_qkv, g_out, g_fc1, g_fc2, layer_out, input_grad, gain_out, bias_out,
        gb_mine, context, dproj, act, attn_t, mlp_t, r_qkv, r_out, r_fc1, r_fc2,
        layer, grad, load, act_load, dh_load, store, through, gb_load,
    ) = refs
    blocks, tokens, mine = gb_mine.shape
    rows = blocks * tokens
    part = gb_all.shape[3]
    inner, hidden = context.shape[2], act.shape[2]
    start = lax.axis_index("dp") * mine
    chunk, offset = start // part, pl.multiple_of(lax.rem(start, part), LANES)
    piece = hidden // 4

    def slice_loads(source, target, sems):
        return [
            pltpu.make_async_copy(
                source.at[i, chunk, :, pl.ds(offset, mine)], target.at[i], sems.at[i]
            )
            for i in range(blocks)
        ]

    def piece_load(source, target, sems, i):
        columns = pl.ds(i * piece, piece)
        return pltpu.make_async_copy(source.at[:, :, columns], target.at[:, :, columns], sems.at[i])

    gb_loads = slice_loads(gb_all, gb_mine, gb_load)
    in_loads = [
        pltpu.make_async_copy(attn_in, attn_t, load.at[0]),
        pltpu.make_async_copy(mlp_in, mlp_t, load.at[1]),
    ]
    context_load = pltpu.make_async_copy(context_all, context, load.at[2])
    dproj_load = pltpu.make_async_copy(dproj_all, dproj, load.at[3])
    act_loads = [piece_load(act_all, act, act_load, i) for i in range(4)]
    dh_loads = [piece_load(dh_all, act, dh_load, i) for i in range(4)]
    gain_out[...] = gain_in[...]
    bias_out[...] = bias_in[...]
    ins = [
        pltpu.make_async_copy(layer_in, layer, through.at[0]),
        pltpu.make_async_copy(grad_in, grad, through.at[1]),
    ]
    outs = [
        pltpu.make_async_copy(layer, layer_out, through.at[2]),
        pltpu.make_async_copy(grad, input_grad, through.at[3]),
    ]
    for copy in gb_loads + [context_load]:
        copy.start()

    def out_copy(source, target, index):
        return pltpu.make_async_copy(source, target, store.at[index])

    for copy in gb_loads + [context_load]:
        copy.wait()
    for copy in act_loads + in_loads[1:]:
        copy.start()
    gb_rows = gb_mine[...].reshape(rows, mine)

    def out_tile(i):
        tile = tile_of(i, TILE)
        r_out[tile, :] = dot_tn(context[:, :, tile].reshape(rows, TILE), gb_rows)

    loop(inner // TILE, out_tile)
    copies = [out_copy(r_out, g_out, 0)]
    copies[0].start()

    def fc2_copy(i):
        tile = tile_of(i, TILE)
        return out_copy(r_fc2.at[tile, :], g_fc2.at[tile, :], 1 + i)

    def fc2_tile(i):
        tile = tile_of(i, TILE)
        r_fc2[tile, :] = dot_tn(act[:, :, tile].reshape(rows, TILE), gb_mine[...].reshape(rows, mine))
        fc2_copy(i).start()

    per = piece // TILE
    for i in range(4):
        act_loads[i].wait()
        loop(per, lambda j: fc2_tile(i * per + j))
        dh_loads[i].start()
    for copy in [dproj_load] + in_loads[:1] + ins:
        copy.start()

    def fc1_copy(i):
        tile = tile_of(i, TILE)
        return out_copy(r_fc1.at[:, tile], g_fc1.at[:, tile], 1 + hidden // TILE + i)

    def fc1_tile(i):
        tile = tile_of(i, TILE)
        r_fc1[:, tile] = dot(mlp_t[...], act[:, :, tile].reshape(rows, TILE))
        fc1_copy(i).start()

    in_loads[1].wait()
    for i in range(4):
        dh_loads[i].wait()
        loop(per, lambda j: fc1_tile(i * per + j))
    dproj_load.wait()
    in_loads[0].wait()
    for copy in ins:
        copy.wait()
    for copy in outs:
        copy.start()
    per = inner // TILE

    def qkv_copy(i):
        which, tile = i // per, tile_of(lax.rem(i, per), TILE)
        return out_copy(r_qkv.at[which, :, tile], g_qkv.at[which, :, tile], 1 + 2 * (hidden // TILE) + i)

    def qkv_tile(i):
        which, tile = i // per, tile_of(lax.rem(i, per), TILE)
        r_qkv[which, :, tile] = dot(attn_t[...], dproj[:, which, :, tile].reshape(rows, TILE))
        qkv_copy(i).start()

    loop(3 * per, qkv_tile)
    for copy in copies + outs:
        copy.wait()
    loop(hidden // TILE, lambda i: fc2_copy(i).wait())
    loop(hidden // TILE, lambda i: fc1_copy(i).wait())
    loop(3 * per, lambda i: qkv_copy(i).wait())


def weight_gradients(
    gb_all, attn_in, mlp_in, context_all, dproj_all, act_all, dh_all, *through
):
    blocks, count, tokens, part = gb_all.shape
    mine = count * part // lax.axis_size("dp")
    inner, hidden = context_all.shape[2], act_all.shape[2]
    anywhere, vmem = pl.BlockSpec(memory_space=pl.ANY), pl.BlockSpec(memory_space=pltpu.VMEM)
    shapes = [(3, mine, inner), (inner, mine), (mine, hidden), (hidden, mine)]
    dma = pltpu.SemaphoreType.DMA
    return pl.pallas_call(
        weight_kernel,
        out_shape=[jax.ShapeDtypeStruct(shape, F32) for shape in shapes]
        + [jax.ShapeDtypeStruct(value.shape, value.dtype) for value in through],
        in_specs=[anywhere] * 7
        + [anywhere, anywhere, vmem, vmem],
        out_specs=[anywhere] * 6 + [vmem, vmem],
        scratch_shapes=[
            pltpu.VMEM((blocks, tokens, mine), BF16),
            pltpu.VMEM((blocks, tokens, inner), BF16),
            pltpu.VMEM((blocks, 3, tokens, inner), BF16),
            pltpu.VMEM((blocks, tokens, hidden), BF16),
            pltpu.VMEM((mine, blocks * tokens), BF16),
            pltpu.VMEM((mine, blocks * tokens), BF16),
        ]
        + [pltpu.VMEM(shape, F32) for shape in shapes]
        + [pltpu.VMEM(value.shape, value.dtype) for value in through[:2]]
        + [
            dma((4,)),
            dma((4,)),
            dma((4,)),
            dma((1 + 2 * (hidden // TILE) + 3 * (inner // TILE),)),
            dma((4,)),
            dma((blocks,)),
        ],
        compiler_params=pltpu.CompilerParams(vmem_limit_bytes=67_043_328),
        name="weights",
    )(gb_all, attn_in, mlp_in, context_all, dproj_all, act_all, dh_all, *through)


def shards(
    block_input, grad_output, segment_ids, w_qkv, w_out, w_fc1, w_fc2, norm_gains, norm_biases
):
    batch, length, width = block_input.shape
    weights = (w_qkv[0], w_out[0], w_fc1[0], w_fc2[0], norm_gains[0], norm_biases[0])
    (
        layer_out, input_grads, gain_grads, bias_grads, _, gb_all, context, d_proj, activated,
        d_hidden, attn_in, mlp_in, *_,
    ) = chain(block_input, grad_output, segment_ids, weights)
    g_qkv, g_out, g_fc1, g_fc2, layer_out, input_grads, gain_grads, bias_grads = weight_gradients(
        gb_all, attn_in, mlp_in, context, d_proj, activated, d_hidden,
        layer_out, input_grads, gain_grads, bias_grads,
    )
    shape = (1, batch, length, width)
    return (
        layer_out.reshape(shape),
        input_grads.reshape(shape),
        jnp.transpose(g_qkv, (1, 0, 2))[None],
        g_out[None],
        g_fc1[None],
        g_fc2[None],
        gain_grads[None],
        bias_grads[None],
    )


def solution(mesh):
    return jax.shard_map(
        shards,
        mesh=mesh,
        in_specs=(
            P("dp", None, None),
            P("dp", None, None),
            P("dp", None),
            P("section", None, None, "tensor"),
            P("section", "tensor", None),
            P("section", None, "tensor"),
            P("section", "tensor", None),
            P("section", None, None),
            P("section", None, None),
        ),
        out_specs=(
            P("section", "dp", None, None),
            P("section", "dp", None, None),
            P("section", "dp", None, "tensor"),
            P("section", "tensor", "dp"),
            P("section", "dp", "tensor"),
            P("section", "tensor", "dp"),
            P("section", None, "dp"),
            P("section", None, "dp"),
        ),
        check_vma=False,
    )
```

```python
import functools
import math

import jax
import jax.numpy as jnp
from jax import lax
from jax.experimental import pallas as pl
from jax.experimental.pallas import tpu as pltpu
from jax.sharding import PartitionSpec as P

HEAD = 256
ROT = 64
LANES = 128
TILE = 256
WIDE_TILE = 512
NORM_EPSILON = 1e-05
MESH = pl.DeviceIdType.MESH
BF16 = jnp.bfloat16
F32 = jnp.float32


def partner(index, step, count):
    if count & (count - 1):
        return lax.rem(index + step, count), lax.rem(index + count - step, count)
    bit = 1
    while bit < count:
        index = index + ((step // bit) % 2) * (bit - 2 * bit * ((index // bit) % 2))
        bit *= 2
    return index, index


def loop(count, body, unroll=1):
    lax.fori_loop(0, count, lambda i, carry: (body(i), carry)[1], 0, unroll=unroll)


def tile_of(i, size):
    return pl.ds(pl.multiple_of(i * size, size), size)


def dot(left, right):
    return jnp.dot(left, right, preferred_element_type=jnp.float32)


def dot_nt(left, right):
    return lax.dot_general(left, right, (((1,), (1,)), ((), ())), preferred_element_type=jnp.float32)


def dot_tn(left, right):
    return lax.dot_general(left, right, (((0,), (0,)), ((), ())), preferred_element_type=jnp.float32)


def gelu_parts(hidden):
    normal_cdf = 0.5 * (1.0 + lax.erf(hidden * (1.0 / math.sqrt(2.0))))
    density = jnp.exp(-0.5 * hidden * hidden) * (1.0 / math.sqrt(2.0 * math.pi))
    return (hidden * normal_cdf, normal_cdf + hidden * density)


def lanes_of(shape):
    return lax.broadcasted_iota(jnp.int32, shape, len(shape) - 1)


def rotated(tile, cosine, sine):
    half = ROT // 2
    left, right = pltpu.roll(tile, LANES - half, 1), pltpu.roll(tile, half, 1)
    lane = lanes_of(tile.shape)
    turned = jnp.where(lane < half, -left, right)
    return tile * cosine + turned * sine


def unrotated(tile, cosine, sine):
    half = ROT // 2
    scaled = tile * sine
    left, right = pltpu.roll(scaled, LANES - half, 1), pltpu.roll(scaled, half, 1)
    lane = lanes_of(tile.shape)
    turned = jnp.where(lane < half, left, jnp.where(lane < ROT, -right, 0.0))
    return tile * cosine + turned


def row_norm(values):
    mean = jnp.mean(values, axis=-1, keepdims=True)
    centred = values - mean
    inv_std = lax.rsqrt(jnp.mean(centred * centred, axis=-1, keepdims=True) + NORM_EPSILON)
    return centred * inv_std, mean, inv_std


def row_norm_backward(summed, normed, inv_std):
    return inv_std * (
        summed
        - jnp.mean(summed, axis=-1, keepdims=True)
        - normed * jnp.mean(summed * normed, axis=-1, keepdims=True)
    )


def chain_kernel(count, batch, *refs):
    (
        x_hbm, go_hbm, seg_row, w3_hbm, wo_hbm, w1_hbm, w2_hbm, gains, biases,
        layer_out, input_grad, gain_grads, bias_grads, x_all, gb_all, context_all, dproj_all, act_all, dh_all, attn_out, mlp_out,
        slope_all, relay_x, qkv_all,
        w3, wo, w1, w2, xv, other, gbv, attn_in, mlp_in, qkv, context, probs, act, slope, dh, dctx,
        dproj, means, inv_stds, tables, term, arrived, parts, full, act_rest, slope_rest,
        stats_all, x_mine, attn_t, mlp_t, vectors, plane_vectors, slices, segments, qkv_rest, dproj_rest, context_rest,
        load, store, send, recv, part_send, part_recv, back_send, back_recv,
        line_send, line_recv, plane_send, plane_recv, rest_load, rest_store, sum_send, sum_recv,
        slice_send, slice_recv, engine_send, segment_send, segment_recv, slice_load, grad_sems, sums, sum_store,
    ) = refs
    section, me = lax.axis_index("section"), lax.axis_index("tensor")
    row, rows_count = lax.axis_index("dp"), lax.axis_size("dp")
    tokens, width = xv.shape
    length = tokens // batch
    heads = qkv.shape[2] // HEAD
    hidden_width = act.shape[1]
    part = width // count
    row_tile = 32 if tokens % 32 == 0 else 16
    row_tiles = tokens // row_tile
    scale = 1.0 / math.sqrt(HEAD)

    qkv_loads = [pltpu.make_async_copy(w3_hbm.at[k], w3.at[k], load.at[k]) for k in range(3)]
    blocks = 4
    block = hidden_width // blocks

    def fc1_load(i):
        columns = tile_of(i, block)
        return pltpu.make_async_copy(w1_hbm.at[:, columns], w1.at[:, columns], load.at[3 + i])

    out_load = pltpu.make_async_copy(wo_hbm, wo, load.at[7])
    fc2_load = pltpu.make_async_copy(w2_hbm, w2, load.at[8])
    x_load = pltpu.make_async_copy(x_hbm, xv, load.at[9])
    go_load = pltpu.make_async_copy(go_hbm, gbv, load.at[10])

    @pl.when(section == 0)
    def _():
        x_load.start()

    go_load.start()

    def start_out_loads():
        out_load.start()
        fc2_load.start()

    pl.when(section == 1)(start_out_loads)
    for copy in qkv_loads:
        copy.start()
    for i in range(blocks):
        fc1_load(i).start()
    pl.when(section == 0)(start_out_loads)

    def at(section, index):
        return {"section": section, "tensor": index}

    steps = list(range(1, count))
    barrier = pltpu.get_barrier_semaphore()
    for step in range(count):
        peer = partner(me, step, count)[0]
        pl.semaphore_signal(barrier, inc=1, device_id=at(1 - section, peer), device_id_type=MESH)
        if step:
            pl.semaphore_signal(barrier, inc=1, device_id=at(section, peer), device_id_type=MESH)

    for step in range(1, rows_count):
        pl.semaphore_signal(
            barrier,
            inc=1,
            device_id={"dp": lax.rem(row + step, rows_count)},
            device_id_type=MESH,
        )

    balanced = count == 4
    opposite = partner(me, count - 1, count)[0]
    flows = (x_all, gb_all)

    def place_of(flow, origin):
        return (
            lambda: x_all.at[origin, me],
            lambda: gb_all.at[origin, me],
            lambda: context_all.at[origin],
            lambda: dproj_all.at[origin],
            lambda: relay_x.at[origin, 0],
            lambda: gb_all.at[origin, opposite],
            lambda: relay_x.at[origin, 1],
        )[flow]()

    def line_copy(flow, origin, up, own=None):
        place = place_of(flow, origin)
        return pltpu.make_async_remote_copy(
            src_ref=place if own is None else own,
            dst_ref=place,
            send_sem=line_send.at[flow, origin if up else jnp.where(origin == row, rows_count, origin)],
            recv_sem=line_recv.at[flow, origin],
            device_id={"dp": row + (1 if up else -1)},
            device_id_type=MESH,
        )

    def plane_copy(flow, origin, step):
        peer = partner(me, step, count)[0]
        return pltpu.make_async_remote_copy(
            src_ref=flows[flow].at[origin, me],
            dst_ref=flows[flow].at[origin, me],
            send_sem=plane_send.at[flow, origin, step],
            recv_sem=plane_recv.at[flow, origin, step],
            device_id=at(section, peer),
            device_id_type=MESH,
        )

    direct_steps = [1, 2] if balanced else steps

    def send_plane(flow, origin):
        for step in direct_steps[::-1]:
            plane_copy(flow, origin, step).start()

    def half_copy(flow, origin, half):
        owner = partner(me, 1 + half, count)[1]
        place = flows[flow].at[origin, owner, pl.ds(half * (tokens // 2), tokens // 2), :]
        return pltpu.make_async_remote_copy(
            src_ref=place,
            dst_ref=place,
            send_sem=plane_send.at[flow, origin, 3 * half],
            recv_sem=plane_recv.at[flow, origin, 3 * half],
            device_id=at(section, partner(me, 2 - half, count)[0]),
            device_id_type=MESH,
        )

    def relay_plane(flow, origin):
        if balanced:
            for step in direct_steps:
                plane_copy(flow, origin, step).wait_recv()
            for half in range(2):
                half_copy(flow, origin, half).start()

    def wait_plane(flow, origin):
        if balanced:
            for half in range(2):
                half_copy(flow, origin, half).wait_recv()
        else:
            for step in steps:
                plane_copy(flow, origin, step).wait_recv()

    def send_plane_of(flow):
        return lambda origin: send_plane(flow, origin)

    def relay_plane_of(flow):
        return lambda origin: relay_plane(flow, origin)

    def engine_copy(origin, step):
        second = balanced and step == 3
        peer = me if second else partner(me, step, count)[0]
        return pltpu.make_async_remote_copy(
            src_ref=relay_x.at[origin, int(second)],
            dst_ref=x_all.at[origin, opposite if second else me],
            send_sem=engine_send.at[origin, step],
            recv_sem=plane_recv.at[0, origin, step],
            device_id=at(1 - section, peer),
            device_id_type=MESH,
        )

    def send_engine(origin):
        for step in direct_steps[::-1] + [0]:
            engine_copy(origin, step).start()

    def send_engine_second(origin):
        if balanced:
            engine_copy(origin, 3).start()

    first_other = jnp.where(row == rows_count - 1, row - 1, row + 1)

    def send_engine_first(origin):
        pl.when(origin == first_other)(lambda: send_engine(origin))

    def send_engine_first_second(origin):
        pl.when(origin == first_other)(lambda: send_engine_second(origin))

    def send_engine_later(origin):
        @pl.when(origin != first_other)
        def _():
            send_engine(origin)
            send_engine_second(origin)

    def start_flow(flow, own):
        if flow in (0, 1, 4):
            own = own.at[:, tile_of(me, part)]
        if flow in (5, 6):
            own = own.at[:, tile_of(opposite, part)]

        @pl.when(row + 1 < rows_count)
        def _():
            line_copy(flow, row, True, own).start()

        @pl.when(row >= 1)
        def _():
            line_copy(flow, row, False, own).start()

    near = 2 * (rows_count - 1) // 3

    def hop(flow, third, after=lambda origin: None, limit=None):
        limit = rows_count if limit is None else limit

        def one(hops):
            @pl.when(row >= hops)
            def _():
                origin = row - hops
                line_copy(flow, origin, True).wait_recv()

                @pl.when((row + 1 < rows_count) & (hops < limit))
                def _():
                    line_copy(flow, origin, True).start()

                after(origin)

            @pl.when(row + hops < rows_count)
            def _():
                origin = row + hops
                line_copy(flow, origin, False).wait_recv()

                @pl.when((row >= 1) & (hops < limit))
                def _():
                    line_copy(flow, origin, False).start()

                after(origin)

        low, high = (1 + (rows_count - 1) * k // 3 for k in (third - 1, third))
        loop(high - low, lambda i: one(low + i))

    def thirds(third, body):
        def one(i):
            hops = 1 + i // 2
            origin = row + hops * (1 - 2 * lax.rem(i, 2))

            @pl.when((origin >= 0) & (origin < rows_count))
            def _():
                body(origin)

        low, high = (2 * ((rows_count - 1) * k // 3) for k in (third, third + 1))
        loop(high - low, lambda i: one(low + i))

    def nth_other(i):
        above, below = rows_count - 1 - row, row
        both = 2 * jnp.minimum(above, below)
        near_side = jnp.where(lax.rem(i, 2) == 0, 1 + i // 2, -(1 + i // 2))
        far_side = (1 + i - both // 2) * jnp.where(above > below, 1, -1)
        return row + jnp.where(i < both, near_side, far_side)

    def others(body, after=()):
        def one(i):
            body(nth_other(i), i)
            for number, action in after:
                pl.when(i == number - 1)(action)

        loop(rows_count - 1, one)

    def finish_flow(flow, limit=None, halves=True):
        limit = rows_count if limit is None else limit

        def one(origin):
            @pl.when((origin <= row) & (row + 1 < rows_count) & (row - origin < limit))
            def _():
                line_copy(flow, origin, True).wait_send()

            @pl.when((origin >= row) & (row >= 1) & (origin - row < limit))
            def _():
                line_copy(flow, origin, False).wait_send()

            @pl.when(origin != row)
            def _():
                if flow < 2:
                    for step in direct_steps:
                        plane_copy(flow, origin, step).wait_send()
                    if balanced and halves:
                        for half in range(2):
                            half_copy(flow, origin, half).wait_send()
                if flow == 4:
                    for step in [0] + steps:
                        engine_copy(origin, step).wait_send()

        loop(rows_count, one)

    def own_stores(flow, own):
        return [
            pltpu.make_async_copy(
                own.at[:, pl.ds(i * part, part)], flows[flow].at[row, i], store.at[flow * count + i]
            )
            for i in range(count)
        ]

    def scatter(kind, step):
        peer = partner(me, step, count)[0]
        return pltpu.make_async_remote_copy(
            src_ref=term.at[peer],
            dst_ref=arrived.at[kind, step - 1],
            send_sem=send.at[kind, step - 1],
            recv_sem=recv.at[kind, step - 1],
            device_id=at(section, peer),
            device_id_type=MESH,
        )

    def gather(number, step, target):
        peer = partner(me, step, count)[0]
        return pltpu.make_async_remote_copy(
            src_ref=parts.at[number, 0],
            dst_ref=parts.at[number, step],
            send_sem=part_send.at[number, step],
            recv_sem=part_recv.at[number, step],
            device_id=at(target, peer),
            device_id_type=MESH,
        )

    def back(number, step):
        return pltpu.make_async_remote_copy(
            src_ref=parts.at[number, step],
            dst_ref=parts.at[number, step],
            send_sem=back_send.at[number, step],
            recv_sem=back_recv.at[number, step],
            device_id=at(1 - section, me),
            device_id_type=MESH,
        )

    def place(number, step, target):
        owner = partner(me, step, count)[1]
        target[:, tile_of(owner, part)] = parts[number, step]

    def reduce(kind, number, with_input):
        for step in steps:
            scatter(kind, step).wait_recv()

        def rows_of(i):
            rows = tile_of(i, row_tile)
            total = term[me, rows, :].astype(F32)
            if with_input:
                total = total + xv[rows, tile_of(me, part)].astype(F32)
            for step in steps:
                total = total + arrived[kind, step - 1, rows, :].astype(F32)
            parts[number, 0, rows, :] = total.astype(BF16)

        loop(row_tiles, rows_of)

    def finish_sends(kind):
        for step in steps:
            scatter(kind, step).wait_send()

    def to_other_section(number):
        for step in steps[::-1] + [0]:
            gather(number, step, 1 - section).start()

    def from_own_section(number, target):
        place(number, 0, target)
        for step in steps:
            back(number, step).wait_recv()
            place(number, step, target)
        for step in [0] + steps:
            gather(number, step, 1 - section).wait_send()

    def from_other_section(number, target):
        gather(number, 0, 1 - section).wait_recv()
        place(number, 0, target)
        for step in steps:
            gather(number, step, 1 - section).wait_recv()
            back(number, step).start()
            place(number, step, target)

    def finish_back(number):
        for step in steps:
            back(number, step).wait_send()

    def start_within(number):
        for step in steps[::-1]:
            gather(number, step, section).start()

    def finish_within(number, target):
        place(number, 0, target)
        for step in steps:
            gather(number, step, section).wait_recv()
            place(number, step, target)
        for step in steps:
            gather(number, step, section).wait_send()

    def each_chunk(kind, compute, sends=True):
        def chunk(i):
            step = count - 1 - i
            owner = partner(me, step, count)[0]
            loop(part // TILE, lambda j: compute(owner, j))

            @pl.when((step > 0) & sends)
            def _():
                scatter(kind, step).start()

        loop(count, chunk)

    lane = lanes_of((1, LANES)).astype(F32)
    exponent = jnp.where(lane < ROT // 2, lane, lane - ROT // 2)
    frequency = jnp.exp(exponent * (-2.0 * math.log(10000.0) / ROT))
    row_index = lax.broadcasted_iota(jnp.int32, (length, length), 0)
    column_index = lax.broadcasted_iota(jnp.int32, (length, length), 1)

    def segments_of(values):
        across = values.astype(F32)
        down = jnp.sum(jnp.where(row_index == column_index, across, 0.0), axis=1, keepdims=True)
        return across, down

    def fill_tables(slot, values_of):
        for b in range(batch):
            rows = pl.ds(b * length, length)
            across, down = segments_of(values_of(b))
            number_of = jnp.sum((across < down).astype(F32), axis=1, keepdims=True)
            index = lax.broadcasted_iota(jnp.int32, (length, 1), 0).astype(F32)
            angles = (index - number_of) * frequency
            inside = lanes_of((length, LANES)) < ROT
            tables[slot, rows, :LANES] = jnp.where(inside, jnp.cos(angles), 1.0)
            tables[slot, rows, LANES:] = jnp.where(inside, jnp.sin(angles), 0.0)

    fill_tables(0, lambda b: seg_row[b : b + 1, :])

    def softmax(projected, values, b, h):
        rows, columns = tile_of(b, length), tile_of(h, HEAD)
        across, down = segments_of(values)
        allowed = (across == down) & (column_index <= row_index)
        scores = dot_nt(projected[0, rows, columns], projected[1, rows, columns]) * scale
        scores = jnp.where(allowed, scores, -jnp.inf)
        row_max = jnp.max(scores, axis=-1, keepdims=True)
        total = jnp.sum(jnp.exp(scores - row_max), axis=-1, keepdims=True)
        return jnp.exp(scores - (row_max + jnp.log(total)))

    def attend(prob, projected, target, b, h):
        rows, columns = tile_of(b, length), tile_of(h, HEAD)
        target[rows, columns] = dot(prob.astype(BF16), projected[2, rows, columns]).astype(BF16)

    def attend_backward(prob, projected, slot, target, b, h):
        rows, columns = tile_of(b, length), tile_of(h, HEAD)
        cosine, sine = tables[slot, rows, :LANES], tables[slot, rows, LANES:]
        queries, keys, values = (projected[k, rows, columns] for k in range(3))
        d_context = dctx[rows, columns]
        d_values = dot_tn(prob.astype(BF16), d_context)
        d_probs = dot_nt(d_context, values)
        delta = jnp.sum(prob * d_probs, axis=-1, keepdims=True)
        d_scores = (prob * (d_probs - delta) * scale).astype(BF16)
        for k, gradient in ((0, dot(d_scores, keys)), (1, dot_tn(d_scores, queries))):
            first = unrotated(gradient[:, :LANES], cosine, sine)
            start = pl.multiple_of(h * HEAD, HEAD)
            target[k, rows, pl.ds(start, LANES)] = first.astype(BF16)
            start = pl.multiple_of(h * HEAD + LANES, LANES)
            target[k, rows, pl.ds(start, HEAD - LANES)] = gradient[:, LANES:].astype(BF16)
        target[2, rows, columns] = d_values.astype(BF16)

    def each_pair(body):
        def row_of(b):
            for h in range(heads):
                body(b, h)

        loop(batch, row_of)

    def project(projected, slot):
        def rotary_head(i):
            which, h = i // heads, lax.rem(i, heads)
            tile = dot(attn_in[...], w3[which, :, tile_of(h, HEAD)])
            first = rotated(tile[:, :LANES], tables[slot, :, :LANES], tables[slot, :, LANES:])
            start = pl.multiple_of(h * HEAD, HEAD)
            projected[which, :, pl.ds(start, LANES)] = first.astype(BF16)
            start = pl.multiple_of(h * HEAD + LANES, LANES)
            projected[which, :, pl.ds(start, HEAD - LANES)] = tile[:, LANES:].astype(BF16)

        def value_head(h):
            columns = tile_of(h, HEAD)
            projected[2, :, columns] = dot(attn_in[...], w3[2, :, columns]).astype(BF16)

        loop(2 * heads, rotary_head)
        loop(heads, value_head)

    def segment_copy(step):
        return pltpu.make_async_remote_copy(
            src_ref=seg_row,
            dst_ref=segments.at[row],
            send_sem=segment_send.at[step],
            recv_sem=segment_recv.at[step],
            device_id={"dp": lax.rem(row + step, rows_count)},
            device_id_type=MESH,
        )

    def d_context_head(h):
        dctx[:, tile_of(h, HEAD)] = dot_nt(gbv[...], wo[tile_of(h, HEAD), :]).astype(BF16)

    def meet():
        pl.semaphore_wait(barrier, 2 * count - 1 + rows_count - 1)
        for step in range(1, rows_count):
            segment_copy(step).start()


    @pl.when(section == 0)
    def _():
        x_load.wait()

    @pl.when(section == 1)
    def _():
        meet()
        start_flow(4, x_hbm)
        go_load.wait()
        out_load.wait()
        loop(heads, d_context_head)
        if balanced:
            start_flow(6, x_hbm)
        hop(4, 1, send_engine_first)
        if balanced:
            hop(6, 1, send_engine_first_second)
        fc2_load.wait()

        def d_act_tile(i):
            columns = tile_of(i, TILE)
            slope[:, columns] = dot_nt(gbv[...], w2[columns, :])

        loop(hidden_width // TILE, d_act_tile)
        for third in (2, 3):
            if balanced:
                hop(6, third)
            hop(4, third)
            if third == 2:
                start_flow(1, gbv)
                if balanced:
                    start_flow(5, gbv)
        hop(1, 1)
        if balanced:
            hop(5, 1)
        from_other_section(0, xv)
        start_flow(0, xv)
        for third in range(3):
            thirds(third, send_engine_later)

    for copy in own_stores(0, xv):
        copy.start()

    def norm_rows(i):
        rows = tile_of(i, row_tile)
        normed, mean, inv_std = row_norm(xv[rows, :].astype(F32))
        means[rows, :] = mean
        inv_stds[rows, :] = inv_std
        attn_in[rows, :] = (normed * gains[0:1, :] + biases[0:1, :]).astype(BF16)
        mlp_in[rows, :] = (normed * gains[1:2, :] + biases[1:2, :]).astype(BF16)

    loop(row_tiles, norm_rows)

    for copy in qkv_loads:
        copy.wait()
    project(qkv, 0)

    def own_attention(b, h):
        prob = softmax(qkv, seg_row[pl.ds(b, 1), :], b, h)
        probs[b * heads + h] = prob
        attend(prob, qkv, context, b, h)

    each_pair(own_attention)

    @pl.when(section == 1)
    def _():
        hop(0, 1, send_plane_of(0))
        hop(1, 2)
        if balanced:
            hop(5, 2)


    def fc1_block(i):
        fc1_load(i).wait()

        def fc1_tile(j):
            columns = tile_of(i * (block // TILE) + j, TILE)
            value, derivative = gelu_parts(dot(mlp_in[...], w1[:, columns]))
            act[:, columns] = value.astype(BF16)

            @pl.when(section == 0)
            def _():
                slope[:, columns] = derivative

            @pl.when(section == 1)
            def _():
                dh[:, columns] = (slope[:, columns] * derivative).astype(BF16)

        loop(block // TILE, fc1_tile)

    loop(blocks, fc1_block)

    @pl.when(section == 1)
    def _():
        hop(0, 2, send_plane_of(0))

    @pl.when(section == 0)
    def _():
        out_load.wait()
        fc2_load.wait()
        go_load.wait()

    tiles = hidden_width // TILE

    def act_store(origin, i):
        columns = tile_of(i, TILE)
        return pltpu.make_async_copy(
            act_rest.at[:, columns], act_all.at[origin, :, columns], rest_store.at[0]
        )

    def dh_store(origin, i):
        columns = tile_of(i, TILE)
        return pltpu.make_async_copy(
            act_rest.at[:, columns], dh_all.at[origin, :, columns], rest_store.at[0]
        )

    def slope_store(origin, i):
        columns = tile_of(i, TILE)
        return pltpu.make_async_copy(
            slope_rest.at[:, columns], slope_all.at[origin, :, columns], rest_store.at[1]
        )

    def load_block(flow, origin):
        if flow == 0:

            @pl.when(section == 0)
            def _():
                for step in [0] + steps:
                    engine_copy(origin, step).wait_recv()

            pl.when(section == 1)(lambda: wait_plane(flow, origin))
        else:
            pl.when(section == 0)(lambda: wait_plane(flow, origin))

            @pl.when(section == 1)
            def _():
                for step in direct_steps:
                    plane_copy(flow, origin, step).wait_recv()

        copies = [
            pltpu.make_async_copy(
                flows[flow].at[origin, i], attn_in.at[:, pl.ds(i * part, part)], rest_load.at[i]
            )
            for i in range(count)
        ]
        for copy in copies:
            copy.start()
        return copies

    def attention_stores(origin):
        return [
            pltpu.make_async_copy(qkv_rest, qkv_all.at[origin], rest_load.at[count + 1]),
            pltpu.make_async_copy(context_rest, context_all.at[origin], rest_load.at[count + 2]),
        ]

    def far_of(origin):
        return (section == 0) & ((origin - row > near) | (row - origin > near))

    def rest_forward(origin, index):
        for copy in load_block(0, origin):
            copy.wait()

        def norm_rows(i):
            rows = tile_of(i, row_tile)
            normed, mean, inv_std = row_norm(attn_in[rows, :].astype(F32))
            first = lanes_of((row_tile, LANES)) == 0
            stats_all[origin, rows, :] = jnp.where(first, mean, inv_std)
            mlp_in[rows, :] = (normed * gains[1:2, :] + biases[1:2, :]).astype(BF16)
            attn_in[rows, :] = (normed * gains[0:1, :] + biases[0:1, :]).astype(BF16)

        loop(row_tiles, norm_rows)

        @pl.when(section == 0)
        def _():
            fill_tables(1, lambda b: segments[origin, b : b + 1, :])
            project(qkv_rest, 1)

            def attention(b, h):
                prob = softmax(qkv_rest, segments[origin, pl.ds(b, 1), :], b, h)
                attend(prob, qkv_rest, context_rest, b, h)

            each_pair(attention)
            for copy in attention_stores(origin):
                copy.start()

        def tile(i):
            columns = tile_of(i, TILE)
            value, derivative = gelu_parts(dot(mlp_in[...], w1[:, columns]))
            act_rest[:, columns] = value.astype(BF16)
            slope_rest[:, columns] = derivative
            act_store(origin, i).start()
            slope_store(origin, i).start()

        loop(tiles, tile)

        pltpu.make_async_copy(act_rest, act_all.at[origin], rest_store.at[0]).wait()
        pltpu.make_async_copy(slope_rest, slope_all.at[origin], rest_store.at[1]).wait()

        @pl.when(section == 0)
        def _():
            for copy in attention_stores(origin):
                copy.wait()

    def slope_load(origin):
        return pltpu.make_async_copy(slope_all.at[origin], slope_rest, rest_load.at[count])

    def rest_backward(origin, index):
        copies = load_block(1, origin)
        for copy in copies + [slope_load(origin)]:
            copy.wait()

        def tile(i):
            columns = tile_of(i, TILE)
            d_act = dot_nt(attn_in[...], w2[columns, :])
            act_rest[:, columns] = (d_act * slope_rest[:, columns]).astype(BF16)
            dh_store(origin, i).start()

        qkv_load = pltpu.make_async_copy(qkv_all.at[origin], qkv_rest, rest_load.at[count + 1])
        dproj_store = pltpu.make_async_copy(
            dproj_rest, dproj_all.at[origin], rest_load.at[count + 2]
        )
        far = far_of(origin)
        pl.when(far)(qkv_load.start)
        loop(tiles, tile)

        @pl.when(index < rows_count - 2)
        def _():
            slope_load(nth_other(index + 1)).start()

        @pl.when(far)
        def _():
            qkv_load.wait()
            fill_tables(1, lambda b: segments[origin, b : b + 1, :])

            def head(h):
                columns = tile_of(h, HEAD)
                dctx[:, columns] = dot_nt(attn_in[...], wo[columns, :]).astype(BF16)

            loop(heads, head)

            def attention(b, h):
                prob = softmax(qkv_rest, segments[origin, pl.ds(b, 1), :], b, h)
                attend_backward(prob, qkv_rest, 1, dproj_rest, b, h)

            each_pair(attention)
            dproj_store.start()
            dproj_store.wait()

        pltpu.make_async_copy(act_rest, dh_all.at[origin], rest_store.at[0]).wait()

    def out_tile(owner, j):
        columns = tile_of(owner * (part // TILE) + j, TILE)
        total = dot(context[...], wo[:, columns]) + dot(act[...], w2[:, columns])
        term[owner, :, tile_of(j, TILE)] = total.astype(BF16)

    def own_stats(i):
        rows = tile_of(i, row_tile)
        first = lanes_of((row_tile, LANES)) == 0
        stats_all[row, rows, :] = jnp.where(first, means[rows, :], inv_stds[rows, :])

    layer_store = pltpu.make_async_copy(other, layer_out, store.at[2 * count + 4])

    def grad_store(i):
        rows = tile_of(i, row_tile)
        return pltpu.make_async_copy(slope.at[rows, :], input_grad.at[rows, :], grad_sems.at[0])

    transposed_stores = [
        pltpu.make_async_copy(attn_t, attn_out, store.at[2 * count + 6]),
        pltpu.make_async_copy(mlp_t, mlp_out, store.at[2 * count + 7]),
    ]
    width_mine = width // rows_count

    def transposed_inputs():
        for copy in own_stores(0, xv):
            copy.wait()
        start = row * width_mine
        chunk, offset = start // part, pl.multiple_of(lax.rem(start, part), LANES)
        loads = [
            pltpu.make_async_copy(
                x_all.at[i, chunk, :, pl.ds(offset, width_mine)], x_mine.at[i], slice_load.at[i]
            )
            for i in range(rows_count)
        ]
        for copy in loads:
            copy.start()
        for copy in loads:
            copy.wait()
        all_tokens = rows_count * tokens

        def columns_of(i):
            columns = tile_of(i, LANES)
            mean = stats_all[:, :, 0:1].reshape(all_tokens, 1)
            inv_std = stats_all[:, :, 1:2].reshape(all_tokens, 1)
            values = x_mine[:, :, columns].reshape(all_tokens, LANES).astype(F32)
            normed = (values - mean) * inv_std
            whole = tile_of(start // LANES + i, LANES)
            for j, target in enumerate((attn_t, mlp_t)):
                scaled = normed * gains[j : j + 1, whole] + biases[j : j + 1, whole]
                target[columns, :] = scaled.astype(BF16).T

        loop(width_mine // LANES, columns_of)
        for copy in transposed_stores:
            copy.start()


    @pl.when(section == 0)
    def _():
        meet()
        each_chunk(0, out_tile)
        reduce(0, 0, True)
        to_other_section(0)
        finish_sends(0)
        for step in range(1, rows_count):
            segment_copy(step).wait_recv()
        others(rest_forward)
        from_own_section(0, other)
        layer_store.start()
        from_other_section(1, full)

        def gradient_rows(i):
            rows = tile_of(i, row_tile)
            normed, _, inv_std = row_norm(other[rows, :].astype(F32))
            dx = row_norm_backward(full[rows, :].astype(F32), normed, inv_std)
            gbv[rows, :] = (gbv[rows, :].astype(F32) + dx).astype(BF16)

        loop(row_tiles, gradient_rows)
        start_flow(1, gbv)
        finish_back(1)

        def d_hidden_tile(i):
            columns = tile_of(i, TILE)
            d_act = dot_nt(gbv[...], w2[columns, :])
            dh[:, columns] = (d_act * slope[:, columns]).astype(BF16)

        loop(hidden_width // TILE, d_hidden_tile)
        loop(heads, d_context_head)


    each_pair(lambda b, h: attend_backward(probs[b * heads + h], qkv, 0, dproj, b, h))

    @pl.when(section == 0)
    def _():
        hop(1, 1, send_plane_of(1))

    @pl.when(section == 1)
    def _():
        start_flow(3, dproj)

    def gradient_tile(owner, j):
        columns = tile_of(owner * (part // TILE) + j, TILE)
        d_attn = dot_nt(dproj[0], w3[0, columns, :])
        d_attn = d_attn + dot_nt(dproj[1], w3[1, columns, :])
        d_attn = d_attn + dot_nt(dproj[2], w3[2, columns, :])
        d_mlp = dot_nt(dh[...], w1[columns, :])
        normed = (xv[:, columns].astype(F32) - means[...]) * inv_stds[...]
        total = d_attn * gains[0:1, columns] + d_mlp * gains[1:2, columns]
        term[owner, :, tile_of(j, TILE)] = total.astype(BF16)
        vectors[0:1, columns] = jnp.sum(d_attn * normed, axis=0, keepdims=True)
        vectors[1:2, columns] = jnp.sum(d_mlp * normed, axis=0, keepdims=True)
        vectors[2:3, columns] = jnp.sum(d_attn, axis=0, keepdims=True)
        vectors[3:4, columns] = jnp.sum(d_mlp, axis=0, keepdims=True)

    each_chunk(1, gradient_tile, section == 1)

    outs = [
        (act, act_all.at[row]),
        (context, context_all.at[row]),
        (dh, dh_all.at[row]),
        (dproj, dproj_all.at[row]),
    ]
    stores = own_stores(1, gbv)
    stores += [
        pltpu.make_async_copy(a, b, store.at[2 * count + i]) for i, (a, b) in enumerate(outs)
    ]
    for copy in stores:
        copy.start()

    def sum_copy(step):
        peer = partner(me, step, count)[0]
        return pltpu.make_async_remote_copy(
            src_ref=vectors,
            dst_ref=plane_vectors.at[step],
            send_sem=sum_send.at[step],
            recv_sem=sum_recv.at[step],
            device_id=at(section, peer),
            device_id_type=MESH,
        )

    mine = width // rows_count

    def slice_copy(step):
        target = lax.rem(row + step, rows_count)
        return pltpu.make_async_remote_copy(
            src_ref=plane_vectors.at[0, :, tile_of(target, mine)],
            dst_ref=slices.at[step],
            send_sem=slice_send.at[step],
            recv_sem=slice_recv.at[step],
            device_id={"dp": target},
            device_id_type=MESH,
        )

    for step in steps:
        sum_copy(step).start()

    def sum_plane():
        total = vectors[...]
        for step in steps:
            sum_copy(step).wait_recv()
            total = total + plane_vectors[step]
        plane_vectors[0] = total
        for step in range(1, rows_count):
            slice_copy(step).start()

    sum_stores = [
        pltpu.make_async_copy(sums.at[0], gain_grads, sum_store.at[0]),
        pltpu.make_async_copy(sums.at[1], bias_grads, sum_store.at[1]),
    ]

    def sum_line():
        total = plane_vectors[0, :, tile_of(row, mine)]
        for step in range(1, rows_count):
            slice_copy(step).wait_recv()
            total = total + slices[step]
        sums[0] = total[:2]
        sums[1] = total[2:]
        for copy in sum_stores:
            copy.start()
        for step in range(1, rows_count):
            slice_copy(step).wait_send()
        for step in steps:
            sum_copy(step).wait_send()


    def input_gradient():
        def rows_of(i):
            rows = tile_of(i, row_tile)
            inv_std = inv_stds[rows, :]
            normed = (xv[rows, :].astype(F32) - means[rows, :]) * inv_std
            dx = row_norm_backward(full[rows, :].astype(F32), normed, inv_std)
            slope[rows, :] = gbv[rows, :].astype(F32) + dx
            grad_store(i).start()

        loop(row_tiles, rows_of)

    @pl.when(section == 0)
    def _():
        slope_load(nth_other(0)).start()
        thirds(0, relay_plane_of(1))
        hop(1, 2, send_plane_of(1))
        loop(row_tiles, own_stats)
        transposed_inputs()
        hop(1, 3, send_plane_of(1))
        start_flow(3, dproj)
        at_end = (row == 0) | (row == rows_count - 1)
        pl.when(at_end)(lambda: thirds(1, relay_plane_of(1)))

        def after_first():
            pl.when(jnp.logical_not(at_end))(lambda: thirds(1, relay_plane_of(1)))
            thirds(2, relay_plane_of(1))
            for step in steps[::-1]:
                scatter(1, step).start()
            sum_plane()

        def after_second():
            reduce(1, 2, False)
            start_within(2)
            hop(3, 1, limit=near)
            sum_line()

        others(rest_backward, [(1, after_first), (2, after_second)])
        finish_within(2, full)
        finish_sends(1)
        input_gradient()
        hop(3, 2, limit=near)

    @pl.when(section == 1)
    def _():
        finish_back(0)
        hop(1, 3)
        if balanced:
            hop(5, 3)
        reduce(1, 1, False)
        to_other_section(1)
        thirds(0, relay_plane_of(0))
        hop(0, 3, send_plane_of(0))
        thirds(1, relay_plane_of(0))
        finish_sends(1)
        each_chunk(0, out_tile, False)
        hop(3, 1)
        start_flow(2, context)
        loop(row_tiles, own_stats)
        from_own_section(1, full)
        for step in steps[::-1]:
            scatter(0, step).start()
        sum_plane()

        def share_gradients():
            for third in range(3):
                thirds(third, send_plane_of(1))
            hop(3, 2)
            hop(2, 1)

        others(
            rest_forward, [(1, lambda: thirds(2, relay_plane_of(0))), (2, share_gradients)]
        )
        slope_load(nth_other(0)).start()
        input_gradient()

        def after_second():
            transposed_inputs()
            reduce(0, 2, True)
            start_within(2)
            sum_line()
            hop(2, 2)

        others(rest_backward, [(2, after_second)])
        finish_within(2, other)
        layer_store.start()
        hop(3, 3)
        hop(2, 3)
        finish_sends(0)

    for copy in stores + [layer_store] + transposed_stores + sum_stores:
        copy.wait()
    pltpu.make_async_copy(slope, input_grad, grad_sems.at[0]).wait()
    @pl.when(section == 0)
    def _():
        finish_flow(1)
        finish_flow(3, near)

    @pl.when(section == 1)
    def _():
        for step in range(1, rows_count):
            segment_copy(step).wait_recv()
        finish_flow(1, halves=False)
        for flow in (0, 2, 3, 4) + ((5, 6) if balanced else ()):
            finish_flow(flow)

    for step in range(1, rows_count):
        segment_copy(step).wait_send()


def chain(attn_input, grad_output, segment_ids, weights):
    w_qkv, w_out, w_fc1, w_fc2, gains, biases = weights
    batch, length, width = attn_input.shape
    tokens = batch * length
    count = lax.axis_size("tensor")
    inner, hidden = w_qkv.shape[2], w_fc1.shape[1]
    part = width // count
    heads = inner // HEAD
    anywhere, vmem = pl.BlockSpec(memory_space=pl.ANY), pl.BlockSpec(memory_space=pltpu.VMEM)
    like = jax.ShapeDtypeStruct
    rows_count = lax.axis_size("dp")
    wide, narrow = (tokens, width), (tokens, inner)
    dma = pltpu.SemaphoreType.DMA
    return pl.pallas_call(
        functools.partial(chain_kernel, count, batch),
        out_shape=[
            like(wide, BF16),
            like(wide, F32),
            like((2, width // rows_count), F32),
            like((2, width // rows_count), F32),
            like((rows_count, count, tokens, part), BF16),
            like((rows_count, count, tokens, part), BF16),
            like((rows_count, tokens, inner), BF16),
            like((rows_count, 3, tokens, inner), BF16),
            like((rows_count, tokens, hidden), BF16),
            like((rows_count, tokens, hidden), BF16),
            like((width // rows_count, rows_count * tokens), BF16),
            like((width // rows_count, rows_count * tokens), BF16),
            like((rows_count, tokens, hidden), F32),
            like((rows_count, 2, tokens, part), BF16),
            like((rows_count, 3, tokens, inner), BF16),
        ],
        in_specs=[anywhere, anywhere, vmem] + [anywhere] * 4 + [vmem, vmem],
        out_specs=[anywhere] * 10 + [anywhere] * 5,
        scratch_shapes=[
            pltpu.VMEM((3, width, inner), BF16),
            pltpu.VMEM((inner, width), BF16),
            pltpu.VMEM((width, hidden), BF16),
            pltpu.VMEM((hidden, width), BF16),
            pltpu.VMEM(wide, BF16),
            pltpu.VMEM(wide, BF16),
            pltpu.VMEM(wide, BF16),
            pltpu.VMEM(wide, BF16),
            pltpu.VMEM(wide, BF16),
            pltpu.VMEM((3, tokens, inner), BF16),
            pltpu.VMEM(narrow, BF16),
            pltpu.VMEM((batch * heads, length, length), F32),
            pltpu.VMEM((tokens, hidden), BF16),
            pltpu.VMEM((tokens, hidden), F32),
            pltpu.VMEM((tokens, hidden), BF16),
            pltpu.VMEM(narrow, BF16),
            pltpu.VMEM((3, tokens, inner), BF16),
            pltpu.VMEM((tokens, 1), F32),
            pltpu.VMEM((tokens, 1), F32),
            pltpu.VMEM((2, tokens, 2 * LANES), F32),
            pltpu.VMEM((count, tokens, part), BF16),
            pltpu.VMEM((2, count - 1, tokens, part), BF16),
            pltpu.VMEM((3, count, tokens, part), BF16),
            pltpu.VMEM(wide, BF16),
            pltpu.VMEM((tokens, hidden), BF16),
            pltpu.VMEM((tokens, hidden), F32),
            pltpu.VMEM((rows_count, tokens, LANES), F32),
            pltpu.VMEM((rows_count, tokens, width // rows_count), BF16),
            pltpu.VMEM((width // rows_count, rows_count * tokens), BF16),
            pltpu.VMEM((width // rows_count, rows_count * tokens), BF16),
            pltpu.VMEM((4, width), F32),
            pltpu.VMEM((count, 4, width), F32),
            pltpu.VMEM((rows_count, 4, width // rows_count), F32),
            pltpu.VMEM((rows_count, batch, length), jnp.int32),
            pltpu.VMEM((3, tokens, inner), BF16),
            pltpu.VMEM((3, tokens, inner), BF16),
            pltpu.VMEM(narrow, BF16),
            dma((11,)),
            dma((2 * count + 8,)),
            dma((2, count - 1)),
            dma((2, count - 1)),
            dma((3, count)),
            dma((3, count)),
            dma((2, count)),
            dma((2, count)),
            dma((7, rows_count + 1)),
            dma((7, rows_count)),
            dma((2, rows_count, count)),
            dma((2, rows_count, count)),
            dma((count + 3,)),
            dma((2,)),
            dma((count,)),
            dma((count,)),
            dma((rows_count,)),
            dma((rows_count,)),
            dma((rows_count, count)),
            dma((rows_count,)),
            dma((rows_count,)),
            dma((rows_count,)),
            dma((1,)),
            pltpu.VMEM((2, 2, width // rows_count), F32),
            dma((2,)),
        ],
        compiler_params=pltpu.CompilerParams(
            collective_id=0, has_side_effects=True, vmem_limit_bytes=67_043_328
        ),
        name="chain",
    )(
        attn_input.reshape(wide),
        grad_output.reshape(wide),
        segment_ids,
        jnp.transpose(w_qkv, (1, 0, 2)),
        w_out,
        w_fc1,
        w_fc2,
        gains,
        biases,
    )


def weight_kernel(*refs):
    (
        gb_all, attn_in, mlp_in, context_all, dproj_all, act_all, dh_all,
        layer_in, grad_in, gain_in, bias_in,
        g_qkv, g_out, g_fc1, g_fc2, layer_out, input_grad, gain_out, bias_out,
        gb_mine, context, dproj, act, attn_t, mlp_t, r_qkv, r_out, r_fc1, r_fc2,
        layer, grad, load, act_load, dh_load, store, through, gb_load,
    ) = refs
    blocks, tokens, mine = gb_mine.shape
    rows = blocks * tokens
    part = gb_all.shape[3]
    inner, hidden = context.shape[2], act.shape[2]
    start = lax.axis_index("dp") * mine
    chunk, offset = start // part, pl.multiple_of(lax.rem(start, part), LANES)
    piece = hidden // 4

    def slice_loads(source, target, sems):
        return [
            pltpu.make_async_copy(
                source.at[i, chunk, :, pl.ds(offset, mine)], target.at[i], sems.at[i]
            )
            for i in range(blocks)
        ]

    def piece_load(source, target, sems, i):
        columns = pl.ds(i * piece, piece)
        return pltpu.make_async_copy(source.at[:, :, columns], target.at[:, :, columns], sems.at[i])

    gb_loads = slice_loads(gb_all, gb_mine, gb_load)
    in_loads = [
        pltpu.make_async_copy(attn_in, attn_t, load.at[0]),
        pltpu.make_async_copy(mlp_in, mlp_t, load.at[1]),
    ]
    context_load = pltpu.make_async_copy(context_all, context, load.at[2])
    dproj_load = pltpu.make_async_copy(dproj_all, dproj, load.at[3])
    act_loads = [piece_load(act_all, act, act_load, i) for i in range(4)]
    dh_loads = [piece_load(dh_all, act, dh_load, i) for i in range(4)]
    gain_out[...] = gain_in[...]
    bias_out[...] = bias_in[...]
    ins = [
        pltpu.make_async_copy(layer_in, layer, through.at[0]),
        pltpu.make_async_copy(grad_in, grad, through.at[1]),
    ]
    outs = [
        pltpu.make_async_copy(layer, layer_out, through.at[2]),
        pltpu.make_async_copy(grad, input_grad, through.at[3]),
    ]
    for copy in gb_loads + [context_load]:
        copy.start()

    def out_copy(source, target, index):
        return pltpu.make_async_copy(source, target, store.at[index])

    for copy in gb_loads + [context_load]:
        copy.wait()
    for copy in act_loads + in_loads[1:]:
        copy.start()
    gb_rows = gb_mine[...].reshape(rows, mine)

    def out_tile(i):
        tile = tile_of(i, WIDE_TILE)
        r_out[tile, :] = dot_tn(context[:, :, tile].reshape(rows, WIDE_TILE), gb_rows)

    loop(inner // WIDE_TILE, out_tile)
    copies = [out_copy(r_out, g_out, 0)]
    copies[0].start()

    def fc2_copy(i):
        tile = tile_of(i, WIDE_TILE)
        return out_copy(r_fc2.at[tile, :], g_fc2.at[tile, :], 1 + i)

    def fc2_tile(i):
        tile = tile_of(i, WIDE_TILE)
        r_fc2[tile, :] = dot_tn(act[:, :, tile].reshape(rows, WIDE_TILE), gb_mine[...].reshape(rows, mine))
        fc2_copy(i).start()

    per = piece // WIDE_TILE
    for i in range(4):
        act_loads[i].wait()
        loop(per, lambda j: fc2_tile(i * per + j))
        dh_loads[i].start()
    for copy in [dproj_load] + in_loads[:1] + ins:
        copy.start()

    def fc1_copy(i):
        tile = tile_of(i, WIDE_TILE)
        return out_copy(r_fc1.at[:, tile], g_fc1.at[:, tile], 1 + hidden // WIDE_TILE + i)

    def fc1_tile(i):
        tile = tile_of(i, WIDE_TILE)
        r_fc1[:, tile] = dot(mlp_t[...], act[:, :, tile].reshape(rows, WIDE_TILE))
        fc1_copy(i).start()

    in_loads[1].wait()
    for i in range(4):
        dh_loads[i].wait()
        loop(per, lambda j: fc1_tile(i * per + j))
    dproj_load.wait()
    in_loads[0].wait()
    for copy in ins:
        copy.wait()
    for copy in outs:
        copy.start()
    per = inner // WIDE_TILE

    def qkv_copy(i):
        which, tile = i // per, tile_of(lax.rem(i, per), WIDE_TILE)
        return out_copy(r_qkv.at[which, :, tile], g_qkv.at[which, :, tile], 1 + 2 * (hidden // WIDE_TILE) + i)

    def qkv_tile(i):
        which, tile = i // per, tile_of(lax.rem(i, per), WIDE_TILE)
        r_qkv[which, :, tile] = dot(attn_t[...], dproj[:, which, :, tile].reshape(rows, WIDE_TILE))
        qkv_copy(i).start()

    loop(3 * per, qkv_tile)
    for copy in copies + outs:
        copy.wait()
    loop(hidden // WIDE_TILE, lambda i: fc2_copy(i).wait())
    loop(hidden // WIDE_TILE, lambda i: fc1_copy(i).wait())
    loop(3 * per, lambda i: qkv_copy(i).wait())


def weight_gradients(
    gb_all, attn_in, mlp_in, context_all, dproj_all, act_all, dh_all, *through
):
    blocks, count, tokens, part = gb_all.shape
    mine = count * part // lax.axis_size("dp")
    inner, hidden = context_all.shape[2], act_all.shape[2]
    anywhere, vmem = pl.BlockSpec(memory_space=pl.ANY), pl.BlockSpec(memory_space=pltpu.VMEM)
    shapes = [(3, mine, inner), (inner, mine), (mine, hidden), (hidden, mine)]
    dma = pltpu.SemaphoreType.DMA
    return pl.pallas_call(
        weight_kernel,
        out_shape=[jax.ShapeDtypeStruct(shape, F32) for shape in shapes]
        + [jax.ShapeDtypeStruct(value.shape, value.dtype) for value in through],
        in_specs=[anywhere] * 7
        + [anywhere, anywhere, vmem, vmem],
        out_specs=[anywhere] * 6 + [vmem, vmem],
        scratch_shapes=[
            pltpu.VMEM((blocks, tokens, mine), BF16),
            pltpu.VMEM((blocks, tokens, inner), BF16),
            pltpu.VMEM((blocks, 3, tokens, inner), BF16),
            pltpu.VMEM((blocks, tokens, hidden), BF16),
            pltpu.VMEM((mine, blocks * tokens), BF16),
            pltpu.VMEM((mine, blocks * tokens), BF16),
        ]
        + [pltpu.VMEM(shape, F32) for shape in shapes]
        + [pltpu.VMEM(value.shape, value.dtype) for value in through[:2]]
        + [
            dma((4,)),
            dma((4,)),
            dma((4,)),
            dma((1 + 2 * (hidden // WIDE_TILE) + 3 * (inner // WIDE_TILE),)),
            dma((4,)),
            dma((blocks,)),
        ],
        compiler_params=pltpu.CompilerParams(vmem_limit_bytes=67_043_328),
        name="weights",
    )(gb_all, attn_in, mlp_in, context_all, dproj_all, act_all, dh_all, *through)


def shards(
    block_input, grad_output, segment_ids, w_qkv, w_out, w_fc1, w_fc2, norm_gains, norm_biases
):
    batch, length, width = block_input.shape
    weights = (w_qkv[0], w_out[0], w_fc1[0], w_fc2[0], norm_gains[0], norm_biases[0])
    (
        layer_out, input_grads, gain_grads, bias_grads, _, gb_all, context, d_proj, activated,
        d_hidden, attn_in, mlp_in, *_,
    ) = chain(block_input, grad_output, segment_ids, weights)
    g_qkv, g_out, g_fc1, g_fc2, layer_out, input_grads, gain_grads, bias_grads = weight_gradients(
        gb_all, attn_in, mlp_in, context, d_proj, activated, d_hidden,
        layer_out, input_grads, gain_grads, bias_grads,
    )
    shape = (1, batch, length, width)
    return (
        layer_out.reshape(shape),
        input_grads.reshape(shape),
        jnp.transpose(g_qkv, (1, 0, 2))[None],
        g_out[None],
        g_fc1[None],
        g_fc2[None],
        gain_grads[None],
        bias_grads[None],
    )


def solution(mesh):
    return jax.shard_map(
        shards,
        mesh=mesh,
        in_specs=(
            P("dp", None, None),
            P("dp", None, None),
            P("dp", None),
            P("section", None, None, "tensor"),
            P("section", "tensor", None),
            P("section", None, "tensor"),
            P("section", "tensor", None),
            P("section", None, None),
            P("section", None, None),
        ),
        out_specs=(
            P("section", "dp", None, None),
            P("section", "dp", None, None),
            P("section", "dp", None, "tensor"),
            P("section", "tensor", "dp"),
            P("section", "dp", "tensor"),
            P("section", "tensor", "dp"),
            P("section", None, "dp"),
            P("section", None, "dp"),
        ),
        check_vma=False,
    )
```
